128 devices in a mesh: blk: 32 (over x_hi, z, y), sub: 4 (over x_lo, core).
Axes of the slice: x: 4 (x_hi: 2, x_lo: 2; x = x_hi * 2 + x_lo), y: 4, z: 4, core: 2. Of those that a mesh axis runs over, the one named last changes fastest.
Arguments:
- integrals: float32 [32, 4, 32, 6144], P('blk', 'sub'), may hold values from -1 to 1
- slot_order: int32 [32, 4, 32], P('blk', 'sub'), may hold values from 0 to 31, each once within a row
- factor_rows: float32 [32, 4, 32, 4096], P(None, 'sub'), may hold values from -1 to 1.5, as said below
- occ_energy: float32 [384], replicated, may hold values from -1.5 to -0.3
- slab_index: int32 [1], replicated, may hold values from 0 to 127
- virt_energy: float32 [2048], replicated, may hold values from 0.1 to 3
Outputs:
- amplitudes: float32 [6144, 6144], P('blk', 'sub')
The draws below stay inside these ranges and needn't reach their ends.
Inputs may be any that keep to these rules, and one draw needn't show every extreme that they name: `slot_order`: each row of 32 entries holds every number from 0 to 31 once. `factor_rows`: the factor is lower triangular (zero above its diagonal) with diagonal entries between 0.5 and 1.5.
All inputs are finite; a program needn't handle non-finite values.
Results may differ from the reference program's by a relative error of at most 0.0001.
Values sent between devices are 32-bit elements; how exact they have to be, the bound alone decides.
A program may use at most 128 MiB of HBM per device.

```python
import jax
import jax.numpy as jnp
from jax import lax

NAUX = 4096
NVIRT = 2048
NOCC = 3
NOCC_ALL = 384
PIECE = 32
ROUND = 128
ROUNDS = 32
PAIRS = 6144
N_SUB = 4


def draw_factor_rows(key, part):
    diag_key = jax.random.fold_in(key, 11)
    noise_key = jax.random.fold_in(key, 23)
    degrees = 2 * NAUX
    row_ids = jnp.arange(NAUX, dtype=jnp.int32)
    shapes = (degrees - row_ids).astype(jnp.float32) * 0.5
    chi_square = 2.0 * jax.random.gamma(diag_key, shapes, (NAUX,), jnp.float32)
    diagonal = jnp.sqrt(chi_square / jnp.float32(degrees))
    noise = jnp.clip(jax.random.normal(noise_key, (NAUX, NAUX), jnp.float32), -6.0, 6.0)
    row_scale = jnp.ones((NAUX,), jnp.float32)
    below = row_ids[:, None] > row_ids[None, :]
    on_diag = row_ids[:, None] == row_ids[None, :]
    off_part = noise / jnp.sqrt(jnp.float32(degrees))
    diag_part = jnp.clip(diagonal * row_scale, 0.5, 1.5)
    whole = jnp.where(below, off_part, 0.0)
    whole = jnp.where(on_diag, diag_part[:, None], whole)
    return whole.reshape(ROUNDS, ROUND // PIECE, PIECE, NAUX).astype(jnp.float32)


def block_levels(stream_key, shape, shards, low, high):
    def one(dim, blocks):
        steps = jax.random.uniform(jax.random.fold_in(jax.random.fold_in(stream_key, 6), dim), (blocks,), jnp.float32, low / len(shards), high / len(shards))
        return jnp.repeat(jnp.exp(steps), shape[dim] // blocks).reshape((-1,) + (1,) * (len(shape) - dim - 1))

    loudness = one(*shards[0])
    for cut in shards[1:]:
        loudness = loudness * one(*cut)
    return loudness


def centred(own_key, shape, deviation, most, split=(), kind=jnp.bfloat16):
    result = jax.random.normal(own_key, shape, jnp.float32) * deviation
    if len(split) > 0:
        result = block_levels(own_key, shape, split, -0.22, 0.18) * result
    return jnp.clip(result, min=-most, max=most).astype(kind)


def setup_inputs(seed: int = 0) -> dict:
    seeds = jax.random.split(jax.random.key(seed), 7)
    return {
        "integrals": centred(seeds[0], (ROUNDS, N_SUB, PIECE, PAIRS), 0.125, 1.0, ((0, 32), (1, 4)), jnp.float32),
        "slot_order": jax.vmap(lambda own: jax.random.permutation(own, PIECE))(jax.random.split(seeds[1], ROUNDS * N_SUB)).reshape((ROUNDS, N_SUB, PIECE)).astype(jnp.int32),
        "factor_rows": draw_factor_rows(jax.random.fold_in(seeds[6], 71), 0),
        "occ_energy": jnp.clip(jax.random.uniform(seeds[3], (NOCC_ALL,), jnp.float32, -1.5, -0.3), -1.5, -0.3),
        "slab_index": jax.random.randint(seeds[4], (1,), 0, NOCC_ALL // NOCC).astype(jnp.int32),
        "virt_energy": jnp.clip(jax.random.uniform(seeds[5], (NVIRT,), jnp.float32, 0.1, 3.0), 0.1, 3.0),
    }


PRECISE = lax.Precision.HIGHEST

def reference(integrals, slot_order, factor_rows, occ_energy, slab_index, virt_energy):
    piece_len = integrals.shape[2]
    places = jnp.arange(piece_len, dtype=jnp.int32)
    onehot = (slot_order[..., None] == places).astype(jnp.float32)
    canonical = jnp.einsum('rscq,rscp->rsqp', onehot, integrals.astype(jnp.float32), precision=PRECISE)
    right_side = canonical.reshape(NAUX, PAIRS)
    factor = factor_rows.reshape(NAUX, NAUX)
    fitted = jax.scipy.linalg.solve_triangular(factor, right_side, lower=True)
    coulomb = lax.dot_general(fitted, fitted, (((0,), (0,)), ((), ())), precision=PRECISE)
    slab_start = slab_index[0].astype(jnp.int32) * NOCC
    occ_slab = lax.dynamic_slice_in_dim(occ_energy, slab_start, NOCC)
    pair_energy = jnp.repeat(occ_slab, NVIRT) - jnp.tile(virt_energy, NOCC)
    return coulomb / (pair_energy[:, None] + pair_energy[None, :])
```

```python
import functools

import jax
import jax.numpy as jnp
from jax import lax
from jax.experimental import pallas as pl
from jax.experimental.pallas import tpu as pltpu
from jax.sharding import PartitionSpec as P

NVIRT = 2048
NOCC = 3
PRECISE = lax.Precision.HIGHEST
F32 = jnp.float32
BF16 = jnp.bfloat16
MESH = pl.DeviceIdType.MESH
NN = (((1,), (0,)), ((), ()))
NT = (((1,), (1,)), ((), ()))


def split(x):
    high = x.astype(BF16)
    return high, (x - high.astype(F32)).astype(BF16)


def dot3(a, b, dims):
    def one(p, q):
        return lax.dot_general(p, q, dims, preferred_element_type=F32)

    return one(a[0], b[0]) + (one(a[0], b[1]) + one(a[1], b[0]))


def canonical_order(integrals, slot_order):
    piece_len = integrals.shape[2]
    places = jnp.arange(piece_len, dtype=jnp.int32)
    onehot = (slot_order[..., None] == places).astype(jnp.float32)
    return jnp.einsum("rscq,rscp->rsqp", onehot, integrals, precision=PRECISE)


def inverse_of(block):
    n = block.shape[0]
    row = lax.broadcasted_iota(jnp.int32, (n, n), 0)
    col = lax.broadcasted_iota(jnp.int32, (n, n), 1)
    diag = jnp.sum(jnp.where(row == col, block, 0.0), axis=1, keepdims=True)
    inv = jnp.where(row == col, 1.0 / diag, 0.0)
    size = 1
    while size < n:
        below = (row // size == col // size + 1) & (row // (2 * size) == col // (2 * size))
        part = split(jnp.where(below, block, 0.0))
        now = split(inv)
        inv = inv - dot3(now, split(dot3(part, now, NN)), NN)
        size *= 2
    return inv


def inverse_kernel(diag_ref, inv_ref):
    for k in range(diag_ref.shape[0]):
        inv_ref[k] = inverse_of(diag_ref[k])


def diag_inverses(diag_blocks):
    rounds, width, _ = diag_blocks.shape
    batch = 8
    spec = pl.BlockSpec((batch, width, width), lambda i: (i, 0, 0))
    return pl.pallas_call(
        inverse_kernel,
        grid=(rounds // batch,),
        in_specs=[spec],
        out_specs=spec,
        out_shape=jax.ShapeDtypeStruct(diag_blocks.shape, F32),
    )(diag_blocks)


def gram_kernel(own, out, rowbuf, colbuf, acc, colh, coll, exch, total, final,
                y_send, y_recv, z_send, z_recv, s_send, s_recv, t_send, t_recv):
    chunks, rows, depth = own.shape
    half = 2 * rows
    blk, sub = lax.axis_index("blk"), lax.axis_index("sub")
    y, z, xh = blk % 4, (blk // 4) % 4, blk // 16
    xl, core = sub // 2, sub % 2
    same = xh == xl

    def y_at(offset):
        return {"blk": blk - y + (y + offset + 4) % 4, "sub": sub}

    def z_at(offset):
        return {"blk": blk - 4 * z + 4 * ((z + offset + 4) % 4), "sub": sub}

    swap = {"blk": blk + (1 - 2 * xh) * 16, "sub": sub + (1 - 2 * xl) * 2}
    mate = {"blk": blk, "sub": sub + 1 - 2 * core}

    barrier = pltpu.get_barrier_semaphore()
    for who in (y_at(1), y_at(-1), y_at(2), z_at(1), z_at(-1), swap, mate):
        pl.semaphore_signal(barrier, inc=1, device_id=who, device_id_type=MESH)
    pl.semaphore_wait(barrier, 7)

    def copy(src, dst, send, recv, who):
        return pltpu.make_async_remote_copy(
            src_ref=src, dst_ref=dst, send_sem=send, recv_sem=recv,
            device_id=who, device_id_type=MESH)

    def y_own(c):
        for k, offset in enumerate((1, -1)):
            copy(own.at[c], rowbuf.at[y, c], y_send.at[k, c], y_recv.at[k, c], y_at(offset)).start()

    def z_own(c):
        @pl.when(same)
        def _():
            for k, offset in enumerate((1, -1)):
                copy(own.at[c], colbuf.at[z, c], z_send.at[k, c], z_recv.at[k, c], z_at(offset)).start()

        @pl.when(jnp.logical_not(same))
        def _():
            copy(own.at[c], colbuf.at[z, c], s_send.at[c], s_recv.at[c], swap).wait_recv()
            for k, offset in enumerate((1, -1)):
                copy(colbuf.at[z, c], colbuf.at[z, c], z_send.at[k, c], z_recv.at[k, c], z_at(offset)).start()

    def got(buf, recv, send, place, k, c):
        copy(buf.at[place, c], buf.at[place, c], send.at[k, c], recv.at[k, c], mate).wait_recv()

    def forward(c):
        odd = c % 2
        step = 1 - 2 * odd
        src = (y - step + 4) % 4
        got(rowbuf, y_recv, y_send, src, odd, c)
        copy(rowbuf.at[src, c], rowbuf.at[src, c], y_send.at[2, c], y_recv.at[2, c], y_at(step)).start()
        src = (z - step + 4) % 4
        got(colbuf, z_recv, z_send, src, odd, c)
        copy(colbuf.at[src, c], colbuf.at[src, c], z_send.at[2, c], z_recv.at[2, c], z_at(step)).start()

    def product(c, first):
        odd = c % 2
        step = 1 - 2 * odd
        got(rowbuf, y_recv, y_send, (y + step + 4) % 4, 1 - odd, c)
        got(colbuf, z_recv, z_send, (z + step + 4) % 4, 1 - odd, c)
        got(rowbuf, y_recv, y_send, (y + 2) % 4, 2, c)
        got(colbuf, z_recv, z_send, (z + 2) % 4, 2, c)
        for k in range(4):
            high, low = split(colbuf[k, c])
            colh[k * rows:(k + 1) * rows] = high
            coll[k * rows:(k + 1) * rows] = low

        def part(k, _):
            term = dot3(split(rowbuf[k, c]), (colh[...], coll[...]), NT)
            acc[k] = term if first else acc[k] + term
            return 0

        lax.fori_loop(0, 4, part, 0)

    @pl.when(jnp.logical_not(same))
    def _():
        def send(c, _):
            copy(own.at[c], colbuf.at[z, c], s_send.at[c], s_recv.at[c], swap).start()
            return 0

        lax.fori_loop(0, chunks, send, 0)

    y_own(0)
    y_own(1)
    rowbuf[y] = own[...]

    @pl.when(same)
    def _():
        colbuf[z] = own[...]

    z_own(0)
    z_own(1)
    y_own(2)
    forward(0)
    z_own(2)
    y_own(3)
    forward(1)
    product(0, True)

    def step(c, _):
        @pl.when(c + 1 < chunks)
        def _():
            z_own(c + 1)

        @pl.when(c + 2 < chunks)
        def _():
            y_own(c + 2)

        forward(c)
        product(c - 1, False)
        return 0

    lax.fori_loop(2, chunks, step, 0)
    product(chunks - 1, False)

    mine = pl.ds(pl.multiple_of(core * half, 128), half)
    theirs = pl.ds(pl.multiple_of((1 - core) * half, 128), half)
    trade = copy(acc.at[:, :, theirs], exch, t_send.at[3], t_recv.at[3], mate)
    trade.start()
    trade.wait()

    total[...] = acc[:, :, mine] + exch[...]
    sends = []
    for k, offset in enumerate((2, 1, -1)):
        to = (y + offset + 4) % 4
        sends.append(copy(total.at[to], final.at[y], t_send.at[k], t_recv.at[k], y_at(offset)))
        sends[-1].start()
    final[y] = total[y]
    for k, offset in enumerate((2, 1, -1)):
        src = (y - offset + 4) % 4
        copy(final.at[src], final.at[src], t_send.at[k], t_recv.at[k], mate).wait_recv()
    for k in range(2):
        for q in range(4):
            place = (k * 4 + q) * rows
            out[:, place:place + rows] = final[q, :, k * rows:(k + 1) * rows]
    for one in sends:
        one.wait_send()

    def drain(c, _):
        for k in range(3):
            copy(own.at[c], own.at[c], y_send.at[k, c], y_recv.at[k, c], mate).wait_send()
            copy(own.at[c], own.at[c], z_send.at[k, c], z_recv.at[k, c], mate).wait_send()

        @pl.when(jnp.logical_not(same))
        def _():
            copy(own.at[c], own.at[c], s_send.at[c], s_recv.at[c], swap).wait_send()

        return 0

    lax.fori_loop(0, chunks, drain, 0)


def gram(own):
    chunks, rows, depth = own.shape
    dma = pltpu.SemaphoreType.DMA
    return pl.pallas_call(
        gram_kernel,
        out_shape=jax.ShapeDtypeStruct((rows, 8 * rows), F32),
        in_specs=[pl.BlockSpec(memory_space=pltpu.VMEM)],
        out_specs=pl.BlockSpec(memory_space=pltpu.VMEM),
        scratch_shapes=[
            pltpu.VMEM((4, chunks, rows, depth), F32),
            pltpu.VMEM((4, chunks, rows, depth), F32),
            pltpu.VMEM((4, rows, 4 * rows), F32),
            pltpu.VMEM((4 * rows, depth), BF16),
            pltpu.VMEM((4 * rows, depth), BF16),
            pltpu.VMEM((4, rows, 2 * rows), F32),
            pltpu.VMEM((4, rows, 2 * rows), F32),
            pltpu.VMEM((4, rows, 2 * rows), F32),
            dma((3, chunks)), dma((3, chunks)), dma((3, chunks)), dma((3, chunks)),
            dma((chunks,)), dma((chunks,)), dma((4,)), dma((4,)),
        ],
        compiler_params=pltpu.CompilerParams(
            collective_id=1, has_side_effects=True, vmem_limit_bytes=50 * 2**20),
    )(own)


def after_section(solved, own_rows, rhs_rows, diag_inverse, first, reach):
    round_width = diag_inverse.shape[1]
    pair_cols = solved.shape[2]
    width = reach * round_width
    rows_part = own_rows[:, :, :width]

    def advance(round_id, solved):
        factor_part = lax.dynamic_index_in_dim(rows_part, round_id, 0, keepdims=False)
        known_part = jnp.dot(
            factor_part, solved[:reach].reshape(width, pair_cols), precision=PRECISE
        )
        updated = lax.dynamic_index_in_dim(rhs_rows, round_id, 0, keepdims=False) - known_part
        round_block = lax.all_gather(updated[None], "sub", axis=0, tiled=True).reshape(
            round_width, pair_cols
        )
        inverse = lax.dynamic_index_in_dim(diag_inverse, round_id, 0, keepdims=False)
        solved_round = jnp.dot(inverse, round_block, precision=PRECISE)
        return lax.dynamic_update_index_in_dim(solved, solved_round, round_id, 0)

    return lax.fori_loop(first, reach, advance, solved, unroll=True)


def shards(integrals, slot_order, factor_rows, occ_energy, slab_index, virt_energy):
    canonical = canonical_order(integrals, slot_order)
    local_rhs = lax.all_to_all(canonical, "blk", split_axis=3, concat_axis=0, tiled=True)
    rounds = factor_rows.shape[0]
    piece_len = factor_rows.shape[2]
    sub_count = lax.axis_size("sub")
    round_width = sub_count * piece_len
    pair_cols = local_rhs.shape[3]
    own_diag = jnp.stack([factor_rows[k, 0, :, k * round_width:(k + 1) * round_width] for k in range(rounds)])
    diag_blocks = lax.all_gather(own_diag[:, None], "sub", axis=1, tiled=True).reshape(
        rounds, round_width, round_width
    )
    diag_inverse = diag_inverses(diag_blocks)
    rhs_rows = local_rhs[:, 0]
    own_rows = factor_rows[:, 0]
    solved = jnp.zeros((rounds, round_width, pair_cols), jnp.float32)
    section_count = min(8, rounds)
    per_section = rounds // section_count
    for section_id in range(section_count):
        solved = after_section(
            solved, own_rows, rhs_rows, diag_inverse,
            section_id * per_section, (section_id + 1) * per_section,
        )
    sub_index = lax.axis_index("sub")
    total_pairs = pair_cols * lax.axis_size("blk")
    quarter = total_pairs // sub_count
    core_half = lax.dynamic_slice_in_dim(solved, (sub_index % 2) * (rounds // 2), rounds // 2)
    own = core_half.reshape(8, rounds // 2 * round_width // 8, pair_cols).transpose(0, 2, 1)
    coulomb = gram(own)
    slab_start = slab_index[0] * NOCC
    occ_slab = lax.dynamic_slice_in_dim(occ_energy, slab_start, NOCC)
    pair_energy = jnp.repeat(occ_slab, NVIRT) - jnp.tile(virt_energy, NOCC)
    row_energy = lax.dynamic_slice_in_dim(pair_energy, lax.axis_index("blk") * pair_cols, pair_cols)
    col_energy = lax.dynamic_slice_in_dim(pair_energy, sub_index * quarter, quarter)
    return coulomb / (row_energy[:, None] + col_energy[None, :])


def solution(mesh):
    in_specs = (
        P("blk", "sub", None, None),
        P("blk", "sub", None),
        P(None, "sub", None, None),
        P(),
        P(),
        P(),
    )
    out_specs = P("blk", "sub")
    return jax.shard_map(shards, mesh=mesh, in_specs=in_specs, out_specs=out_specs, check_vma=False)
```

```python
import functools

import jax
import jax.numpy as jnp
from jax import lax
from jax.experimental import pallas as pl
from jax.experimental.pallas import tpu as pltpu
from jax.sharding import PartitionSpec as P

NVIRT = 2048
NOCC = 3
PRECISE = lax.Precision.HIGHEST
F32 = jnp.float32
BF16 = jnp.bfloat16
MESH = pl.DeviceIdType.MESH
NN = (((1,), (0,)), ((), ()))
NT = (((1,), (1,)), ((), ()))


def split(x):
    high = x.astype(BF16)
    return high, (x - high.astype(F32)).astype(BF16)


def dot3(a, b, dims):
    def one(p, q):
        return lax.dot_general(p, q, dims, preferred_element_type=F32)

    return one(a[0], b[0]) + (one(a[0], b[1]) + one(a[1], b[0]))


def copy(src, dst, send, recv, who):
    return pltpu.make_async_remote_copy(
        src_ref=src, dst_ref=dst, send_sem=send, recv_sem=recv,
        device_id=who, device_id_type=MESH)


def panel_place(i, r):
    if isinstance(i, int):
        return (i, r - 2 * i) if i < 8 else (15 - i, r + 2)
    return jnp.where(i < 8, i, 15 - i), jnp.where(i < 8, r - 2 * i, r + 2)


def solve_kernel(integrals, slots, factor, out, pan, blocks, half_inv, half_tmp, dinv, sb, rhs, gbuf,
                 xh, xlow, xbuf, tx, xt,
                 pan_local, pan_send, pan_recv, diag_send, diag_recv, a_send, a_recv,
                 inv_send, inv_recv, g_send, g_recv, x_send, x_recv):
    blk, sub = lax.axis_index("blk"), lax.axis_index("sub")
    hi = blk // 16
    xl, core = sub // 2, sub % 2
    x = 2 * hi + xl
    mate = {"blk": blk, "sub": sub + 1 - 2 * core}
    peer = {"blk": blk, "sub": sub + 2 - 4 * xl}

    def beside(offset, to_core):
        other = (x + offset + 4) % 4
        return {"blk": blk + (other // 2 - hi) * 16, "sub": (other % 2) * 2 + to_core}

    for i in range(16):
        for q in range(2):
            copy(factor.at[2 * i + q, :, 256 * i:256 * i + 256], blocks.at[i // 2, q, xl, core],
                 diag_send, diag_recv, beside(1 if i < 8 else -1, i % 2)).start()
    for i in range(16):
        k, row = panel_place(i, 2 * i)
        piece = factor.at[2 * i:32, :, 256 * i:256 * i + 256]
        place = pan.at[k, row:row + 32 - 2 * i, core]
        pltpu.make_async_copy(piece, place, pan_local.at[i]).start()
        copy(piece, place, pan_send.at[i], pan_recv.at[i], mate).start()

    onehot = (slots[...] == lax.broadcasted_iota(jnp.int32, (32, 32), 0)).astype(F32).astype(BF16)

    def pick(v):
        return lax.dot_general(onehot, v, NN, preferred_element_type=F32)

    for g in range(16):
        value = integrals[:, 384 * g:384 * g + 384]
        high = value.astype(BF16)
        rest = value - high.astype(F32)
        mid = rest.astype(BF16)
        low = (rest - mid.astype(F32)).astype(BF16)
        picked = pick(high) + (pick(mid) + pick(low))
        for k in range(4):
            sb[4 * g + k] = picked[:, 96 * k:96 * k + 96]

    def spread(k, _):
        to = (blk + k) % 32
        for c in range(2):
            copy(sb.at[2 * to + c], rhs.at[2 * blk + core], a_send, a_recv,
                 {"blk": to, "sub": 2 * xl + c}).start()
        return 0

    lax.fori_loop(1, 32, spread, 0)
    copy(sb.at[2 * blk + 1 - core], rhs.at[2 * blk + core], a_send, a_recv, mate).start()
    rhs[2 * blk + core] = sb[2 * blk + core]

    for i in range(16):
        k, row = panel_place(i, 2 * i)
        piece = pan.at[k, row:row + 32 - 2 * i, core]
        pltpu.make_async_copy(piece, piece, pan_local.at[i]).wait()
        copy(piece, piece, pan_send.at[i], pan_recv.at[i], mate).wait_recv()
    copy(blocks.at[0:4], blocks.at[0:4], diag_send, diag_recv, mate).wait_recv()

    def place_own(j, _):
        k, row = panel_place(2 * j + core, 2 * (2 * j + core))
        for q in range(2):
            blocks[j, q, xl] = pan[k, row + q]
        return 0

    lax.fori_loop(0, 8, place_own, 0)

    row = lax.broadcasted_iota(jnp.int32, (128, 128), 0)
    col = lax.broadcasted_iota(jnp.int32, (128, 128), 1)

    def invert(g, _):
        def block(n):
            q = n % 2
            return blocks[2 * g + n // 2, q, :, :, :, 128 * q:128 * q + 128].reshape(128, 128)

        for n in range(4):
            value = block(n)
            diag = jnp.where(row == col, value, 0.0)
            down = 1.0 / jnp.sum(diag, axis=1, keepdims=True)
            across = 1.0 / jnp.sum(diag, axis=0, keepdims=True)
            below = (row == col + 1) & (row % 2 == 1)
            half_inv[4 * g + n] = jnp.where(row == col, down, 0.0) - jnp.where(below, value * down * across, 0.0)
        size = 2
        while size < 128:
            below = (row // size == col // size + 1) & (row // (2 * size) == col // (2 * size))
            for n in range(4):
                part = jnp.where(below, block(n), 0.0)
                half_tmp[n] = dot3(split(part), split(half_inv[4 * g + n]), NN)
            for n in range(4):
                now = half_inv[4 * g + n]
                half_inv[4 * g + n] = now - dot3(split(now), split(half_tmp[n]), NN)
            size *= 2
        for n in range(2):
            lower = blocks[2 * g + n, 1, :, :, :, 0:128].reshape(128, 128)
            half_tmp[n] = dot3(split(lower), split(half_inv[4 * g + 2 * n]), NN)
        for n in range(2):
            i = 2 * (2 * g + n) + core
            dinv[i, 0:128, 0:128] = half_inv[4 * g + 2 * n]
            dinv[i, 128:256, 128:256] = half_inv[4 * g + 2 * n + 1]
            dinv[i, 0:128, 128:256] = jnp.zeros((128, 128), F32)
            dinv[i, 128:256, 0:128] = -dot3(split(half_inv[4 * g + 2 * n + 1]), split(half_tmp[n]), NN)
        return 0

    lax.fori_loop(0, 4, invert, 0)

    def share(j, _):
        copy(dinv.at[2 * j + core], dinv.at[2 * j + core], inv_send, inv_recv, mate).start()
        return 0

    lax.fori_loop(0, 8, share, 0)
    copy(rhs.at[0:63], rhs.at[0:63], a_send, a_recv, mate).wait_recv()
    copy(dinv.at[0:8], dinv.at[0:8], inv_send, inv_recv, mate).wait_recv()

    def offer(i, value):
        gbuf[i, :, xl] = value.reshape(2, 64, 96)
        copy(gbuf.at[i, :, xl], gbuf.at[i, :, xl], g_send.at[i], g_recv.at[i], peer).start()

    def factor_part(i, t):
        k, at = panel_place(i, 2 * t)
        return split(pan[k, pl.ds(at, 2)].reshape(128, 256))

    offer(0, rhs[0:4].reshape(128, 96))

    def round_of(i, _):
        inverse = split(dinv[i])

        @pl.when(i > 0)
        def _():
            def later(t, _):
                term = dot3(factor_part(i - 1, t), (xh[...], xlow[...]), NN)
                rows = pl.ds(4 * t, 4)
                rhs[rows] = rhs[rows] - term.reshape(4, 32, 96)
                return 0

            lax.fori_loop(i + 1, 16, later, 0)

        other = gbuf.at[i, :, 1 - xl]
        copy(other, other, g_send.at[i], g_recv.at[i], peer).wait_recv()
        solved = dot3(inverse, split(gbuf[i].reshape(256, 96)), NN)
        high, low = split(solved)
        xh[...] = high
        xlow[...] = low

        @pl.when(i < 15)
        def _():
            term = dot3(factor_part(i, i + 1), (high, low), NN)
            offer(i + 1, rhs[pl.ds(4 * i + 4, 4)].reshape(128, 96) - term)

        xbuf[...] = solved.reshape(2, 128, 96)
        tx[i] = xbuf[1 - core].T
        copy(tx.at[i], xt.at[i, core], x_send, x_recv, mate).start()
        xt[i, core] = xbuf[core].T
        return 0

    lax.fori_loop(0, 16, round_of, 0)

    copy(tx, tx, x_send, x_recv, mate).wait_recv()
    out[...] = xt[...]

    for i in range(16):
        k, row = panel_place(i, 2 * i)
        piece = pan.at[k, row:row + 32 - 2 * i, core]
        copy(piece, piece, pan_send.at[i], pan_recv.at[i], mate).wait_send()
        mine = gbuf.at[i, :, xl]
        copy(mine, mine, g_send.at[i], g_recv.at[i], peer).wait_send()
    copy(blocks.at[0:4], blocks.at[0:4], diag_send, diag_recv, mate).wait_send()
    copy(sb.at[0:63], sb.at[0:63], a_send, a_recv, mate).wait_send()
    copy(dinv.at[0:8], dinv.at[0:8], inv_send, inv_recv, mate).wait_send()
    copy(tx, tx, x_send, x_recv, mate).wait_send()


def solve(integrals, slots, factor):
    dma = pltpu.SemaphoreType.DMA
    vmem = pl.BlockSpec(memory_space=pltpu.VMEM)
    return pl.pallas_call(
        solve_kernel,
        out_shape=jax.ShapeDtypeStruct((16, 2, 96, 128), F32),
        in_specs=[vmem, vmem, pl.BlockSpec(memory_space=pl.ANY)],
        out_specs=vmem,
        scratch_shapes=[
            pltpu.VMEM((8, 34, 2, 32, 256), F32),
            pltpu.VMEM((8, 2, 2, 2, 32, 256), F32),
            pltpu.VMEM((16, 128, 128), F32),
            pltpu.VMEM((4, 128, 128), F32),
            pltpu.VMEM((16, 256, 256), F32),
            pltpu.VMEM((64, 32, 96), F32),
            pltpu.VMEM((64, 32, 96), F32),
            pltpu.VMEM((16, 2, 2, 64, 96), F32),
            pltpu.VMEM((256, 96), BF16),
            pltpu.VMEM((256, 96), BF16),
            pltpu.VMEM((2, 128, 96), F32),
            pltpu.VMEM((16, 96, 128), F32),
            pltpu.VMEM((16, 2, 96, 128), F32),
            dma((16,)), dma((16,)), dma((16,)), dma, dma, dma, dma, dma, dma,
            dma((16,)), dma((16,)), dma, dma,
        ],
        compiler_params=pltpu.CompilerParams(
            has_side_effects=True, vmem_limit_bytes=56 * 2**20),
    )(integrals, slots, factor)


def gram_kernel(own, out, rowbuf, colbuf, acc, colh, coll, exch, total, final,
                y_send, y_recv, z_send, z_recv, s_send, s_recv, t_send, t_recv):
    chunks, _, rows, depth = own.shape
    half = 2 * rows
    blk, sub = lax.axis_index("blk"), lax.axis_index("sub")
    y, z, xh = blk % 4, (blk // 4) % 4, blk // 16
    xl, core = sub // 2, sub % 2
    same = xh == xl

    def y_at(offset):
        return {"blk": blk - y + (y + offset + 4) % 4, "sub": sub}

    def z_at(offset):
        return {"blk": blk - 4 * z + 4 * ((z + offset + 4) % 4), "sub": sub}

    swap = {"blk": blk + (1 - 2 * xh) * 16, "sub": sub + (1 - 2 * xl) * 2}
    mate = {"blk": blk, "sub": sub + 1 - 2 * core}

    barrier = pltpu.get_barrier_semaphore()
    for who in (y_at(1), y_at(-1), y_at(2), z_at(1), z_at(-1), swap, mate):
        pl.semaphore_signal(barrier, inc=1, device_id=who, device_id_type=MESH)
    pl.semaphore_wait(barrier, 7)

    def whole(buf, k, c):
        return jnp.concatenate([buf[k, c, 0], buf[k, c, 1]], axis=1)

    def y_own(c):
        for k, offset in enumerate((1, -1)):
            copy(own.at[c], rowbuf.at[y, c], y_send.at[k, c], y_recv.at[k, c], y_at(offset)).start()

    def z_own(c):
        @pl.when(same)
        def _():
            for k, offset in enumerate((1, -1)):
                copy(own.at[c], colbuf.at[z, c], z_send.at[k, c], z_recv.at[k, c], z_at(offset)).start()

        @pl.when(jnp.logical_not(same))
        def _():
            copy(own.at[c], colbuf.at[z, c], s_send.at[c], s_recv.at[c], swap).wait_recv()
            for k, offset in enumerate((1, -1)):
                copy(colbuf.at[z, c], colbuf.at[z, c], z_send.at[k, c], z_recv.at[k, c], z_at(offset)).start()

    def got(buf, recv, send, place, k, c):
        copy(buf.at[place, c], buf.at[place, c], send.at[k, c], recv.at[k, c], mate).wait_recv()

    def forward(c):
        odd = c % 2
        step = 1 - 2 * odd
        src = (y - step + 4) % 4
        got(rowbuf, y_recv, y_send, src, odd, c)
        copy(rowbuf.at[src, c], rowbuf.at[src, c], y_send.at[2, c], y_recv.at[2, c], y_at(step)).start()
        src = (z - step + 4) % 4
        got(colbuf, z_recv, z_send, src, odd, c)
        copy(colbuf.at[src, c], colbuf.at[src, c], z_send.at[2, c], z_recv.at[2, c], z_at(step)).start()

    def product(c, first):
        odd = c % 2
        step = 1 - 2 * odd
        got(rowbuf, y_recv, y_send, (y + step + 4) % 4, 1 - odd, c)
        got(colbuf, z_recv, z_send, (z + step + 4) % 4, 1 - odd, c)
        got(rowbuf, y_recv, y_send, (y + 2) % 4, 2, c)
        got(colbuf, z_recv, z_send, (z + 2) % 4, 2, c)
        for k in range(4):
            high, low = split(whole(colbuf, k, c))
            colh[k * rows:(k + 1) * rows] = high
            coll[k * rows:(k + 1) * rows] = low

        def part(k, _):
            term = dot3(split(whole(rowbuf, k, c)), (colh[...], coll[...]), NT)
            acc[k] = term if first else acc[k] + term
            return 0

        lax.fori_loop(0, 4, part, 0)

    @pl.when(jnp.logical_not(same))
    def _():
        def send(c, _):
            copy(own.at[c], colbuf.at[z, c], s_send.at[c], s_recv.at[c], swap).start()
            return 0

        lax.fori_loop(0, chunks, send, 0)

    y_own(0)
    y_own(1)
    rowbuf[y] = own[...]

    @pl.when(same)
    def _():
        colbuf[z] = own[...]

    z_own(0)
    z_own(1)
    y_own(2)
    forward(0)
    z_own(2)
    y_own(3)
    forward(1)
    product(0, True)

    def step(c, _):
        @pl.when(c + 1 < chunks)
        def _():
            z_own(c + 1)

        @pl.when(c + 2 < chunks)
        def _():
            y_own(c + 2)

        forward(c)
        product(c - 1, False)
        return 0

    lax.fori_loop(2, chunks, step, 0)
    product(chunks - 1, False)

    mine = pl.ds(pl.multiple_of(core * half, 128), half)
    theirs = pl.ds(pl.multiple_of((1 - core) * half, 128), half)
    trade = copy(acc.at[:, :, theirs], exch, t_send.at[3], t_recv.at[3], mate)
    trade.start()
    trade.wait()

    total[...] = acc[:, :, mine] + exch[...]
    sends = []
    for k, offset in enumerate((2, 1, -1)):
        to = (y + offset + 4) % 4
        sends.append(copy(total.at[to], final.at[y], t_send.at[k], t_recv.at[k], y_at(offset)))
        sends[-1].start()
    final[y] = total[y]
    for k, offset in enumerate((2, 1, -1)):
        src = (y - offset + 4) % 4
        copy(final.at[src], final.at[src], t_send.at[k], t_recv.at[k], mate).wait_recv()
    for k in range(2):
        for q in range(4):
            place = (k * 4 + q) * rows
            out[:, place:place + rows] = final[q, :, k * rows:(k + 1) * rows]
    for one in sends:
        one.wait_send()

    def drain(c, _):
        for k in range(3):
            copy(own.at[c], own.at[c], y_send.at[k, c], y_recv.at[k, c], mate).wait_send()
            copy(own.at[c], own.at[c], z_send.at[k, c], z_recv.at[k, c], mate).wait_send()

        @pl.when(jnp.logical_not(same))
        def _():
            copy(own.at[c], own.at[c], s_send.at[c], s_recv.at[c], swap).wait_send()

        return 0

    lax.fori_loop(0, chunks, drain, 0)


def gram(own):
    chunks, _, rows, depth = own.shape
    dma = pltpu.SemaphoreType.DMA
    return pl.pallas_call(
        gram_kernel,
        out_shape=jax.ShapeDtypeStruct((rows, 8 * rows), F32),
        in_specs=[pl.BlockSpec(memory_space=pltpu.VMEM)],
        out_specs=pl.BlockSpec(memory_space=pltpu.VMEM),
        scratch_shapes=[
            pltpu.VMEM((4, chunks, 2, rows, depth), F32),
            pltpu.VMEM((4, chunks, 2, rows, depth), F32),
            pltpu.VMEM((4, rows, 4 * rows), F32),
            pltpu.VMEM((4 * rows, 2 * depth), BF16),
            pltpu.VMEM((4 * rows, 2 * depth), BF16),
            pltpu.VMEM((4, rows, 2 * rows), F32),
            pltpu.VMEM((4, rows, 2 * rows), F32),
            pltpu.VMEM((4, rows, 2 * rows), F32),
            dma((3, chunks)), dma((3, chunks)), dma((3, chunks)), dma((3, chunks)),
            dma((chunks,)), dma((chunks,)), dma((4,)), dma((4,)),
        ],
        compiler_params=pltpu.CompilerParams(
            collective_id=1, has_side_effects=True, vmem_limit_bytes=50 * 2**20),
    )(own)


def shards(integrals, slot_order, factor_rows, occ_energy, slab_index, virt_energy):
    fitted = solve(integrals[0, 0], slot_order[0], factor_rows[:, 0])
    coulomb = gram(fitted.reshape(8, 2, 192, 128))
    pair_rows, quarter = coulomb.shape
    slab_start = slab_index[0] * NOCC
    occ_slab = lax.dynamic_slice_in_dim(occ_energy, slab_start, NOCC)
    pair_energy = jnp.repeat(occ_slab, NVIRT) - jnp.tile(virt_energy, NOCC)
    row_energy = lax.dynamic_slice_in_dim(pair_energy, lax.axis_index("blk") * pair_rows, pair_rows)
    col_energy = lax.dynamic_slice_in_dim(pair_energy, lax.axis_index("sub") * quarter, quarter)
    return coulomb / (row_energy[:, None] + col_energy[None, :])


def solution(mesh):
    in_specs = (
        P("blk", "sub", None, None),
        P("blk", "sub", None),
        P(None, "sub", None, None),
        P(),
        P(),
        P(),
    )
    out_specs = P("blk", "sub")
    return jax.shard_map(shards, mesh=mesh, in_specs=in_specs, out_specs=out_specs, check_vma=False)
```

```python
import functools

import jax
import jax.numpy as jnp
from jax import lax
from jax.experimental import pallas as pl
from jax.experimental.pallas import tpu as pltpu
from jax.sharding import PartitionSpec as P

NVIRT = 2048
NOCC = 3
PRECISE = lax.Precision.HIGHEST
F32 = jnp.float32
BF16 = jnp.bfloat16
MESH = pl.DeviceIdType.MESH
NN = (((1,), (0,)), ((), ()))
NT = (((1,), (1,)), ((), ()))


def split(x):
    high = x.astype(BF16)
    return high, (x - high.astype(F32)).astype(BF16)


def dot3(a, b, dims):
    def one(p, q):
        return lax.dot_general(p, q, dims, preferred_element_type=F32)

    return one(a[0], b[0]) + (one(a[0], b[1]) + one(a[1], b[0]))


def copy(src, dst, send, recv, who):
    return pltpu.make_async_remote_copy(
        src_ref=src, dst_ref=dst, send_sem=send, recv_sem=recv,
        device_id=who, device_id_type=MESH)


def panel_place(i, r):
    if isinstance(i, int):
        return (i, r - 2 * i) if i < 8 else (15 - i, r + 2)
    return jnp.where(i < 8, i, 15 - i), jnp.where(i < 8, r - 2 * i, r + 2)


def fused_kernel(integrals, slots, factor, out, pan, blocks, half_inv, half_tmp, dinv, sb, rhs, gbuf,
                 xh, xlow, xbuf, tx, rowbuf, colbuf, acc, colh, coll, exch, total, final, relay,
                 pan_local, pan_send, pan_recv, diag_send, diag_recv, a_send, a_recv,
                 inv_send, inv_recv, g_send, g_recv, x_send, x_recv,
                 y_send, y_recv, z_send, z_recv, s_send, s_recv, t_send, t_recv, e_send, e_recv):
    blk, sub = lax.axis_index("blk"), lax.axis_index("sub")
    hi = blk // 16
    xl, core = sub // 2, sub % 2
    x = 2 * hi + xl
    y, z = blk % 4, (blk // 4) % 4
    same = hi == xl
    mate = {"blk": blk, "sub": sub + 1 - 2 * core}
    peer = {"blk": blk, "sub": sub + 2 - 4 * xl}

    def beside(offset, to_core):
        other = (x + offset + 4) % 4
        return {"blk": blk + (other // 2 - hi) * 16, "sub": (other % 2) * 2 + to_core}

    def y_at(offset):
        return {"blk": blk - y + (y + offset + 4) % 4, "sub": sub}

    def z_at(offset):
        return {"blk": blk - 4 * z + 4 * ((z + offset + 4) % 4), "sub": sub}

    swap = {"blk": blk + (1 - 2 * hi) * 16, "sub": sub + (1 - 2 * xl) * 2}

    for i in range(16):
        for q in range(2):
            copy(factor.at[2 * i + q, :, 256 * i:256 * i + 256], blocks.at[i // 2, q, xl, core],
                 diag_send, diag_recv, beside(1 if i < 8 else -1, i % 2)).start()
    for i in range(16):
        k, row = panel_place(i, 2 * i)
        piece = factor.at[2 * i:32, :, 256 * i:256 * i + 256]
        place = pan.at[k, row:row + 32 - 2 * i, core]
        pltpu.make_async_copy(piece, place, pan_local.at[i]).start()
        copy(piece, place, pan_send.at[i], pan_recv.at[i], mate).start()

    onehot = (slots[...] == lax.broadcasted_iota(jnp.int32, (32, 32), 0)).astype(F32).astype(BF16)

    def pick(v):
        return lax.dot_general(onehot, v, NN, preferred_element_type=F32)

    for g in range(16):
        value = integrals[:, 384 * g:384 * g + 384]
        high = value.astype(BF16)
        rest = value - high.astype(F32)
        mid = rest.astype(BF16)
        low = (rest - mid.astype(F32)).astype(BF16)
        picked = pick(high) + (pick(mid) + pick(low))
        for k in range(4):
            sb[4 * g + k] = picked[:, 96 * k:96 * k + 96]

    def spread(k, _):
        to = (blk + k) % 32
        for c in range(2):
            copy(sb.at[2 * to + c], rhs.at[2 * blk + core], a_send, a_recv,
                 {"blk": to, "sub": 2 * xl + c}).start()
        return 0

    lax.fori_loop(1, 32, spread, 0)
    copy(sb.at[2 * blk + 1 - core], rhs.at[2 * blk + core], a_send, a_recv, mate).start()
    rhs[2 * blk + core] = sb[2 * blk + core]

    for i in range(16):
        k, row = panel_place(i, 2 * i)
        piece = pan.at[k, row:row + 32 - 2 * i, core]
        pltpu.make_async_copy(piece, piece, pan_local.at[i]).wait()
        copy(piece, piece, pan_send.at[i], pan_recv.at[i], mate).wait_recv()
    copy(blocks.at[0:4], blocks.at[0:4], diag_send, diag_recv, mate).wait_recv()

    def place_own(j, _):
        k, row = panel_place(2 * j + core, 2 * (2 * j + core))
        for q in range(2):
            blocks[j, q, xl] = pan[k, row + q]
        return 0

    lax.fori_loop(0, 8, place_own, 0)

    row = lax.broadcasted_iota(jnp.int32, (128, 128), 0)
    col = lax.broadcasted_iota(jnp.int32, (128, 128), 1)

    def invert(g, _):
        def block(n):
            q = n % 2
            return blocks[2 * g + n // 2, q, :, :, :, 128 * q:128 * q + 128].reshape(128, 128)

        for n in range(4):
            value = block(n)
            diag = jnp.where(row == col, value, 0.0)
            down = 1.0 / jnp.sum(diag, axis=1, keepdims=True)
            across = 1.0 / jnp.sum(diag, axis=0, keepdims=True)
            below = (row == col + 1) & (row % 2 == 1)
            half_inv[4 * g + n] = jnp.where(row == col, down, 0.0) - jnp.where(below, value * down * across, 0.0)
        size = 2
        while size < 128:
            below = (row // size == col // size + 1) & (row // (2 * size) == col // (2 * size))
            for n in range(4):
                part = jnp.where(below, block(n), 0.0)
                half_tmp[n] = dot3(split(part), split(half_inv[4 * g + n]), NN)
            for n in range(4):
                now = half_inv[4 * g + n]
                half_inv[4 * g + n] = now - dot3(split(now), split(half_tmp[n]), NN)
            size *= 2
        for n in range(2):
            lower = blocks[2 * g + n, 1, :, :, :, 0:128].reshape(128, 128)
            half_tmp[n] = dot3(split(lower), split(half_inv[4 * g + 2 * n]), NN)
        for n in range(2):
            i = 2 * (2 * g + n) + core
            dinv[i, 0:128, 0:128] = half_inv[4 * g + 2 * n]
            dinv[i, 128:256, 128:256] = half_inv[4 * g + 2 * n + 1]
            dinv[i, 0:128, 128:256] = jnp.zeros((128, 128), F32)
            dinv[i, 128:256, 0:128] = -dot3(split(half_inv[4 * g + 2 * n + 1]), split(half_tmp[n]), NN)
        return 0

    lax.fori_loop(0, 4, invert, 0)

    def share(j, _):
        copy(dinv.at[2 * j + core], dinv.at[2 * j + core], inv_send, inv_recv, mate).start()
        return 0

    lax.fori_loop(0, 8, share, 0)
    copy(rhs.at[0:63], rhs.at[0:63], a_send, a_recv, mate).wait_recv()
    copy(dinv.at[0:8], dinv.at[0:8], inv_send, inv_recv, mate).wait_recv()

    def offer(i, value):
        gbuf[i, :, xl] = value.reshape(2, 64, 96)
        copy(gbuf.at[i, :, xl], gbuf.at[i, :, xl], g_send.at[i], g_recv.at[i], peer).start()

    def factor_part(i, t):
        k, at = panel_place(i, 2 * t)
        return split(pan[k, pl.ds(at, 2)].reshape(128, 256))

    def own_out(i):
        half = rowbuf.at[y, i, 1 - core]
        copy(half, half, x_send, x_recv.at[i], mate).wait_recv()
        for k, offset in enumerate((1, -1)):
            copy(rowbuf.at[y, i], rowbuf.at[y, i], y_send.at[k, i], y_recv.at[k, i], y_at(offset)).start()

        @pl.when(same)
        def _():
            for k, offset in enumerate((1, -1)):
                copy(rowbuf.at[y, i], colbuf.at[z, i], z_send.at[k, i], z_recv.at[k, i], z_at(offset)).start()
            colbuf[z, i] = rowbuf[y, i]

        @pl.when(jnp.logical_not(same))
        def _():
            copy(rowbuf.at[y, i], colbuf.at[z, i], s_send.at[i], s_recv.at[i], swap).start()

    def swapped_out(i):
        @pl.when(jnp.logical_not(same))
        def _():
            copy(colbuf.at[z, i], colbuf.at[z, i], s_send.at[i], s_recv.at[i], swap).wait_recv()
            for k, offset in enumerate((1, -1)):
                copy(colbuf.at[z, i], colbuf.at[z, i], z_send.at[k, i], z_recv.at[k, i], z_at(offset)).start()

    def got(buf, send, recv, place, k, i):
        copy(buf.at[place, i], buf.at[place, i], send.at[k, i], recv.at[k, i], mate).wait_recv()

    def forward(i):
        odd = i % 2
        step = 1 - 2 * odd
        src = (y - step + 4) % 4
        got(rowbuf, y_send, y_recv, src, odd, i)
        copy(rowbuf.at[src, i], rowbuf.at[src, i], y_send.at[2, i], y_recv.at[2, i], y_at(step)).start()
        src = (z - step + 4) % 4
        got(colbuf, z_send, z_recv, src, odd, i)
        copy(colbuf.at[src, i], colbuf.at[src, i], z_send.at[2, i], z_recv.at[2, i], z_at(step)).start()

    def whole(buf, k, c):
        return jnp.concatenate([buf[k, 2 * c].reshape(192, 128), buf[k, 2 * c + 1].reshape(192, 128)], axis=1)

    def arrived(c):
        for odd in range(2):
            i = 2 * c + odd
            step = 1 - 2 * odd
            got(rowbuf, y_send, y_recv, (y + step + 4) % 4, 1 - odd, i)
            got(colbuf, z_send, z_recv, (z + step + 4) % 4, 1 - odd, i)
            got(rowbuf, y_send, y_recv, (y + 2) % 4, 2, i)
            got(colbuf, z_send, z_recv, (z + 2) % 4, 2, i)
        for k in range(4):
            high, low = split(whole(colbuf, k, c))
            colh[k * 192:k * 192 + 192] = high
            coll[k * 192:k * 192 + 192] = low

    def product_rows(c, k):
        acc[k] = acc[k] + dot3(split(whole(rowbuf, k, c)), (colh[...], coll[...]), NT)

    def product(c):
        arrived(c)

        def part(k, _):
            product_rows(c, k)
            return 0

        lax.fori_loop(0, 4, part, 0)

    acc[...] = jnp.zeros_like(acc)
    offer(0, rhs[0:4].reshape(128, 96))

    def round_of(i, _):
        inverse = split(dinv[i])

        @pl.when(i > 0)
        def _():
            def later(t, _):
                term = dot3(factor_part(i - 1, t), (xh[...], xlow[...]), NN)
                rows = pl.ds(4 * t, 4)
                rhs[rows] = rhs[rows] - term.reshape(4, 32, 96)
                return 0

            lax.fori_loop(i + 1, 16, later, 0)
            own_out(i - 1)

        @pl.when(i > 1)
        def _():
            swapped_out(i - 2)

        @pl.when(i > 3)
        def _():
            forward(i - 4)

        @pl.when((i > 6) & (i % 2 == 1))
        def _():
            product((i - 7) // 2)

        other = gbuf.at[i, :, 1 - xl]
        copy(other, other, g_send.at[i], g_recv.at[i], peer).wait_recv()
        solved = dot3(inverse, split(gbuf[i].reshape(256, 96)), NN)
        high, low = split(solved)
        xh[...] = high
        xlow[...] = low

        @pl.when(i < 15)
        def _():
            term = dot3(factor_part(i, i + 1), (high, low), NN)
            offer(i + 1, rhs[pl.ds(4 * i + 4, 4)].reshape(128, 96) - term)

        xbuf[...] = solved.reshape(2, 128, 96)
        tx[i] = xbuf[1 - core].T
        copy(tx.at[i], rowbuf.at[y, i, core], x_send, x_recv.at[i], mate).start()
        rowbuf[y, i, core] = xbuf[core].T
        return 0

    lax.fori_loop(0, 16, round_of, 0)

    own_out(15)
    swapped_out(14)
    forward(12)
    forward(13)
    swapped_out(15)
    product(5)
    forward(14)
    product(6)
    forward(15)
    arrived(7)

    mine = pl.ds(pl.multiple_of(core * 384, 128), 384)
    theirs = pl.ds(pl.multiple_of((1 - core) * 384, 128), 384)
    order = [(y + 2) % 4, (y + 1) % 4, (y + 3) % 4, y]

    def trade(n):
        k = order[n]
        return copy(acc.at[k, :, theirs], exch.at[k], t_send.at[n], t_recv.at[n], mate)

    for n in range(4):
        product_rows(7, order[n])
        trade(n).start()

    def summed(n):
        trade(n).wait_recv()
        k = order[n]
        total[k] = acc[k, :, mine] + exch[k]

    summed(0)
    hops = []
    for at, offset in enumerate((1, -1)):
        hops.append(copy(total.at[order[0], 96 * at:96 * at + 96], relay.at[at],
                         e_send.at[at], e_recv.at[at], y_at(offset)))
        hops[-1].start()
    for n, offset in ((1, 1), (2, -1)):
        summed(n)
        hops.append(copy(total.at[order[n]], final.at[y], e_send.at[n + 1], e_recv.at[n + 1], y_at(offset)))
        hops[-1].start()
    for at, offset in enumerate((1, -1)):
        copy(relay.at[at], relay.at[at], e_send.at[at], e_recv.at[at], mate).wait_recv()
        src = (y - offset + 4) % 4
        hops.append(copy(relay.at[at], final.at[src, 96 * at:96 * at + 96],
                         e_send.at[4 + at], e_recv.at[4 + at], y_at(offset)))
        hops[-1].start()
    summed(3)
    final[y] = total[y]
    for n, offset in ((1, 1), (2, -1)):
        src = (y - offset + 4) % 4
        copy(final.at[src], final.at[src], e_send.at[n + 1], e_recv.at[n + 1], mate).wait_recv()
    src = (y + 2) % 4
    for at in range(2):
        piece = final.at[src, 96 * at:96 * at + 96]
        copy(piece, piece, e_send.at[4 + at], e_recv.at[4 + at], mate).wait_recv()
    for k in range(2):
        for q in range(4):
            place = (k * 4 + q) * 192
            out[:, place:place + 192] = final[q, :, k * 192:k * 192 + 192]
    for hop in hops:
        hop.wait_send()
    for n in range(4):
        trade(n).wait_send()

    def drain(i, _):
        piece = rowbuf.at[y, i]
        for k in range(3):
            copy(piece, piece, y_send.at[k, i], y_recv.at[k, i], mate).wait_send()
            copy(piece, piece, z_send.at[k, i], z_recv.at[k, i], mate).wait_send()

        @pl.when(jnp.logical_not(same))
        def _():
            copy(piece, piece, s_send.at[i], s_recv.at[i], swap).wait_send()

        return 0

    lax.fori_loop(0, 16, drain, 0)

    for i in range(16):
        k, row = panel_place(i, 2 * i)
        piece = pan.at[k, row:row + 32 - 2 * i, core]
        copy(piece, piece, pan_send.at[i], pan_recv.at[i], mate).wait_send()
        mine = gbuf.at[i, :, xl]
        copy(mine, mine, g_send.at[i], g_recv.at[i], peer).wait_send()
    copy(blocks.at[0:4], blocks.at[0:4], diag_send, diag_recv, mate).wait_send()
    copy(sb.at[0:63], sb.at[0:63], a_send, a_recv, mate).wait_send()
    copy(dinv.at[0:8], dinv.at[0:8], inv_send, inv_recv, mate).wait_send()
    copy(tx, tx, x_send, x_recv.at[0], mate).wait_send()


def coulomb_block(integrals, slots, factor):
    dma = pltpu.SemaphoreType.DMA
    vmem = pl.BlockSpec(memory_space=pltpu.VMEM)
    return pl.pallas_call(
        fused_kernel,
        out_shape=jax.ShapeDtypeStruct((192, 1536), F32),
        in_specs=[vmem, vmem, pl.BlockSpec(memory_space=pl.ANY)],
        out_specs=vmem,
        scratch_shapes=[
            pltpu.VMEM((8, 34, 2, 32, 256), F32),
            pltpu.VMEM((8, 2, 2, 2, 32, 256), F32),
            pltpu.VMEM((16, 128, 128), F32),
            pltpu.VMEM((4, 128, 128), F32),
            pltpu.VMEM((16, 256, 256), F32),
            pltpu.VMEM((64, 32, 96), F32),
            pltpu.VMEM((64, 32, 96), F32),
            pltpu.VMEM((16, 2, 2, 64, 96), F32),
            pltpu.VMEM((256, 96), BF16),
            pltpu.VMEM((256, 96), BF16),
            pltpu.VMEM((2, 128, 96), F32),
            pltpu.VMEM((16, 96, 128), F32),
            pltpu.VMEM((4, 16, 2, 96, 128), F32),
            pltpu.VMEM((4, 16, 2, 96, 128), F32),
            pltpu.VMEM((4, 192, 768), F32),
            pltpu.VMEM((768, 256), BF16),
            pltpu.VMEM((768, 256), BF16),
            pltpu.VMEM((4, 192, 384), F32),
            pltpu.VMEM((4, 192, 384), F32),
            pltpu.VMEM((4, 192, 384), F32),
            pltpu.VMEM((2, 96, 384), F32),
            dma((16,)), dma((16,)), dma((16,)), dma, dma, dma, dma, dma, dma,
            dma((16,)), dma((16,)), dma, dma((16,)),
            dma((3, 16)), dma((3, 16)), dma((3, 16)), dma((3, 16)), dma((16,)), dma((16,)),
            dma((4,)), dma((4,)), dma((6,)), dma((6,)),
        ],
        compiler_params=pltpu.CompilerParams(
            has_side_effects=True, vmem_limit_bytes=60 * 2**20),
    )(integrals, slots, factor)


def shards(integrals, slot_order, factor_rows, occ_energy, slab_index, virt_energy):
    coulomb = coulomb_block(integrals[0, 0], slot_order[0], factor_rows[:, 0])
    pair_rows, quarter = coulomb.shape
    slab_start = slab_index[0] * NOCC
    occ_slab = lax.dynamic_slice_in_dim(occ_energy, slab_start, NOCC)
    pair_energy = jnp.repeat(occ_slab, NVIRT) - jnp.tile(virt_energy, NOCC)
    row_energy = lax.dynamic_slice_in_dim(pair_energy, lax.axis_index("blk") * pair_rows, pair_rows)
    col_energy = lax.dynamic_slice_in_dim(pair_energy, lax.axis_index("sub") * quarter, quarter)
    return coulomb / (row_energy[:, None] + col_energy[None, :])


def solution(mesh):
    in_specs = (
        P("blk", "sub", None, None),
        P("blk", "sub", None),
        P(None, "sub", None, None),
        P(),
        P(),
        P(),
    )
    out_specs = P("blk", "sub")
    return jax.shard_map(shards, mesh=mesh, in_specs=in_specs, out_specs=out_specs, check_vma=False)
```

```python
import functools

import jax
import jax.numpy as jnp
from jax import lax
from jax.experimental import pallas as pl
from jax.experimental.pallas import tpu as pltpu
from jax.sharding import PartitionSpec as P

NOCC = 3
F32 = jnp.float32
BF16 = jnp.bfloat16
MESH = pl.DeviceIdType.MESH
NN = (((1,), (0,)), ((), ()))
NT = (((1,), (1,)), ((), ()))


def split(x):
    high = x.astype(BF16)
    return high, (x - high.astype(F32)).astype(BF16)


def dot3(a, b, dims):
    def one(p, q):
        return lax.dot_general(p, q, dims, preferred_element_type=F32)

    return one(a[0], b[0]) + (one(a[0], b[1]) + one(a[1], b[0]))


def copy(src, dst, send, recv, who):
    return pltpu.make_async_remote_copy(
        src_ref=src, dst_ref=dst, send_sem=send, recv_sem=recv,
        device_id=who, device_id_type=MESH)


def panel_place(i, r):
    if isinstance(i, int):
        return (i, r - 2 * i) if i < 8 else (15 - i, r + 2)
    return jnp.where(i < 8, i, 15 - i), jnp.where(i < 8, r - 2 * i, r + 2)


def fused_kernel(integrals, slots, factor, occ, slab, virt, out, pan, blocks, half_inv, half_tmp, dinv, sb, rhs, gbuf,
                 xh, xlow, xbuf, tx, rowbuf, colbuf, acc, cols, colh, coll, pairs, exch, total, final, relay,
                 pan_local, pan_send, pan_recv, diag_send, diag_recv, a_send, a_recv,
                 inv_send, inv_recv, g_send, g_recv, x_send, x_recv,
                 y_send, y_recv, z_send, z_recv, s_send, s_recv, t_send, t_recv, e_send, e_recv):
    blk, sub = lax.axis_index("blk"), lax.axis_index("sub")
    hi = blk // 16
    xl, core = sub // 2, sub % 2
    x = 2 * hi + xl
    y, z = blk % 4, (blk // 4) % 4
    same = hi == xl
    mate = {"blk": blk, "sub": sub + 1 - 2 * core}
    peer = {"blk": blk, "sub": sub + 2 - 4 * xl}

    def beside(offset, to_core):
        other = (x + offset + 4) % 4
        return {"blk": blk + (other // 2 - hi) * 16, "sub": (other % 2) * 2 + to_core}

    def y_at(offset):
        return {"blk": blk - y + (y + offset + 4) % 4, "sub": sub}

    def z_at(offset):
        return {"blk": blk - 4 * z + 4 * ((z + offset + 4) % 4), "sub": sub}

    swap = {"blk": blk + (1 - 2 * hi) * 16, "sub": sub + (1 - 2 * xl) * 2}

    barrier = pltpu.get_barrier_semaphore()

    def greet(k, _):
        for c in range(2):
            pl.semaphore_signal(barrier, inc=1, device_id_type=MESH,
                                device_id={"blk": (blk + k) % 32, "sub": 2 * xl + c})
        return 0

    lax.fori_loop(1, 32, greet, 0)
    pl.semaphore_signal(barrier, inc=1, device_id=mate, device_id_type=MESH)
    for offset in (1, -1):
        for c in range(2):
            pl.semaphore_signal(barrier, inc=1, device_id=beside(offset, c), device_id_type=MESH)

    def slab_of(i, q):
        wide = 128 * (q + 1)
        return factor.at[2 * i + q, :, pl.ds(pl.multiple_of(256 * i, 256), wide)]

    def slab_place(j, q, at_core):
        return blocks.at[j, q, xl, at_core, :, 0:128 * (q + 1)]

    order = (0, 1, 4, 5, 2, 3, 6, 7)
    for j in order:
        for q in range(2):
            pltpu.make_async_copy(slab_of(2 * j + core, q), slab_place(j, q, core), diag_recv.at[q, j // 2]).start()

    onehot = (slots[...] == lax.broadcasted_iota(jnp.int32, (32, 32), 0)).astype(F32).astype(BF16)

    def pick(v):
        return lax.dot_general(onehot, v, NN, preferred_element_type=F32)

    for g in range(16):
        value = integrals[:, 384 * g:384 * g + 384]
        high = value.astype(BF16)
        rest = value - high.astype(F32)
        mid = rest.astype(BF16)
        low = (rest - mid.astype(F32)).astype(BF16)
        picked = pick(high) + (pick(mid) + pick(low))
        for k in range(4):
            sb[4 * g + k] = picked[:, 96 * k:96 * k + 96]

    pl.semaphore_wait(barrier, 67)

    for j in order:
        for q in range(2):
            for c in range(2):
                copy(slab_of(2 * j + c, q), slab_place(j, q, core), diag_send.at[q], diag_recv.at[q, j // 2],
                     beside(1 if j < 4 else -1, c)).start()
            copy(slab_of(2 * j + 1 - core, q), slab_place(j, q, core), diag_send.at[q], diag_recv.at[q, j // 2],
                 mate).start()

    def spread(k, _):
        to = (blk + k) % 32
        for c in range(2):
            copy(sb.at[2 * to + c], rhs.at[2 * blk + core], a_send, a_recv,
                 {"blk": to, "sub": 2 * xl + c}).start()
        return 0

    lax.fori_loop(1, 32, spread, 0)
    copy(sb.at[2 * blk + 1 - core], rhs.at[2 * blk + core], a_send, a_recv, mate).start()
    rhs[2 * blk + core] = sb[2 * blk + core]

    for i in range(16):
        k, row = panel_place(i, 2 * i)
        piece = factor.at[2 * i:32, :, 256 * i:256 * i + 256]
        place = pan.at[k, row:row + 32 - 2 * i, core]
        pltpu.make_async_copy(piece, place, pan_local.at[i]).start()
        copy(piece, place, pan_send.at[i], pan_recv.at[i], mate).start()

    for t in range(12):
        pairs[:, 512 * t:512 * t + 512] = occ[slab[0] * NOCC + t // 4] - virt[:, 512 * (t % 4):512 * (t % 4) + 512]

    row = lax.broadcasted_iota(jnp.int32, (128, 128), 0)
    col = lax.broadcasted_iota(jnp.int32, (128, 128), 1)

    def invert(turn, _):
        g = (turn % 2) * 2 + turn // 2
        for q in range(2):
            piece = blocks.at[pl.ds(2 * g, 2), q, :, :, :, 0:128 * (q + 1)]
            pltpu.make_async_copy(piece, piece, diag_recv.at[q, g]).wait()

        def block(n):
            q = n % 2
            return blocks[2 * g + n // 2, q, :, :, :, 128 * q:128 * q + 128].reshape(128, 128)

        for n in range(4):
            value = block(n)
            diag = jnp.where(row == col, value, 0.0)
            down = 1.0 / jnp.sum(diag, axis=1, keepdims=True)
            across = 1.0 / jnp.sum(diag, axis=0, keepdims=True)
            below = (row == col + 1) & (row % 2 == 1)
            half_inv[4 * g + n] = jnp.where(row == col, down, 0.0) - jnp.where(below, value * down * across, 0.0)
        size = 2
        while size < 128:
            below = (row // size == col // size + 1) & (row // (2 * size) == col // (2 * size))
            for n in range(4):
                part = jnp.where(below, block(n), 0.0)
                half_tmp[n] = dot3(split(part), split(half_inv[4 * g + n]), NN)
            for n in range(4):
                now = half_inv[4 * g + n]
                half_inv[4 * g + n] = now - dot3(split(now), split(half_tmp[n]), NN)
            size *= 2
        for n in range(2):
            lower = blocks[2 * g + n, 1, :, :, :, 0:128].reshape(128, 128)
            half_tmp[n] = dot3(split(lower), split(half_inv[4 * g + 2 * n]), NN)
        for n in range(2):
            i = 2 * (2 * g + n) + core
            dinv[i, 0:128, 0:128] = half_inv[4 * g + 2 * n]
            dinv[i, 128:256, 128:256] = half_inv[4 * g + 2 * n + 1]
            dinv[i, 0:128, 128:256] = jnp.zeros((128, 128), F32)
            dinv[i, 128:256, 0:128] = -dot3(split(half_inv[4 * g + 2 * n + 1]), split(half_tmp[n]), NN)
        for n in range(2):
            i = 2 * (2 * g + n) + core
            copy(dinv.at[i], dinv.at[i], inv_send, inv_recv.at[g], mate).start()
        return 0

    lax.fori_loop(0, 4, invert, 0)

    copy(rhs.at[0:63], rhs.at[0:63], a_send, a_recv, mate).wait_recv()

    def offer(i, value):
        gbuf[i, :, xl] = value.reshape(2, 64, 96)
        copy(gbuf.at[i, :, xl], gbuf.at[i, :, xl], g_send.at[i], g_recv.at[i], peer).start()

    def factor_part(i, t):
        k, at = panel_place(i, 2 * t)
        return split(pan[k, pl.ds(at, 2)].reshape(128, 256))

    def own_out(i):
        half = rowbuf.at[y, i, 1 - core]
        copy(half, half, x_send, x_recv.at[i], mate).wait_recv()
        for k, offset in enumerate((1, -1)):
            copy(rowbuf.at[y, i], rowbuf.at[y, i], y_send.at[k, i], y_recv.at[k, i], y_at(offset)).start()

        @pl.when(same)
        def _():
            for k, offset in enumerate((1, -1)):
                copy(rowbuf.at[y, i], colbuf.at[z, i], z_send.at[k, i], z_recv.at[k, i], z_at(offset)).start()
            colbuf[z, i] = rowbuf[y, i]

        @pl.when(jnp.logical_not(same))
        def _():
            copy(rowbuf.at[y, i], colbuf.at[z, i], s_send.at[i], s_recv.at[i], swap).start()

    def swapped_out(i):
        @pl.when(jnp.logical_not(same))
        def _():
            copy(colbuf.at[z, i], colbuf.at[z, i], s_send.at[i], s_recv.at[i], swap).wait_recv()
            for k, offset in enumerate((1, -1)):
                copy(colbuf.at[z, i], colbuf.at[z, i], z_send.at[k, i], z_recv.at[k, i], z_at(offset)).start()

    def got(buf, send, recv, place, k, i):
        copy(buf.at[place, i], buf.at[place, i], send.at[k, i], recv.at[k, i], mate).wait_recv()

    def forward(i):
        odd = i % 2
        step = 1 - 2 * odd
        src = (y - step + 4) % 4
        got(rowbuf, y_send, y_recv, src, odd, i)
        copy(rowbuf.at[src, i], rowbuf.at[src, i], y_send.at[2, i], y_recv.at[2, i], y_at(step)).start()
        src = (z - step + 4) % 4
        got(colbuf, z_send, z_recv, src, odd, i)
        copy(colbuf.at[src, i], colbuf.at[src, i], z_send.at[2, i], z_recv.at[2, i], z_at(step)).start()

    def whole(buf, k, c):
        return jnp.concatenate([buf[k, 2 * c].reshape(192, 128), buf[k, 2 * c + 1].reshape(192, 128)], axis=1)

    def arrived(c):
        for odd in range(2):
            i = 2 * c + odd
            step = 1 - 2 * odd
            got(rowbuf, y_send, y_recv, (y + step + 4) % 4, 1 - odd, i)
            got(colbuf, z_send, z_recv, (z + step + 4) % 4, 1 - odd, i)
            got(rowbuf, y_send, y_recv, (y + 2) % 4, 2, i)
            got(colbuf, z_send, z_recv, (z + 2) % 4, 2, i)
        for k in range(4):
            cols[k * 192:k * 192 + 192] = whole(colbuf, k, c)
        for m in range(6):
            high, low = split(cols[128 * m:128 * m + 128].T)
            colh[:, 128 * m:128 * m + 128] = high
            coll[:, 128 * m:128 * m + 128] = low

    def product_rows(c, k):
        acc[k] = acc[k] + dot3(split(whole(rowbuf, k, c)), (colh[...], coll[...]), NN)

    def product(c):
        arrived(c)

        def part(k, _):
            product_rows(c, k)
            return 0

        lax.fori_loop(0, 4, part, 0)

    acc[...] = jnp.zeros_like(acc)
    for i in range(16):
        k, row = panel_place(i, 2 * i)
        piece = pan.at[k, row:row + 32 - 2 * i, core]
        pltpu.make_async_copy(piece, piece, pan_local.at[i]).wait()
        copy(piece, piece, pan_send.at[i], pan_recv.at[i], mate).wait_recv()
    offer(0, rhs[0:4].reshape(128, 96))

    def round_of(i, _):
        @pl.when(i % 4 == 0)
        def _():
            copy(dinv.at[0:2], dinv.at[0:2], inv_send, inv_recv.at[i // 4], mate).wait_recv()

        inverse = split(dinv[i])

        @pl.when(i > 0)
        def _():
            def later(u, _):
                k, at = panel_place(i - 1, 4 * u)
                part = split(pan[k, pl.ds(at, 4)].reshape(256, 256))
                term = dot3(part, (xh[...], xlow[...]), NN)
                rows = pl.ds(8 * u, 8)
                rhs[rows] = rhs[rows] - term.reshape(8, 32, 96)
                return 0

            lax.fori_loop((i + 1) // 2, 8, later, 0)
            own_out(i - 1)

        @pl.when(i > 1)
        def _():
            swapped_out(i - 2)

        @pl.when(i > 3)
        def _():
            forward(i - 4)

        @pl.when((i > 6) & (i % 2 == 1))
        def _():
            product((i - 7) // 2)

        other = gbuf.at[i, :, 1 - xl]
        copy(other, other, g_send.at[i], g_recv.at[i], peer).wait_recv()
        solved = dot3(inverse, split(gbuf[i].reshape(256, 96)), NN)
        high, low = split(solved)
        xh[...] = high
        xlow[...] = low

        @pl.when(i < 15)
        def _():
            term = dot3(factor_part(i, i + 1), (high, low), NN)
            offer(i + 1, rhs[pl.ds(4 * i + 4, 4)].reshape(128, 96) - term)

        xbuf[...] = solved.reshape(2, 128, 96)
        tx[i] = xbuf[1 - core].T
        copy(tx.at[i], rowbuf.at[y, i, core], x_send, x_recv.at[i], mate).start()
        rowbuf[y, i, core] = xbuf[core].T
        return 0

    lax.fori_loop(0, 16, round_of, 0)

    own_out(15)
    swapped_out(14)
    forward(12)
    forward(13)
    swapped_out(15)
    product(5)
    forward(14)
    product(6)
    forward(15)
    arrived(7)

    mine = pl.ds(pl.multiple_of(core * 384, 128), 384)
    theirs = pl.ds(pl.multiple_of((1 - core) * 384, 128), 384)
    order = ((y + 2) % 4, (y + 1) % 4, (y + 3) % 4, y)

    def trade(n):
        k = order[n]
        return copy(acc.at[k, :, theirs], exch.at[k], t_send.at[n], t_recv.at[n], mate)

    for n in range(4):
        product_rows(7, order[n])
        trade(n).start()

    def summed(n):
        trade(n).wait_recv()
        k = order[n]
        total[k] = acc[k, :, mine] + exch[k]

    summed(0)
    hops = []
    for at, offset in enumerate((1, -1)):
        hops.append(copy(total.at[order[0], 96 * at:96 * at + 96], relay.at[at],
                         e_send.at[at], e_recv.at[at], y_at(offset)))
        hops[-1].start()
    for n, offset in ((1, 1), (2, -1)):
        summed(n)
        hops.append(copy(total.at[order[n]], final.at[y], e_send.at[n + 1], e_recv.at[n + 1], y_at(offset)))
        hops[-1].start()
    for at, offset in enumerate((1, -1)):
        copy(relay.at[at], relay.at[at], e_send.at[at], e_recv.at[at], mate).wait_recv()
        src = (y - offset + 4) % 4
        hops.append(copy(relay.at[at], final.at[src, 96 * at:96 * at + 96],
                         e_send.at[4 + at], e_recv.at[4 + at], y_at(offset)))
        hops[-1].start()
    summed(3)
    final[y] = total[y]
    for n, offset in ((1, 1), (2, -1)):
        src = (y - offset + 4) % 4
        copy(final.at[src], final.at[src], e_send.at[n + 1], e_recv.at[n + 1], mate).wait_recv()
    src = (y + 2) % 4
    for at in range(2):
        piece = final.at[src, 96 * at:96 * at + 96]
        copy(piece, piece, e_send.at[4 + at], e_recv.at[4 + at], mate).wait_recv()
    window = pairs[:, pl.ds(pl.multiple_of((blk * 192) // 128 * 128, 128), 256)]
    across = jnp.where(blk % 2 == 1, window[:, 64:256], window[:, 0:192])
    line = lax.broadcasted_iota(jnp.int32, (192, 192), 0)
    lane = lax.broadcasted_iota(jnp.int32, (192, 192), 1)
    down = jnp.sum(jnp.where(line == lane, across, 0.0), axis=1, keepdims=True)
    for k in range(2):
        wide = pairs[:, pl.ds(pl.multiple_of(sub * 1536 + k * 768, 128), 768)]
        sums = jnp.concatenate([final[q, :, k * 192:k * 192 + 192] for q in range(4)], axis=1)
        out[:, k * 768:k * 768 + 768] = sums / (down + wide)
    for hop in hops:
        hop.wait_send()
    for n in range(4):
        trade(n).wait_send()

    def drain(i, _):
        piece = rowbuf.at[y, i]
        for k in range(3):
            copy(piece, piece, y_send.at[k, i], y_recv.at[k, i], mate).wait_send()
            copy(piece, piece, z_send.at[k, i], z_recv.at[k, i], mate).wait_send()

        @pl.when(jnp.logical_not(same))
        def _():
            copy(piece, piece, s_send.at[i], s_recv.at[i], swap).wait_send()

        return 0

    lax.fori_loop(0, 16, drain, 0)

    for i in range(16):
        k, row = panel_place(i, 2 * i)
        piece = pan.at[k, row:row + 32 - 2 * i, core]
        copy(piece, piece, pan_send.at[i], pan_recv.at[i], mate).wait_send()
        mine = gbuf.at[i, :, xl]
        copy(mine, mine, g_send.at[i], g_recv.at[i], peer).wait_send()
    for q in range(2):
        piece = blocks.at[0:6, q, :, :, :, 0:128 * (q + 1)]
        copy(piece, piece, diag_send.at[q], diag_recv.at[q, 0], mate).wait_send()
    copy(sb.at[0:63], sb.at[0:63], a_send, a_recv, mate).wait_send()
    copy(dinv.at[0:8], dinv.at[0:8], inv_send, inv_recv.at[0], mate).wait_send()
    copy(tx, tx, x_send, x_recv.at[0], mate).wait_send()


def amplitude_block(integrals, slots, factor, occ, slab, virt):
    dma = pltpu.SemaphoreType.DMA
    vmem = pl.BlockSpec(memory_space=pltpu.VMEM)
    smem = pl.BlockSpec(memory_space=pltpu.SMEM)
    return pl.pallas_call(
        fused_kernel,
        out_shape=jax.ShapeDtypeStruct((192, 1536), F32),
        in_specs=[vmem, vmem, pl.BlockSpec(memory_space=pl.ANY), smem, smem, vmem],
        out_specs=vmem,
        scratch_shapes=[
            pltpu.VMEM((8, 34, 2, 32, 256), F32),
            pltpu.VMEM((8, 2, 2, 2, 32, 256), F32),
            pltpu.VMEM((16, 128, 128), F32),
            pltpu.VMEM((4, 128, 128), F32),
            pltpu.VMEM((16, 256, 256), F32),
            pltpu.VMEM((64, 32, 96), F32),
            pltpu.VMEM((64, 32, 96), F32),
            pltpu.VMEM((16, 2, 2, 64, 96), F32),
            pltpu.VMEM((256, 96), BF16),
            pltpu.VMEM((256, 96), BF16),
            pltpu.VMEM((2, 128, 96), F32),
            pltpu.VMEM((16, 96, 128), F32),
            pltpu.VMEM((4, 16, 2, 96, 128), F32),
            pltpu.VMEM((4, 16, 2, 96, 128), F32),
            pltpu.VMEM((4, 192, 768), F32),
            pltpu.VMEM((768, 256), F32),
            pltpu.VMEM((256, 768), BF16),
            pltpu.VMEM((256, 768), BF16),
            pltpu.VMEM((1, 6144), F32),
            pltpu.VMEM((4, 192, 384), F32),
            pltpu.VMEM((4, 192, 384), F32),
            pltpu.VMEM((4, 192, 384), F32),
            pltpu.VMEM((2, 96, 384), F32),
            dma((16,)), dma((16,)), dma((16,)), dma((2,)), dma((2, 4)), dma, dma, dma, dma((4,)),
            dma((16,)), dma((16,)), dma, dma((16,)),
            dma((3, 16)), dma((3, 16)), dma((3, 16)), dma((3, 16)), dma((16,)), dma((16,)),
            dma((4,)), dma((4,)), dma((6,)), dma((6,)),
        ],
        compiler_params=pltpu.CompilerParams(
            collective_id=0, has_side_effects=True, vmem_limit_bytes=60 * 2**20),
    )(integrals, slots, factor, occ, slab, virt)


def shards(integrals, slot_order, factor_rows, occ_energy, slab_index, virt_energy):
    return amplitude_block(integrals[0, 0], slot_order[0], factor_rows[:, 0],
                           occ_energy, slab_index, virt_energy[None])


def solution(mesh):
    in_specs = (
        P("blk", "sub", None, None),
        P("blk", "sub", None),
        P(None, "sub", None, None),
        P(),
        P(),
        P(),
    )
    out_specs = P("blk", "sub")
    return jax.shard_map(shards, mesh=mesh, in_specs=in_specs, out_specs=out_specs, check_vma=False)
```

```python
import functools

import jax
import jax.numpy as jnp
from jax import lax
from jax.experimental import pallas as pl
from jax.experimental.pallas import tpu as pltpu
from jax.sharding import PartitionSpec as P

NOCC = 3
F32 = jnp.float32
BF16 = jnp.bfloat16
MESH = pl.DeviceIdType.MESH
NN = (((1,), (0,)), ((), ()))
NT = (((1,), (1,)), ((), ()))


def split(x):
    high = x.astype(BF16)
    return high, (x - high.astype(F32)).astype(BF16)


def dot3(a, b, dims):
    def one(p, q):
        return lax.dot_general(p, q, dims, preferred_element_type=F32)

    return one(a[0], b[0]) + (one(a[0], b[1]) + one(a[1], b[0]))


def copy(src, dst, send, recv, who):
    return pltpu.make_async_remote_copy(
        src_ref=src, dst_ref=dst, send_sem=send, recv_sem=recv,
        device_id=who, device_id_type=MESH)


def panel_place(i, r):
    if isinstance(i, int):
        return (i, r - 2 * i) if i < 8 else (15 - i, r + 2)
    return jnp.where(i < 8, i, 15 - i), jnp.where(i < 8, r - 2 * i, r + 2)


def fused_kernel(integrals, slots, factor, occ, slab_hbm, virt, out, slab, pan, blocks, half_inv, half_tmp, dinv, sb, rhs, known, gbuf,
                 xh, xlow, xbuf, tx, rowbuf, colbuf, acc, cols, colh, coll, pairs, exch, total, final, relay,
                 in_local, pan_local, pan_send, pan_recv, diag_send, diag_recv, a_send, a_recv,
                 inv_send, inv_recv, g_send, g_recv, x_send, x_recv,
                 y_send, y_recv, z_send, z_recv, s_send, s_recv, t_send, t_recv, e_send, e_recv):
    blk, sub = lax.axis_index("blk"), lax.axis_index("sub")
    hi = blk // 16
    xl, core = sub // 2, sub % 2
    x = 2 * hi + xl
    y, z = blk % 4, (blk // 4) % 4
    same = hi == xl
    mate = {"blk": blk, "sub": sub + 1 - 2 * core}
    peer = {"blk": blk, "sub": sub + 2 - 4 * xl}

    def beside(offset, to_core):
        other = (x + offset + 4) % 4
        return {"blk": blk + (other // 2 - hi) * 16, "sub": (other % 2) * 2 + to_core}

    def y_at(offset):
        return {"blk": blk - y + (y + offset + 4) % 4, "sub": sub}

    def z_at(offset):
        return {"blk": blk - 4 * z + 4 * ((z + offset + 4) % 4), "sub": sub}

    swap = {"blk": blk + (1 - 2 * hi) * 16, "sub": sub + (1 - 2 * xl) * 2}

    pltpu.make_async_copy(slab_hbm, slab, in_local).start()
    barrier = pltpu.get_barrier_semaphore()

    def greet(k, _):
        for c in range(2):
            pl.semaphore_signal(barrier, inc=1, device_id_type=MESH,
                                device_id={"blk": (blk + k) % 32, "sub": 2 * xl + c})
        return 0

    lax.fori_loop(1, 32, greet, 0)
    pl.semaphore_signal(barrier, inc=1, device_id=mate, device_id_type=MESH)
    for offset in (1, -1):
        for c in range(2):
            pl.semaphore_signal(barrier, inc=1, device_id=beside(offset, c), device_id_type=MESH)

    def slab_of(i, q):
        wide = 128 * (q + 1)
        return factor.at[2 * i + q, :, pl.ds(pl.multiple_of(256 * i, 256), wide)]

    def slab_place(j, q, at_core):
        return blocks.at[j, q, xl, at_core, :, 0:128 * (q + 1)]

    order = (0, 1, 4, 5, 2, 3, 6, 7)
    for j in order:
        for q in range(2):
            pltpu.make_async_copy(slab_of(2 * j + core, q), slab_place(j, q, core), diag_recv.at[q, j // 2]).start()

    onehot = (slots[...] == lax.broadcasted_iota(jnp.int32, (32, 32), 0)).astype(F32).astype(BF16)

    def pick(v):
        return lax.dot_general(onehot, v, NN, preferred_element_type=F32)

    for g in range(16):
        value = integrals[:, 384 * g:384 * g + 384]
        high = value.astype(BF16)
        rest = value - high.astype(F32)
        mid = rest.astype(BF16)
        low = (rest - mid.astype(F32)).astype(BF16)
        picked = pick(high) + (pick(mid) + pick(low))
        for k in range(4):
            sb[4 * g + k] = picked[:, 96 * k:96 * k + 96]

    pl.semaphore_wait(barrier, 67)

    for j in order:
        for q in range(2):
            for c in range(2):
                copy(slab_of(2 * j + c, q), slab_place(j, q, core), diag_send.at[q], diag_recv.at[q, j // 2],
                     beside(1 if j < 4 else -1, c)).start()
            copy(slab_of(2 * j + 1 - core, q), slab_place(j, q, core), diag_send.at[q], diag_recv.at[q, j // 2],
                 mate).start()

    def spread(k, _):
        to = (blk + k) % 32
        for c in range(2):
            copy(sb.at[2 * to + c], rhs.at[2 * blk + core], a_send, a_recv.at[blk // 2],
                 {"blk": to, "sub": 2 * xl + c}).start()
        return 0

    lax.fori_loop(1, 32, spread, 0)
    copy(sb.at[2 * blk + 1 - core], rhs.at[2 * blk + core], a_send, a_recv.at[blk // 2], mate).start()
    rhs[2 * blk + core] = sb[2 * blk + core]

    for i in range(16):
        k, row = panel_place(i, 2 * i)
        piece = factor.at[2 * i:32, :, 256 * i:256 * i + 256]
        place = pan.at[k, row:row + 32 - 2 * i, core]
        pltpu.make_async_copy(piece, place, pan_local.at[i]).start()
        copy(piece, place, pan_send.at[i], pan_recv.at[i], mate).start()

    pltpu.make_async_copy(slab_hbm, slab, in_local).wait()
    for t in range(3):
        pairs[:, 2048 * t:2048 * t + 2048] = occ[slab[0] * NOCC + t] - virt[...]

    row = lax.broadcasted_iota(jnp.int32, (128, 128), 0)
    col = lax.broadcasted_iota(jnp.int32, (128, 128), 1)

    def invert(turn, _):
        g = (turn % 2) * 2 + turn // 2
        for q in range(2):
            piece = blocks.at[pl.ds(2 * g, 2), q, :, :, :, 0:128 * (q + 1)]
            pltpu.make_async_copy(piece, piece, diag_recv.at[q, g]).wait()

        def block(n):
            q = n % 2
            return blocks[2 * g + n // 2, q, :, :, :, 128 * q:128 * q + 128].reshape(128, 128)

        for n in range(4):
            value = block(n)
            diag = jnp.where(row == col, value, 0.0)
            down = 1.0 / jnp.sum(diag, axis=1, keepdims=True)
            across = 1.0 / jnp.sum(diag, axis=0, keepdims=True)
            below = (row == col + 1) & (row % 2 == 1)
            half_inv[4 * g + n] = jnp.where(row == col, down, 0.0) - jnp.where(below, value * down * across, 0.0)
        size = 2
        while size < 128:
            below = (row // size == col // size + 1) & (row // (2 * size) == col // (2 * size))
            for n in range(4):
                part = jnp.where(below, block(n), 0.0)
                half_tmp[n] = dot3(split(part), split(half_inv[4 * g + n]), NN)
            for n in range(4):
                now = half_inv[4 * g + n]
                half_inv[4 * g + n] = now - dot3(split(now), split(half_tmp[n]), NN)
            size *= 2
        for n in range(2):
            lower = blocks[2 * g + n, 1, :, :, :, 0:128].reshape(128, 128)
            half_tmp[n] = dot3(split(lower), split(half_inv[4 * g + 2 * n]), NN)
        for n in range(2):
            i = 2 * (2 * g + n) + core
            dinv[i, 0:128, 0:128] = half_inv[4 * g + 2 * n]
            dinv[i, 128:256, 128:256] = half_inv[4 * g + 2 * n + 1]
            dinv[i, 0:128, 128:256] = jnp.zeros((128, 128), F32)
            dinv[i, 128:256, 0:128] = -dot3(split(half_inv[4 * g + 2 * n + 1]), split(half_tmp[n]), NN)
        for n in range(2):
            i = 2 * (2 * g + n) + core
            copy(dinv.at[i], dinv.at[i], inv_send, inv_recv.at[g], mate).start()
        return 0

    lax.fori_loop(0, 4, invert, 0)

    def offer(i, value):
        gbuf[i, :, xl] = value.reshape(2, 64, 96)
        copy(gbuf.at[i, :, xl], gbuf.at[i, :, xl], g_send.at[i], g_recv.at[i], peer).start()

    def right_side(i):
        for count, here in ((3, blk // 2 == i), (4, blk // 2 != i)):
            @pl.when(here)
            def _(count=count):
                piece = rhs.at[0:count]
                copy(piece, piece, a_send, a_recv.at[i], mate).wait_recv()

        return rhs[pl.ds(4 * i, 4)].reshape(128, 96)

    def factor_part(i, t):
        k, at = panel_place(i, 2 * t)
        return split(pan[k, pl.ds(at, 2)].reshape(128, 256))

    def own_out(i):
        half = rowbuf.at[y, i, 1 - core]
        copy(half, half, x_send, x_recv.at[i], mate).wait_recv()
        for k, offset in enumerate((1, -1)):
            copy(rowbuf.at[y, i], rowbuf.at[y, i], y_send.at[k, i], y_recv.at[k, i], y_at(offset)).start()

        @pl.when(same)
        def _():
            for k, offset in enumerate((1, -1)):
                copy(rowbuf.at[y, i], colbuf.at[z, i], z_send.at[k, i], z_recv.at[k, i], z_at(offset)).start()
            colbuf[z, i] = rowbuf[y, i]

        @pl.when(jnp.logical_not(same))
        def _():
            copy(rowbuf.at[y, i], colbuf.at[z, i], s_send.at[i], s_recv.at[i], swap).start()

    def swapped_out(i):
        @pl.when(jnp.logical_not(same))
        def _():
            copy(colbuf.at[z, i], colbuf.at[z, i], s_send.at[i], s_recv.at[i], swap).wait_recv()
            for k, offset in enumerate((1, -1)):
                copy(colbuf.at[z, i], colbuf.at[z, i], z_send.at[k, i], z_recv.at[k, i], z_at(offset)).start()

    def got(buf, send, recv, place, k, i):
        copy(buf.at[place, i], buf.at[place, i], send.at[k, i], recv.at[k, i], mate).wait_recv()

    def forward(buf, send, recv, me, at, i):
        odd = i % 2
        step = 1 - 2 * odd
        src = (me - step + 4) % 4
        got(buf, send, recv, src, odd, i)
        copy(buf.at[src, i], buf.at[src, i], send.at[2, i], recv.at[2, i], at(step)).start()

    def forward_y(i):
        forward(rowbuf, y_send, y_recv, y, y_at, i)

    def forward_z(i):
        forward(colbuf, z_send, z_recv, z, z_at, i)

    def whole(buf, k, c):
        return jnp.concatenate([buf[k, 2 * c].reshape(192, 128), buf[k, 2 * c + 1].reshape(192, 128)], axis=1)

    def arrived(c):
        for odd in range(2):
            i = 2 * c + odd
            step = 1 - 2 * odd
            got(rowbuf, y_send, y_recv, (y + step + 4) % 4, 1 - odd, i)
            got(colbuf, z_send, z_recv, (z + step + 4) % 4, 1 - odd, i)
            got(rowbuf, y_send, y_recv, (y + 2) % 4, 2, i)
            got(colbuf, z_send, z_recv, (z + 2) % 4, 2, i)
        for k in range(4):
            cols[k * 192:k * 192 + 192] = whole(colbuf, k, c)
        for m in range(6):
            high, low = split(cols[128 * m:128 * m + 128].T)
            colh[:, 128 * m:128 * m + 128] = high
            coll[:, 128 * m:128 * m + 128] = low

    def product_rows(c, k):
        acc[k] = acc[k] + dot3(split(whole(rowbuf, k, c)), (colh[...], coll[...]), NN)

    def product_half(c, half):
        def part(k, _):
            product_rows(c, k)
            return 0

        lax.fori_loop(2 * half, 2 * half + 2, part, 0)

    acc[...] = jnp.zeros_like(acc)
    for i in range(16):
        k, row = panel_place(i, 2 * i)
        piece = pan.at[k, row:row + 32 - 2 * i, core]
        pltpu.make_async_copy(piece, piece, pan_local.at[i]).wait()
        copy(piece, piece, pan_send.at[i], pan_recv.at[i], mate).wait_recv()
    known[...] = jnp.zeros_like(known)
    offer(0, right_side(0))

    def round_of(i, _):
        @pl.when(i % 4 == 0)
        def _():
            copy(dinv.at[0:2], dinv.at[0:2], inv_send, inv_recv.at[i // 4], mate).wait_recv()

        inverse = split(dinv[i])

        @pl.when(i > 0)
        def _():
            def later(u, _):
                k, at = panel_place(i - 1, 4 * u)
                part = split(pan[k, pl.ds(at, 4)].reshape(256, 256))
                term = dot3(part, (xh[...], xlow[...]), NN)
                rows = pl.ds(8 * u, 8)
                known[rows] = known[rows] + term.reshape(8, 32, 96)
                return 0

            lax.fori_loop((i + 1) // 2, 8, later, 0)
            own_out(i - 1)

        @pl.when(i > 1)
        def _():
            swapped_out(i - 2)

        @pl.when((i > 5) & (i % 2 == 0))
        def _():
            arrived((i - 6) // 2)

        @pl.when(i > 5)
        def _():
            product_half((i - 6) // 2, i % 2)

        @pl.when(i > 1)
        def _():
            forward_y(i - 2)

        @pl.when(i > 2)
        def _():
            forward_z(i - 3)

        @pl.when(i < 15)
        def _():
            rest = right_side(i + 1) - known[pl.ds(4 * i + 4, 4)].reshape(128, 96)
            rhs[pl.ds(4 * i + 4, 4)] = rest.reshape(4, 32, 96)

        other = gbuf.at[i, :, 1 - xl]
        copy(other, other, g_send.at[i], g_recv.at[i], peer).wait_recv()
        solved = dot3(inverse, split(gbuf[i].reshape(256, 96)), NN)
        high, low = split(solved)
        xh[...] = high
        xlow[...] = low

        @pl.when(i < 15)
        def _():
            term = dot3(factor_part(i, i + 1), (high, low), NN)
            offer(i + 1, rhs[pl.ds(4 * i + 4, 4)].reshape(128, 96) - term)

        xbuf[...] = solved.reshape(2, 128, 96)
        tx[i] = xbuf[1 - core].T
        copy(tx.at[i], rowbuf.at[y, i, core], x_send, x_recv.at[i], mate).start()
        rowbuf[y, i, core] = xbuf[core].T
        return 0

    lax.fori_loop(0, 16, round_of, 0)

    own_out(15)
    swapped_out(14)
    forward_y(14)
    forward_z(13)
    swapped_out(15)
    arrived(5)
    product_half(5, 0)
    forward_z(14)
    forward_y(15)
    product_half(5, 1)
    arrived(6)
    product_half(6, 0)
    forward_z(15)
    product_half(6, 1)
    arrived(7)

    mine = pl.ds(pl.multiple_of(core * 384, 128), 384)
    theirs = pl.ds(pl.multiple_of((1 - core) * 384, 128), 384)
    order = ((y + 2) % 4, (y + 1) % 4, (y + 3) % 4, y)

    def trade(n):
        k = order[n]
        return copy(acc.at[k, :, theirs], exch.at[k], t_send.at[n], t_recv.at[n], mate)

    for n in range(4):
        product_rows(7, order[n])
        trade(n).start()

    def summed(n):
        trade(n).wait_recv()
        k = order[n]
        total[k] = acc[k, :, mine] + exch[k]

    summed(0)
    hops = []
    for at, offset in enumerate((1, -1)):
        hops.append(copy(total.at[order[0], 96 * at:96 * at + 96], relay.at[at],
                         e_send.at[at], e_recv.at[at], y_at(offset)))
        hops[-1].start()
    for n, offset in ((1, 1), (2, -1)):
        summed(n)
        hops.append(copy(total.at[order[n]], final.at[y], e_send.at[n + 1], e_recv.at[n + 1], y_at(offset)))
        hops[-1].start()
    for at, offset in enumerate((1, -1)):
        copy(relay.at[at], relay.at[at], e_send.at[at], e_recv.at[at], mate).wait_recv()
        src = (y - offset + 4) % 4
        hops.append(copy(relay.at[at], final.at[src, 96 * at:96 * at + 96],
                         e_send.at[4 + at], e_recv.at[4 + at], y_at(offset)))
        hops[-1].start()
    summed(3)
    final[y] = total[y]
    for n, offset in ((1, 1), (2, -1)):
        src = (y - offset + 4) % 4
        copy(final.at[src], final.at[src], e_send.at[n + 1], e_recv.at[n + 1], mate).wait_recv()
    src = (y + 2) % 4
    for at in range(2):
        piece = final.at[src, 96 * at:96 * at + 96]
        copy(piece, piece, e_send.at[4 + at], e_recv.at[4 + at], mate).wait_recv()
    window = pairs[:, pl.ds(pl.multiple_of((blk * 192) // 128 * 128, 128), 256)]
    across = jnp.where(blk % 2 == 1, window[:, 64:256], window[:, 0:192])
    line = lax.broadcasted_iota(jnp.int32, (192, 192), 0)
    lane = lax.broadcasted_iota(jnp.int32, (192, 192), 1)
    down = jnp.sum(jnp.where(line == lane, across, 0.0), axis=1, keepdims=True)
    for k in range(2):
        wide = pairs[:, pl.ds(pl.multiple_of(sub * 1536 + k * 768, 128), 768)]
        sums = jnp.concatenate([final[q, :, k * 192:k * 192 + 192] for q in range(4)], axis=1)
        out[:, k * 768:k * 768 + 768] = sums / (down + wide)
    for hop in hops:
        hop.wait_send()
    for n in range(4):
        trade(n).wait_send()

    def drain(i, _):
        piece = rowbuf.at[y, i]
        for k in range(3):
            copy(piece, piece, y_send.at[k, i], y_recv.at[k, i], mate).wait_send()
            copy(piece, piece, z_send.at[k, i], z_recv.at[k, i], mate).wait_send()

        @pl.when(jnp.logical_not(same))
        def _():
            copy(piece, piece, s_send.at[i], s_recv.at[i], swap).wait_send()

        return 0

    lax.fori_loop(0, 16, drain, 0)

    for i in range(16):
        k, row = panel_place(i, 2 * i)
        piece = pan.at[k, row:row + 32 - 2 * i, core]
        copy(piece, piece, pan_send.at[i], pan_recv.at[i], mate).wait_send()
        mine = gbuf.at[i, :, xl]
        copy(mine, mine, g_send.at[i], g_recv.at[i], peer).wait_send()
    for q in range(2):
        piece = blocks.at[0:6, q, :, :, :, 0:128 * (q + 1)]
        copy(piece, piece, diag_send.at[q], diag_recv.at[q, 0], mate).wait_send()
    copy(sb.at[0:63], sb.at[0:63], a_send, a_recv.at[0], mate).wait_send()
    copy(dinv.at[0:8], dinv.at[0:8], inv_send, inv_recv.at[0], mate).wait_send()
    copy(tx, tx, x_send, x_recv.at[0], mate).wait_send()


def amplitude_block(integrals, slots, factor, occ, slab, virt):
    dma = pltpu.SemaphoreType.DMA
    vmem = pl.BlockSpec(memory_space=pltpu.VMEM)
    hbm = pl.BlockSpec(memory_space=pltpu.HBM)
    return pl.pallas_call(
        fused_kernel,
        out_shape=jax.ShapeDtypeStruct((192, 1536), F32),
        in_specs=[vmem, vmem, hbm, pl.BlockSpec(memory_space=pltpu.SMEM), hbm, vmem],
        out_specs=vmem,
        scratch_shapes=[
            pltpu.SMEM((1,), jnp.int32),
            pltpu.VMEM((8, 34, 2, 32, 256), F32),
            pltpu.VMEM((8, 2, 2, 2, 32, 256), F32),
            pltpu.VMEM((16, 128, 128), F32),
            pltpu.VMEM((4, 128, 128), F32),
            pltpu.VMEM((16, 256, 256), F32),
            pltpu.VMEM((64, 32, 96), F32),
            pltpu.VMEM((64, 32, 96), F32),
            pltpu.VMEM((64, 32, 96), F32),
            pltpu.VMEM((16, 2, 2, 64, 96), F32),
            pltpu.VMEM((256, 96), BF16),
            pltpu.VMEM((256, 96), BF16),
            pltpu.VMEM((2, 128, 96), F32),
            pltpu.VMEM((16, 96, 128), F32),
            pltpu.VMEM((4, 16, 2, 96, 128), F32),
            pltpu.VMEM((4, 16, 2, 96, 128), F32),
            pltpu.VMEM((4, 192, 768), F32),
            pltpu.VMEM((768, 256), F32),
            pltpu.VMEM((256, 768), BF16),
            pltpu.VMEM((256, 768), BF16),
            pltpu.VMEM((1, 6144), F32),
            pltpu.VMEM((4, 192, 384), F32),
            pltpu.VMEM((4, 192, 384), F32),
            pltpu.VMEM((4, 192, 384), F32),
            pltpu.VMEM((2, 96, 384), F32),
            dma, dma((16,)), dma((16,)), dma((16,)), dma((2,)), dma((2, 4)), dma, dma((16,)), dma, dma((4,)),
            dma((16,)), dma((16,)), dma, dma((16,)),
            dma((3, 16)), dma((3, 16)), dma((3, 16)), dma((3, 16)), dma((16,)), dma((16,)),
            dma((4,)), dma((4,)), dma((6,)), dma((6,)),
        ],
        compiler_params=pltpu.CompilerParams(
            collective_id=0, has_side_effects=True, vmem_limit_bytes=52 * 2**20),
    )(integrals, slots, factor, occ, slab, virt)


def shards(integrals, slot_order, factor_rows, occ_energy, slab_index, virt_energy):
    return amplitude_block(integrals[0, 0], slot_order[0], factor_rows[:, 0],
                           occ_energy, slab_index, virt_energy[None])


def solution(mesh):
    in_specs = (
        P("blk", "sub", None, None),
        P("blk", "sub", None),
        P(None, "sub", None, None),
        P(),
        P(),
        P(),
    )
    out_specs = P("blk", "sub")
    return jax.shard_map(shards, mesh=mesh, in_specs=in_specs, out_specs=out_specs, check_vma=False)
```

```python
import functools

import jax
import jax.numpy as jnp
from jax import lax
from jax.experimental import pallas as pl
from jax.experimental.pallas import tpu as pltpu
from jax.sharding import PartitionSpec as P

NOCC = 3
F32 = jnp.float32
BF16 = jnp.bfloat16
MESH = pl.DeviceIdType.MESH
NN = (((1,), (0,)), ((), ()))
NT = (((1,), (1,)), ((), ()))


def split(x):
    high = x.astype(BF16)
    return high, (x - high.astype(F32)).astype(BF16)


def dot3(a, b, dims):
    def one(p, q):
        return lax.dot_general(p, q, dims, preferred_element_type=F32)

    return one(a[0], b[0]) + (one(a[0], b[1]) + one(a[1], b[0]))


def copy(src, dst, send, recv, who):
    return pltpu.make_async_remote_copy(
        src_ref=src, dst_ref=dst, send_sem=send, recv_sem=recv,
        device_id=who, device_id_type=MESH)


def panel_place(i, r):
    if isinstance(i, int):
        return (i, r - 2 * i) if i < 8 else (15 - i, r + 2)
    return jnp.where(i < 8, i, 15 - i), jnp.where(i < 8, r - 2 * i, r + 2)


def fused_kernel(integrals, slots, factor, occ, slab_hbm, virt, out, slab, pan, blocks, half_inv, half_tmp, dinv, sb, rhs, known, near, both, gbuf,
                 xh, xlow, xbuf, tx, rowbuf, colbuf, acc, cols, colh, coll, pairs, exch, total, final, relay,
                 in_local, pan_local, pan_send, pan_recv, diag_send, diag_recv, a_send, a_recv,
                 inv_send, inv_recv, n_send, n_recv, m_send, m_recv, g_send, g_recv, x_send, x_recv,
                 y_send, y_recv, z_send, z_recv, s_send, s_recv, t_send, t_recv, e_send, e_recv):
    blk, sub = lax.axis_index("blk"), lax.axis_index("sub")
    hi = blk // 16
    xl, core = sub // 2, sub % 2
    x = 2 * hi + xl
    y, z = blk % 4, (blk // 4) % 4
    same = hi == xl
    mate = {"blk": blk, "sub": sub + 1 - 2 * core}
    peer = {"blk": blk, "sub": sub + 2 - 4 * xl}

    def beside(offset, to_core):
        other = (x + offset + 4) % 4
        return {"blk": blk + (other // 2 - hi) * 16, "sub": (other % 2) * 2 + to_core}

    def y_at(offset):
        return {"blk": blk - y + (y + offset + 4) % 4, "sub": sub}

    def z_at(offset):
        return {"blk": blk - 4 * z + 4 * ((z + offset + 4) % 4), "sub": sub}

    swap = {"blk": blk + (1 - 2 * hi) * 16, "sub": sub + (1 - 2 * xl) * 2}

    pltpu.make_async_copy(slab_hbm, slab, in_local).start()
    barrier = pltpu.get_barrier_semaphore()

    def greet(k, _):
        for c in range(2):
            pl.semaphore_signal(barrier, inc=1, device_id_type=MESH,
                                device_id={"blk": (blk + k) % 32, "sub": 2 * xl + c})
        return 0

    lax.fori_loop(1, 32, greet, 0)
    pl.semaphore_signal(barrier, inc=1, device_id=mate, device_id_type=MESH)
    for offset in (1, -1):
        for c in range(2):
            pl.semaphore_signal(barrier, inc=1, device_id=beside(offset, c), device_id_type=MESH)

    def slab_of(i, q):
        wide = 128 * (q + 1)
        return factor.at[2 * i + q, :, pl.ds(pl.multiple_of(256 * i, 256), wide)]

    def slab_place(j, q, at_core):
        return blocks.at[j, q, xl, at_core, :, 0:128 * (q + 1)]

    order = (0, 1, 4, 5, 2, 3, 6, 7)
    for j in order:
        for q in range(2):
            pltpu.make_async_copy(slab_of(2 * j + core, q), slab_place(j, q, core), diag_recv.at[q, j // 2]).start()

    onehot = (slots[...] == lax.broadcasted_iota(jnp.int32, (32, 32), 0)).astype(F32).astype(BF16)

    def pick(v):
        return lax.dot_general(onehot, v, NN, preferred_element_type=F32)

    for g in range(16):
        value = integrals[:, 384 * g:384 * g + 384]
        high = value.astype(BF16)
        rest = value - high.astype(F32)
        mid = rest.astype(BF16)
        low = (rest - mid.astype(F32)).astype(BF16)
        picked = pick(high) + (pick(mid) + pick(low))
        for k in range(4):
            sb[4 * g + k] = picked[:, 96 * k:96 * k + 96]

    pl.semaphore_wait(barrier, 67)

    for j in order:
        for q in range(2):
            for c in range(2):
                copy(slab_of(2 * j + c, q), slab_place(j, q, core), diag_send.at[q], diag_recv.at[q, j // 2],
                     beside(1 if j < 4 else -1, c)).start()
            copy(slab_of(2 * j + 1 - core, q), slab_place(j, q, core), diag_send.at[q], diag_recv.at[q, j // 2],
                 mate).start()

    for p in range(8):
        copy(factor.at[4 * p + 2:4 * p + 4, :, 512 * p:512 * p + 256], near.at[p, :, core],
             n_send, n_recv, beside(1 if p < 4 else -1, core)).start()

    def spread(k, _):
        to = (blk + k) % 32
        for c in range(2):
            copy(sb.at[2 * to + c], rhs.at[2 * blk + core], a_send, a_recv.at[blk // 2],
                 {"blk": to, "sub": 2 * xl + c}).start()
        return 0

    lax.fori_loop(1, 32, spread, 0)
    copy(sb.at[2 * blk + 1 - core], rhs.at[2 * blk + core], a_send, a_recv.at[blk // 2], mate).start()
    rhs[2 * blk + core] = sb[2 * blk + core]

    for i in range(16):
        k, row = panel_place(i, 2 * i)
        piece = factor.at[2 * i:32, :, 256 * i:256 * i + 256]
        place = pan.at[k, row:row + 32 - 2 * i, core]
        pltpu.make_async_copy(piece, place, pan_local).start()
        copy(piece, place, pan_send, pan_recv, mate).start()

    pltpu.make_async_copy(slab_hbm, slab, in_local).wait()
    for t in range(3):
        pairs[:, 2048 * t:2048 * t + 2048] = occ[slab[0] * NOCC + t] - virt[...]

    row = lax.broadcasted_iota(jnp.int32, (128, 128), 0)
    col = lax.broadcasted_iota(jnp.int32, (128, 128), 1)

    def invert(turn, _):
        g = (turn % 2) * 2 + turn // 2
        for q in range(2):
            piece = blocks.at[pl.ds(2 * g, 2), q, :, :, :, 0:128 * (q + 1)]
            pltpu.make_async_copy(piece, piece, diag_recv.at[q, g]).wait()

        def block(n):
            q = n % 2
            return blocks[2 * g + n // 2, q, :, :, :, 128 * q:128 * q + 128].reshape(128, 128)

        for n in range(4):
            value = block(n)
            diag = jnp.where(row == col, value, 0.0)
            down = 1.0 / jnp.sum(diag, axis=1, keepdims=True)
            across = 1.0 / jnp.sum(diag, axis=0, keepdims=True)
            below = (row == col + 1) & (row % 2 == 1)
            half_inv[4 * g + n] = jnp.where(row == col, down, 0.0) - jnp.where(below, value * down * across, 0.0)
        size = 2
        while size < 128:
            below = (row // size == col // size + 1) & (row // (2 * size) == col // (2 * size))
            for n in range(4):
                part = jnp.where(below, block(n), 0.0)
                half_tmp[n] = dot3(split(part), split(half_inv[4 * g + n]), NN)
            for n in range(4):
                now = half_inv[4 * g + n]
                half_inv[4 * g + n] = now - dot3(split(now), split(half_tmp[n]), NN)
            size *= 2
        for n in range(2):
            lower = blocks[2 * g + n, 1, :, :, :, 0:128].reshape(128, 128)
            half_tmp[n] = dot3(split(lower), split(half_inv[4 * g + 2 * n]), NN)
        for n in range(2):
            i = 2 * (2 * g + n) + core
            dinv[i, 0:128, 0:128] = half_inv[4 * g + 2 * n]
            dinv[i, 128:256, 128:256] = half_inv[4 * g + 2 * n + 1]
            dinv[i, 0:128, 128:256] = jnp.zeros((128, 128), F32)
            dinv[i, 128:256, 0:128] = -dot3(split(half_inv[4 * g + 2 * n + 1]), split(half_tmp[n]), NN)
        for n in range(2):
            i = 2 * (2 * g + n) + core
            copy(dinv.at[i], dinv.at[i], inv_send, inv_recv.at[g], mate).start()
        return 0

    lax.fori_loop(0, 4, invert, 0)

    def offer(i, value):
        gbuf[i, :, xl] = value.reshape(2, 64, 96)
        copy(gbuf.at[i, :, xl], gbuf.at[i, :, xl], g_send, g_recv.at[i], peer).start()

    def right_side(i):
        for count, here in ((3, blk // 2 == i), (4, blk // 2 != i)):
            @pl.when(here)
            def _(count=count):
                piece = rhs.at[0:count]
                copy(piece, piece, a_send, a_recv.at[i], mate).wait_recv()

        return rhs[pl.ds(4 * i, 4)].reshape(128, 96)

    def factor_rows(i, t, count):
        k, at = panel_place(i, 2 * t)
        return split(pan[k, pl.ds(at, 2 * count)].reshape(128 * count, 256))

    def times_solved(part, which):
        return dot3(part, (xh[which], xlow[which]), NN)

    def learn(u, i, which):
        rows = pl.ds(8 * u, 8)
        known[rows] = known[rows] + times_solved(factor_rows(i, 2 * u, 2), which).reshape(8, 32, 96)

    def own_out(i):
        half = rowbuf.at[y, i, 1 - core]
        copy(half, half, x_send, x_recv.at[i], mate).wait_recv()
        for k, offset in enumerate((1, -1)):
            copy(rowbuf.at[y, i], rowbuf.at[y, i], y_send, y_recv.at[k, i], y_at(offset)).start()

        @pl.when(same)
        def _():
            for k, offset in enumerate((1, -1)):
                copy(rowbuf.at[y, i], colbuf.at[z, i], z_send, z_recv.at[k, i], z_at(offset)).start()
            colbuf[z, i] = rowbuf[y, i]

        @pl.when(jnp.logical_not(same))
        def _():
            copy(rowbuf.at[y, i], colbuf.at[z, i], s_send, s_recv.at[i], swap).start()

    def swapped_out(i):
        @pl.when(jnp.logical_not(same))
        def _():
            copy(colbuf.at[z, i], colbuf.at[z, i], s_send, s_recv.at[i], swap).wait_recv()
            for k, offset in enumerate((1, -1)):
                copy(colbuf.at[z, i], colbuf.at[z, i], z_send, z_recv.at[k, i], z_at(offset)).start()

    def got(buf, send, recv, place, k, i):
        copy(buf.at[place, i], buf.at[place, i], send, recv.at[k, i], mate).wait_recv()

    def forward(buf, send, recv, me, at, i):
        odd = i % 2
        step = 1 - 2 * odd
        src = (me - step + 4) % 4
        got(buf, send, recv, src, odd, i)
        copy(buf.at[src, i], buf.at[src, i], send, recv.at[2, i], at(step)).start()

    def forward_y(i):
        forward(rowbuf, y_send, y_recv, y, y_at, i)

    def forward_z(i):
        forward(colbuf, z_send, z_recv, z, z_at, i)

    def whole(buf, k, c):
        return jnp.concatenate([buf[k, 2 * c].reshape(192, 128), buf[k, 2 * c + 1].reshape(192, 128)], axis=1)

    def arrived(c):
        for odd in range(2):
            i = 2 * c + odd
            step = 1 - 2 * odd
            got(rowbuf, y_send, y_recv, (y + step + 4) % 4, 1 - odd, i)
            got(colbuf, z_send, z_recv, (z + step + 4) % 4, 1 - odd, i)
            got(rowbuf, y_send, y_recv, (y + 2) % 4, 2, i)
            got(colbuf, z_send, z_recv, (z + 2) % 4, 2, i)
        for k in range(4):
            cols[k * 192:k * 192 + 192] = whole(colbuf, k, c)
        for m in range(6):
            high, low = split(cols[128 * m:128 * m + 128].T)
            colh[:, 128 * m:128 * m + 128] = high
            coll[:, 128 * m:128 * m + 128] = low

    def product_rows(c, k):
        acc[k] = acc[k] + dot3(split(whole(rowbuf, k, c)), (colh[...], coll[...]), NN)

    def product_half(c, half):
        def part(k, _):
            product_rows(c, k)
            return 0

        lax.fori_loop(2 * half, 2 * half + 2, part, 0)

    acc[...] = jnp.zeros_like(acc)
    piece = pan.at[:, :, core]
    pltpu.make_async_copy(piece, piece, pan_local).wait()
    copy(piece, piece, pan_send, pan_recv, mate).wait_recv()
    piece = near.at[:, :, core]
    copy(piece, piece, n_send, n_recv, mate).wait_recv()
    copy(piece, piece, m_send, m_recv, mate).start()
    known[...] = jnp.zeros_like(known)
    offer(0, right_side(0))
    offer(1, right_side(1))

    def incoming(i):
        other = gbuf.at[i, :, 1 - xl]
        copy(other, other, g_send, g_recv.at[i], peer).wait_recv()

    def solved_round(i, which, value):
        solved = dot3(split(dinv[i]), split(value.reshape(256, 96)), NN)
        high, low = split(solved)
        xh[which] = high
        xlow[which] = low
        xbuf[which] = solved.reshape(2, 128, 96)

    def spread_round(i, which):
        tx[i] = xbuf[which, 1 - core].T
        copy(tx.at[i], rowbuf.at[y, i, core], x_send, x_recv.at[i], mate).start()
        rowbuf[y, i, core] = xbuf[which, core].T

    def pair_of(p, _):
        a = 2 * p
        b = a + 1

        @pl.when(p % 2 == 0)
        def _():
            copy(dinv.at[0:2], dinv.at[0:2], inv_send, inv_recv.at[p // 2], mate).wait_recv()

        @pl.when(p == 0)
        def _():
            other = near.at[:, :, 1 - core]
            copy(other, other, m_send, m_recv, mate).wait_recv()

        @pl.when(p > 0)
        def _():
            own_out(a - 1)

            def later(u, _):
                learn(u, a - 2, 0)
                learn(u, a - 1, 1)
                return 0

            lax.fori_loop(p + 1, 8, later, 0)

        @pl.when(p > 2)
        def _():
            arrived(p - 3)
            product_half(p - 3, 0)
            product_half(p - 3, 1)

        @pl.when(p > 0)
        def _():
            forward_y(a - 2)

        @pl.when(p > 1)
        def _():
            forward_z(a - 4)
            forward_z(a - 3)

        incoming(a)
        solved_round(a, 0, gbuf[a])
        both[:, xl] = gbuf[b, :, xl] - times_solved(factor_rows(a, b, 1), 0).reshape(2, 64, 96)
        far = times_solved(split(near[p].reshape(128, 256)), 0).reshape(2, 64, 96)
        spread_round(a, 0)
        incoming(b)
        both[:, 1 - xl] = gbuf[b, :, 1 - xl] - far
        solved_round(b, 1, both[...])

        @pl.when(p < 7)
        def _():
            learn(p + 1, a, 0)
            for c in range(2):
                term = times_solved(factor_rows(b, a + 2 + c, 1), 1)
                rows = pl.ds(4 * (a + 2 + c), 4)
                offer(a + 2 + c, right_side(a + 2 + c) - known[rows].reshape(128, 96) - term)

        spread_round(b, 1)
        own_out(a)

        @pl.when(p > 0)
        def _():
            swapped_out(a - 2)
            swapped_out(a - 1)
            forward_y(a - 1)

        return 0

    lax.fori_loop(0, 8, pair_of, 0)

    own_out(15)
    forward_z(12)
    forward_z(13)
    swapped_out(14)
    forward_y(14)
    arrived(5)
    product_half(5, 0)
    swapped_out(15)
    forward_y(15)
    product_half(5, 1)
    forward_z(14)
    arrived(6)
    product_half(6, 0)
    forward_z(15)
    product_half(6, 1)
    arrived(7)

    mine = pl.ds(pl.multiple_of(core * 384, 128), 384)
    theirs = pl.ds(pl.multiple_of((1 - core) * 384, 128), 384)
    order = ((y + 2) % 4, (y + 1) % 4, (y + 3) % 4, y)

    def trade(n):
        k = order[n]
        return copy(acc.at[k, :, theirs], exch.at[k], t_send.at[n], t_recv.at[n], mate)

    for n in range(4):
        product_rows(7, order[n])
        trade(n).start()

    def summed(n):
        trade(n).wait_recv()
        k = order[n]
        total[k] = acc[k, :, mine] + exch[k]

    summed(0)
    hops = []
    for at, offset in enumerate((1, -1)):
        hops.append(copy(total.at[order[0], 96 * at:96 * at + 96], relay.at[at],
                         e_send.at[at], e_recv.at[at], y_at(offset)))
        hops[-1].start()
    for n, offset in ((1, 1), (2, -1)):
        summed(n)
        hops.append(copy(total.at[order[n]], final.at[y], e_send.at[n + 1], e_recv.at[n + 1], y_at(offset)))
        hops[-1].start()
    for at, offset in enumerate((1, -1)):
        copy(relay.at[at], relay.at[at], e_send.at[at], e_recv.at[at], mate).wait_recv()
        src = (y - offset + 4) % 4
        hops.append(copy(relay.at[at], final.at[src, 96 * at:96 * at + 96],
                         e_send.at[4 + at], e_recv.at[4 + at], y_at(offset)))
        hops[-1].start()
    summed(3)
    final[y] = total[y]
    for n, offset in ((1, 1), (2, -1)):
        src = (y - offset + 4) % 4
        copy(final.at[src], final.at[src], e_send.at[n + 1], e_recv.at[n + 1], mate).wait_recv()
    src = (y + 2) % 4
    for at in range(2):
        piece = final.at[src, 96 * at:96 * at + 96]
        copy(piece, piece, e_send.at[4 + at], e_recv.at[4 + at], mate).wait_recv()
    window = pairs[:, pl.ds(pl.multiple_of((blk * 192) // 128 * 128, 128), 256)]
    across = jnp.where(blk % 2 == 1, window[:, 64:256], window[:, 0:192])
    line = lax.broadcasted_iota(jnp.int32, (192, 192), 0)
    lane = lax.broadcasted_iota(jnp.int32, (192, 192), 1)
    down = jnp.sum(jnp.where(line == lane, across, 0.0), axis=1, keepdims=True)
    for k in range(2):
        wide = pairs[:, pl.ds(pl.multiple_of(sub * 1536 + k * 768, 128), 768)]
        sums = jnp.concatenate([final[q, :, k * 192:k * 192 + 192] for q in range(4)], axis=1)
        out[:, k * 768:k * 768 + 768] = sums / (down + wide)
    for hop in hops:
        hop.wait_send()
    for n in range(4):
        trade(n).wait_send()

    piece = rowbuf.at[0:3]
    copy(piece, piece, y_send, y_recv.at[0, 0], mate).wait_send()
    copy(piece, piece, z_send, z_recv.at[0, 0], mate).wait_send()

    @pl.when(jnp.logical_not(same))
    def _():
        copy(rowbuf.at[0], rowbuf.at[0], s_send, s_recv.at[0], swap).wait_send()

    piece = pan.at[:, :, core]
    copy(piece, piece, pan_send, pan_recv, mate).wait_send()
    piece = gbuf.at[:, :, xl]
    copy(piece, piece, g_send, g_recv.at[0], peer).wait_send()
    piece = near.at[:, :, core]
    copy(piece, piece, n_send, n_recv, mate).wait_send()
    copy(piece, piece, m_send, m_recv, mate).wait_send()
    for q in range(2):
        piece = blocks.at[0:6, q, :, :, :, 0:128 * (q + 1)]
        copy(piece, piece, diag_send.at[q], diag_recv.at[q, 0], mate).wait_send()
    copy(sb.at[0:63], sb.at[0:63], a_send, a_recv.at[0], mate).wait_send()
    copy(dinv.at[0:8], dinv.at[0:8], inv_send, inv_recv.at[0], mate).wait_send()
    copy(tx, tx, x_send, x_recv.at[0], mate).wait_send()


def amplitude_block(integrals, slots, factor, occ, slab, virt):
    dma = pltpu.SemaphoreType.DMA
    vmem = pl.BlockSpec(memory_space=pltpu.VMEM)
    hbm = pl.BlockSpec(memory_space=pltpu.HBM)
    return pl.pallas_call(
        fused_kernel,
        out_shape=jax.ShapeDtypeStruct((192, 1536), F32),
        in_specs=[vmem, vmem, hbm, pl.BlockSpec(memory_space=pltpu.SMEM), hbm, vmem],
        out_specs=vmem,
        scratch_shapes=[
            pltpu.SMEM((1,), jnp.int32),
            pltpu.VMEM((8, 34, 2, 32, 256), F32),
            pltpu.VMEM((8, 2, 2, 2, 32, 256), F32),
            pltpu.VMEM((16, 128, 128), F32),
            pltpu.VMEM((4, 128, 128), F32),
            pltpu.VMEM((16, 256, 256), F32),
            pltpu.VMEM((64, 32, 96), F32),
            pltpu.VMEM((64, 32, 96), F32),
            pltpu.VMEM((64, 32, 96), F32),
            pltpu.VMEM((8, 2, 2, 32, 256), F32),
            pltpu.VMEM((2, 2, 64, 96), F32),
            pltpu.VMEM((16, 2, 2, 64, 96), F32),
            pltpu.VMEM((2, 256, 96), BF16),
            pltpu.VMEM((2, 256, 96), BF16),
            pltpu.VMEM((2, 2, 128, 96), F32),
            pltpu.VMEM((16, 96, 128), F32),
            pltpu.VMEM((4, 16, 2, 96, 128), F32),
            pltpu.VMEM((4, 16, 2, 96, 128), F32),
            pltpu.VMEM((4, 192, 768), F32),
            pltpu.VMEM((768, 256), F32),
            pltpu.VMEM((256, 768), BF16),
            pltpu.VMEM((256, 768), BF16),
            pltpu.VMEM((1, 6144), F32),
            pltpu.VMEM((4, 192, 384), F32),
            pltpu.VMEM((4, 192, 384), F32),
            pltpu.VMEM((4, 192, 384), F32),
            pltpu.VMEM((2, 96, 384), F32),
            dma, dma, dma, dma, dma((2,)), dma((2, 4)), dma, dma((16,)), dma, dma((4,)),
            dma, dma, dma, dma, dma, dma((16,)), dma, dma((16,)),
            dma, dma((3, 16)), dma, dma((3, 16)), dma, dma((16,)),
            dma((4,)), dma((4,)), dma((6,)), dma((6,)),
        ],
        compiler_params=pltpu.CompilerParams(
            collective_id=0, has_side_effects=True, vmem_limit_bytes=52 * 2**20),
    )(integrals, slots, factor, occ, slab, virt)


def shards(integrals, slot_order, factor_rows, occ_energy, slab_index, virt_energy):
    return amplitude_block(integrals[0, 0], slot_order[0], factor_rows[:, 0],
                           occ_energy, slab_index, virt_energy[None])


def solution(mesh):
    in_specs = (
        P("blk", "sub", None, None),
        P("blk", "sub", None),
        P(None, "sub", None, None),
        P(),
        P(),
        P(),
    )
    out_specs = P("blk", "sub")
    return jax.shard_map(shards, mesh=mesh, in_specs=in_specs, out_specs=out_specs, check_vma=False)
```

```python
import functools

import jax
import jax.numpy as jnp
from jax import lax
from jax.experimental import pallas as pl
from jax.experimental.pallas import tpu as pltpu
from jax.sharding import PartitionSpec as P

NOCC = 3
F32 = jnp.float32
BF16 = jnp.bfloat16
MESH = pl.DeviceIdType.MESH
NN = (((1,), (0,)), ((), ()))
NT = (((1,), (1,)), ((), ()))


def split(x):
    high = x.astype(BF16)
    return high, (x - high.astype(F32)).astype(BF16)


def dot3(a, b, dims):
    def one(p, q):
        return lax.dot_general(p, q, dims, preferred_element_type=F32)

    return one(a[0], b[0]) + (one(a[0], b[1]) + one(a[1], b[0]))


def copy(src, dst, send, recv, who):
    return pltpu.make_async_remote_copy(
        src_ref=src, dst_ref=dst, send_sem=send, recv_sem=recv,
        device_id=who, device_id_type=MESH)


def panel_place(i, r):
    if isinstance(i, int):
        return (i, r - 2 * i) if i < 8 else (15 - i, r + 2)
    return jnp.where(i < 8, i, 15 - i), jnp.where(i < 8, r - 2 * i, r + 2)


def fused_kernel(integrals, slots, factor, occ, slab_hbm, virt, out, slab, pan, blocks, half_inv, half_tmp, dinv, sb, rhs, known, gbuf,
                 xh, xlow, xbuf, tx, rowbuf, colbuf, acc, cols, colh, coll, pairs, exch, total, final, relay,
                 in_local, pan_send, pan_recv, diag_send, diag_recv, a_send, a_recv,
                 inv_send, inv_recv, g_send, g_recv, x_send, x_recv,
                 y_send, y_recv, z_send, z_recv, s_send, s_recv, t_send, t_recv, e_send, e_recv):
    blk, sub = lax.axis_index("blk"), lax.axis_index("sub")
    hi = blk // 16
    xl, core = sub // 2, sub % 2
    x = 2 * hi + xl
    y, z = blk % 4, (blk // 4) % 4
    same = hi == xl
    mate = {"blk": blk, "sub": sub + 1 - 2 * core}
    peer = {"blk": blk, "sub": sub + 2 - 4 * xl}

    def beside(offset, to_core):
        other = (x + offset + 4) % 4
        return {"blk": blk + (other // 2 - hi) * 16, "sub": (other % 2) * 2 + to_core}

    def y_at(offset):
        return {"blk": blk - y + (y + offset + 4) % 4, "sub": sub}

    def z_at(offset):
        return {"blk": blk - 4 * z + 4 * ((z + offset + 4) % 4), "sub": sub}

    swap = {"blk": blk + (1 - 2 * hi) * 16, "sub": sub + (1 - 2 * xl) * 2}

    pltpu.make_async_copy(slab_hbm, slab, in_local).start()
    barrier = pltpu.get_barrier_semaphore()

    def greet(k, _):
        for c in range(2):
            pl.semaphore_signal(barrier, inc=1, device_id_type=MESH,
                                device_id={"blk": (blk + k) % 32, "sub": 2 * xl + c})
        return 0

    lax.fori_loop(1, 32, greet, 0)
    pl.semaphore_signal(barrier, inc=1, device_id=mate, device_id_type=MESH)
    for offset in (1, -1):
        for c in range(2):
            pl.semaphore_signal(barrier, inc=1, device_id=beside(offset, c), device_id_type=MESH)

    def slab_of(i, q):
        wide = 128 * (q + 1)
        return factor.at[2 * i + q, :, pl.ds(pl.multiple_of(256 * i, 256), wide)]

    def slab_place(j, q, at_core):
        return blocks.at[j, q, xl, at_core, :, 0:128 * (q + 1)]

    order = (0, 1, 4, 5, 2, 3, 6, 7)
    for j in order:
        for q in range(2):
            pltpu.make_async_copy(slab_of(2 * j + core, q), slab_place(j, q, core), diag_recv.at[q, j // 2]).start()

    onehot = (slots[...] == lax.broadcasted_iota(jnp.int32, (32, 32), 0)).astype(F32).astype(BF16)

    def pick(v):
        return lax.dot_general(onehot, v, NN, preferred_element_type=F32)

    for g in range(16):
        value = integrals[:, 384 * g:384 * g + 384]
        high = value.astype(BF16)
        rest = value - high.astype(F32)
        mid = rest.astype(BF16)
        low = (rest - mid.astype(F32)).astype(BF16)
        picked = pick(high) + (pick(mid) + pick(low))
        for k in range(4):
            sb[4 * g + k] = picked[:, 96 * k:96 * k + 96]

    pl.semaphore_wait(barrier, 67)

    for j in order:
        for q in range(2):
            for c in range(2):
                copy(slab_of(2 * j + c, q), slab_place(j, q, core), diag_send.at[q], diag_recv.at[q, j // 2],
                     beside(1 if j < 4 else -1, c)).start()
            copy(slab_of(2 * j + 1 - core, q), slab_place(j, q, core), diag_send.at[q], diag_recv.at[q, j // 2],
                 mate).start()

    def panels(first, last):
        for i in range(first, last):
            k, row = panel_place(i, 2 * i + 2)
            piece = factor.at[2 * i + 2:32, :, 256 * i:256 * i + 256]
            place = pan.at[k, row:row + 30 - 2 * i, core]
            group = (i > 1) + (i > 3) + (i > 7)
            pltpu.make_async_copy(piece, place, pan_recv.at[group]).start()
            copy(piece, place, pan_send, pan_recv.at[group], mate).start()

    panels(0, 4)

    def spread(k, _):
        to = (blk + k) % 32
        for c in range(2):
            copy(sb.at[2 * to + c], rhs.at[2 * blk + core], a_send, a_recv.at[blk // 2],
                 {"blk": to, "sub": 2 * xl + c}).start()
        return 0

    lax.fori_loop(1, 32, spread, 0)
    copy(sb.at[2 * blk + 1 - core], rhs.at[2 * blk + core], a_send, a_recv.at[blk // 2], mate).start()
    rhs[2 * blk + core] = sb[2 * blk + core]

    panels(4, 15)

    pltpu.make_async_copy(slab_hbm, slab, in_local).wait()
    for t in range(3):
        pairs[:, 2048 * t:2048 * t + 2048] = occ[slab[0] * NOCC + t] - virt[...]

    row = lax.broadcasted_iota(jnp.int32, (128, 128), 0)
    col = lax.broadcasted_iota(jnp.int32, (128, 128), 1)

    def invert(turn, _):
        g = (turn % 2) * 2 + turn // 2
        for q in range(2):
            piece = blocks.at[pl.ds(2 * g, 2), q, :, :, :, 0:128 * (q + 1)]
            pltpu.make_async_copy(piece, piece, diag_recv.at[q, g]).wait()

        def block(n):
            q = n % 2
            return blocks[2 * g + n // 2, q, :, :, :, 128 * q:128 * q + 128].reshape(128, 128)

        for n in range(4):
            value = block(n)
            diag = jnp.where(row == col, value, 0.0)
            down = 1.0 / jnp.sum(diag, axis=1, keepdims=True)
            across = 1.0 / jnp.sum(diag, axis=0, keepdims=True)
            below = (row == col + 1) & (row % 2 == 1)
            half_inv[4 * g + n] = jnp.where(row == col, down, 0.0) - jnp.where(below, value * down * across, 0.0)
        size = 2
        while size < 128:
            below = (row // size == col // size + 1) & (row // (2 * size) == col // (2 * size))
            for n in range(4):
                part = jnp.where(below, block(n), 0.0)
                half_tmp[n] = dot3(split(part), split(half_inv[4 * g + n]), NN)
            for n in range(4):
                now = half_inv[4 * g + n]
                half_inv[4 * g + n] = now - dot3(split(now), split(half_tmp[n]), NN)
            size *= 2
        for n in range(2):
            lower = blocks[2 * g + n, 1, :, :, :, 0:128].reshape(128, 128)
            half_tmp[n] = dot3(split(lower), split(half_inv[4 * g + 2 * n]), NN)
        for n in range(2):
            i = 2 * (2 * g + n) + core
            dinv[i, 0:128, 0:128] = half_inv[4 * g + 2 * n]
            dinv[i, 128:256, 128:256] = half_inv[4 * g + 2 * n + 1]
            dinv[i, 0:128, 128:256] = jnp.zeros((128, 128), F32)
            dinv[i, 128:256, 0:128] = -dot3(split(half_inv[4 * g + 2 * n + 1]), split(half_tmp[n]), NN)
        for n in range(2):
            i = 2 * (2 * g + n) + core
            copy(dinv.at[i], dinv.at[i], inv_send, inv_recv.at[g], mate).start()
        return 0

    lax.fori_loop(0, 4, invert, 0)

    def offer(i, value):
        gbuf[i, :, xl] = value.reshape(2, 64, 96)
        copy(gbuf.at[i, :, xl], gbuf.at[i, :, xl], g_send, g_recv.at[i], peer).start()

    def right_side(i):
        for count, here in ((3, blk // 2 == i), (4, blk // 2 != i)):
            @pl.when(here)
            def _(count=count):
                piece = rhs.at[0:count]
                copy(piece, piece, a_send, a_recv.at[i], mate).wait_recv()

        return rhs[pl.ds(4 * i, 4)].reshape(128, 96)

    def factor_part(i, t):
        k, at = panel_place(i, 2 * t)
        return split(pan[k, pl.ds(at, 2)].reshape(128, 256))

    def own_out(i):
        half = rowbuf.at[y, i, 1 - core]
        copy(half, half, x_send, x_recv.at[i], mate).wait_recv()
        for k, offset in enumerate((1, -1)):
            copy(rowbuf.at[y, i], rowbuf.at[y, i], y_send, y_recv.at[k, i], y_at(offset)).start()

        @pl.when(same)
        def _():
            for k, offset in enumerate((1, -1)):
                copy(rowbuf.at[y, i], colbuf.at[z, i], z_send, z_recv.at[k, i], z_at(offset)).start()
            colbuf[z, i] = rowbuf[y, i]

        @pl.when(jnp.logical_not(same))
        def _():
            copy(rowbuf.at[y, i], colbuf.at[z, i], s_send, s_recv.at[i], swap).start()

    def swapped_out(i):
        @pl.when(jnp.logical_not(same))
        def _():
            copy(colbuf.at[z, i], colbuf.at[z, i], s_send, s_recv.at[i], swap).wait_recv()
            for k, offset in enumerate((1, -1)):
                copy(colbuf.at[z, i], colbuf.at[z, i], z_send, z_recv.at[k, i], z_at(offset)).start()

    def got(buf, send, recv, place, k, i):
        copy(buf.at[place, i], buf.at[place, i], send, recv.at[k, i], mate).wait_recv()

    def forward(buf, send, recv, me, at, i):
        odd = i % 2
        step = 1 - 2 * odd
        src = (me - step + 4) % 4
        got(buf, send, recv, src, odd, i)
        copy(buf.at[src, i], buf.at[src, i], send, recv.at[2, i], at(step)).start()

    def forward_y(i):
        forward(rowbuf, y_send, y_recv, y, y_at, i)

    def forward_z(i):
        forward(colbuf, z_send, z_recv, z, z_at, i)

    def whole(buf, k, c):
        return jnp.concatenate([buf[k, 2 * c].reshape(192, 128), buf[k, 2 * c + 1].reshape(192, 128)], axis=1)

    def arrived(c):
        for odd in range(2):
            i = 2 * c + odd
            step = 1 - 2 * odd
            got(rowbuf, y_send, y_recv, (y + step + 4) % 4, 1 - odd, i)
            got(colbuf, z_send, z_recv, (z + step + 4) % 4, 1 - odd, i)
            got(rowbuf, y_send, y_recv, (y + 2) % 4, 2, i)
            got(colbuf, z_send, z_recv, (z + 2) % 4, 2, i)
        for k in range(4):
            cols[k * 192:k * 192 + 192] = whole(colbuf, k, c)
        for m in range(6):
            high, low = split(cols[128 * m:128 * m + 128].T)
            colh[:, 128 * m:128 * m + 128] = high
            coll[:, 128 * m:128 * m + 128] = low

    def product_rows(c, k):
        acc[k] = acc[k] + dot3(split(whole(rowbuf, k, c)), (colh[...], coll[...]), NN)

    def product_half(c, half):
        def part(k, _):
            product_rows(c, k)
            return 0

        lax.fori_loop(2 * half, 2 * half + 2, part, 0)

    acc[...] = jnp.zeros_like(acc)
    known[...] = jnp.zeros_like(known)
    offer(0, right_side(0))

    def round_of(i, _):
        for group, (at, many, wide) in enumerate(((0, 2, 29), (2, 2, 25), (4, 4, 19), (8, 4, 14))):
            @pl.when(i == at)
            def _(group=group, many=many, wide=wide):
                piece = pan.at[0:many, 0:wide]
                pltpu.make_async_copy(piece, piece, pan_recv.at[group]).wait()

        @pl.when(i % 4 == 0)
        def _():
            copy(dinv.at[0:2], dinv.at[0:2], inv_send, inv_recv.at[i // 4], mate).wait_recv()

        inverse = split(dinv[i])

        @pl.when(i > 0)
        def _():
            def later(u, _):
                k, at = panel_place(i - 1, 4 * u)
                part = split(pan[k, pl.ds(at, 4)].reshape(256, 256))
                term = dot3(part, (xh[...], xlow[...]), NN)
                rows = pl.ds(8 * u, 8)
                known[rows] = known[rows] + term.reshape(8, 32, 96)
                return 0

            lax.fori_loop((i + 1) // 2, 8, later, 0)
            own_out(i - 1)

        @pl.when(i > 1)
        def _():
            swapped_out(i - 2)

        @pl.when((i > 5) & (i % 2 == 0))
        def _():
            arrived((i - 6) // 2)

        @pl.when(i > 5)
        def _():
            product_half((i - 6) // 2, i % 2)

        @pl.when(i > 1)
        def _():
            forward_y(i - 2)

        @pl.when(i > 2)
        def _():
            forward_z(i - 3)

        @pl.when(i < 15)
        def _():
            rest = right_side(i + 1) - known[pl.ds(4 * i + 4, 4)].reshape(128, 96)
            rhs[pl.ds(4 * i + 4, 4)] = rest.reshape(4, 32, 96)

        other = gbuf.at[i, :, 1 - xl]
        copy(other, other, g_send, g_recv.at[i], peer).wait_recv()
        solved = dot3(inverse, split(gbuf[i].reshape(256, 96)), NN)
        high, low = split(solved)
        xh[...] = high
        xlow[...] = low

        @pl.when(i < 15)
        def _():
            term = dot3(factor_part(i, i + 1), (high, low), NN)
            offer(i + 1, rhs[pl.ds(4 * i + 4, 4)].reshape(128, 96) - term)

        xbuf[...] = solved.reshape(2, 128, 96)
        tx[i] = xbuf[1 - core].T
        copy(tx.at[i], rowbuf.at[y, i, core], x_send, x_recv.at[i], mate).start()
        rowbuf[y, i, core] = xbuf[core].T
        return 0

    lax.fori_loop(0, 16, round_of, 0)

    own_out(15)
    swapped_out(14)
    forward_y(14)
    forward_z(13)
    swapped_out(15)
    arrived(5)
    product_half(5, 0)
    forward_z(14)
    forward_y(15)
    product_half(5, 1)
    arrived(6)
    product_half(6, 0)
    forward_z(15)
    product_half(6, 1)
    arrived(7)

    mine = pl.ds(pl.multiple_of(core * 384, 128), 384)
    theirs = pl.ds(pl.multiple_of((1 - core) * 384, 128), 384)
    order = ((y + 2) % 4, (y + 1) % 4, (y + 3) % 4, y)

    def trade(n):
        k = order[n]
        return copy(acc.at[k, :, theirs], exch.at[k], t_send.at[n], t_recv.at[n], mate)

    for n in range(4):
        product_rows(7, order[n])
        trade(n).start()

    def summed(n):
        trade(n).wait_recv()
        k = order[n]
        total[k] = acc[k, :, mine] + exch[k]

    summed(0)
    hops = []
    for at, offset in enumerate((1, -1)):
        hops.append(copy(total.at[order[0], 96 * at:96 * at + 96], relay.at[at],
                         e_send.at[at], e_recv.at[at], y_at(offset)))
        hops[-1].start()
    for n, offset in ((1, 1), (2, -1)):
        summed(n)
        hops.append(copy(total.at[order[n]], final.at[y], e_send.at[n + 1], e_recv.at[n + 1], y_at(offset)))
        hops[-1].start()
    for at, offset in enumerate((1, -1)):
        copy(relay.at[at], relay.at[at], e_send.at[at], e_recv.at[at], mate).wait_recv()
        src = (y - offset + 4) % 4
        hops.append(copy(relay.at[at], final.at[src, 96 * at:96 * at + 96],
                         e_send.at[4 + at], e_recv.at[4 + at], y_at(offset)))
        hops[-1].start()
    summed(3)
    final[y] = total[y]
    for n, offset in ((1, 1), (2, -1)):
        src = (y - offset + 4) % 4
        copy(final.at[src], final.at[src], e_send.at[n + 1], e_recv.at[n + 1], mate).wait_recv()
    src = (y + 2) % 4
    for at in range(2):
        piece = final.at[src, 96 * at:96 * at + 96]
        copy(piece, piece, e_send.at[4 + at], e_recv.at[4 + at], mate).wait_recv()
    window = pairs[:, pl.ds(pl.multiple_of((blk * 192) // 128 * 128, 128), 256)]
    across = jnp.where(blk % 2 == 1, window[:, 64:256], window[:, 0:192])
    line = lax.broadcasted_iota(jnp.int32, (192, 192), 0)
    lane = lax.broadcasted_iota(jnp.int32, (192, 192), 1)
    down = jnp.sum(jnp.where(line == lane, across, 0.0), axis=1, keepdims=True)
    for k in range(2):
        wide = pairs[:, pl.ds(pl.multiple_of(sub * 1536 + k * 768, 128), 768)]
        sums = jnp.concatenate([final[q, :, k * 192:k * 192 + 192] for q in range(4)], axis=1)
        out[:, k * 768:k * 768 + 768] = sums / (down + wide)
    for hop in hops:
        hop.wait_send()
    for n in range(4):
        trade(n).wait_send()

    piece = rowbuf.at[0:3]
    copy(piece, piece, y_send, y_recv.at[0, 0], mate).wait_send()
    copy(piece, piece, z_send, z_recv.at[0, 0], mate).wait_send()

    @pl.when(jnp.logical_not(same))
    def _():
        copy(rowbuf.at[0], rowbuf.at[0], s_send, s_recv.at[0], swap).wait_send()

    piece = pan.at[:, 0:30, core]
    copy(piece, piece, pan_send, pan_recv.at[0], mate).wait_send()
    piece = gbuf.at[:, :, xl]
    copy(piece, piece, g_send, g_recv.at[0], peer).wait_send()
    for q in range(2):
        piece = blocks.at[0:6, q, :, :, :, 0:128 * (q + 1)]
        copy(piece, piece, diag_send.at[q], diag_recv.at[q, 0], mate).wait_send()
    copy(sb.at[0:63], sb.at[0:63], a_send, a_recv.at[0], mate).wait_send()
    copy(dinv.at[0:8], dinv.at[0:8], inv_send, inv_recv.at[0], mate).wait_send()
    copy(tx, tx, x_send, x_recv.at[0], mate).wait_send()


def amplitude_block(integrals, slots, factor, occ, slab, virt):
    dma = pltpu.SemaphoreType.DMA
    vmem = pl.BlockSpec(memory_space=pltpu.VMEM)
    hbm = pl.BlockSpec(memory_space=pltpu.HBM)
    return pl.pallas_call(
        fused_kernel,
        out_shape=jax.ShapeDtypeStruct((192, 1536), F32),
        in_specs=[vmem, vmem, hbm, pl.BlockSpec(memory_space=pltpu.SMEM), hbm, vmem],
        out_specs=vmem,
        scratch_shapes=[
            pltpu.SMEM((1,), jnp.int32),
            pltpu.VMEM((8, 34, 2, 32, 256), F32),
            pltpu.VMEM((8, 2, 2, 2, 32, 256), F32),
            pltpu.VMEM((16, 128, 128), F32),
            pltpu.VMEM((4, 128, 128), F32),
            pltpu.VMEM((16, 256, 256), F32),
            pltpu.VMEM((64, 32, 96), F32),
            pltpu.VMEM((64, 32, 96), F32),
            pltpu.VMEM((64, 32, 96), F32),
            pltpu.VMEM((16, 2, 2, 64, 96), F32),
            pltpu.VMEM((256, 96), BF16),
            pltpu.VMEM((256, 96), BF16),
            pltpu.VMEM((2, 128, 96), F32),
            pltpu.VMEM((16, 96, 128), F32),
            pltpu.VMEM((4, 16, 2, 96, 128), F32),
            pltpu.VMEM((4, 16, 2, 96, 128), F32),
            pltpu.VMEM((4, 192, 768), F32),
            pltpu.VMEM((768, 256), F32),
            pltpu.VMEM((256, 768), BF16),
            pltpu.VMEM((256, 768), BF16),
            pltpu.VMEM((1, 6144), F32),
            pltpu.VMEM((4, 192, 384), F32),
            pltpu.VMEM((4, 192, 384), F32),
            pltpu.VMEM((4, 192, 384), F32),
            pltpu.VMEM((2, 96, 384), F32),
            dma, dma, dma((4,)), dma((2,)), dma((2, 4)), dma, dma((16,)), dma, dma((4,)),
            dma, dma((16,)), dma, dma((16,)),
            dma, dma((3, 16)), dma, dma((3, 16)), dma, dma((16,)),
            dma((4,)), dma((4,)), dma((6,)), dma((6,)),
        ],
        compiler_params=pltpu.CompilerParams(
            collective_id=0, has_side_effects=True, vmem_limit_bytes=52 * 2**20),
    )(integrals, slots, factor, occ, slab, virt)


def shards(integrals, slot_order, factor_rows, occ_energy, slab_index, virt_energy):
    return amplitude_block(integrals[0, 0], slot_order[0], factor_rows[:, 0],
                           occ_energy, slab_index, virt_energy[None])


def solution(mesh):
    in_specs = (
        P("blk", "sub", None, None),
        P("blk", "sub", None),
        P(None, "sub", None, None),
        P(),
        P(),
        P(),
    )
    out_specs = P("blk", "sub")
    return jax.shard_map(shards, mesh=mesh, in_specs=in_specs, out_specs=out_specs, check_vma=False)
```

```python
import functools

import jax
import jax.numpy as jnp
from jax import lax
from jax.experimental import pallas as pl
from jax.experimental.pallas import tpu as pltpu
from jax.sharding import PartitionSpec as P

NOCC = 3
F32 = jnp.float32
BF16 = jnp.bfloat16
MESH = pl.DeviceIdType.MESH
NN = (((1,), (0,)), ((), ()))
NT = (((1,), (1,)), ((), ()))


def split(x):
    high = x.astype(BF16)
    return high, (x - high.astype(F32)).astype(BF16)


def dot3(a, b, dims):
    def one(p, q):
        return lax.dot_general(p, q, dims, preferred_element_type=F32)

    return one(a[0], b[0]) + (one(a[0], b[1]) + one(a[1], b[0]))


def copy(src, dst, send, recv, who):
    return pltpu.make_async_remote_copy(
        src_ref=src, dst_ref=dst, send_sem=send, recv_sem=recv,
        device_id=who, device_id_type=MESH)


def panel_place(i, r):
    if isinstance(i, int):
        return (i, r - 2 * i) if i < 8 else (15 - i, r + 2)
    return jnp.where(i < 8, i, 15 - i), jnp.where(i < 8, r - 2 * i, r + 2)


def fused_kernel(integrals, slots, factor, occ, slab_hbm, virt, out, slab, pan, blocks, half_inv, half_tmp, dinv, sb, rhs, known, gbuf,
                 xh, xlow, xbuf, tx, rowbuf, colbuf, acc, cols, colh, coll, pairs, exch, total, final, relay,
                 in_local, pan_send, pan_recv, diag_send, diag_recv, a_send, a_recv,
                 inv_send, inv_recv, g_send, g_recv, x_send, x_recv,
                 y_send, y_recv, z_send, z_recv, s_send, s_recv, t_send, t_recv, e_send, e_recv):
    blk, sub = lax.axis_index("blk"), lax.axis_index("sub")
    hi = blk // 16
    xl, core = sub // 2, sub % 2
    x = 2 * hi + xl
    y, z = blk % 4, (blk // 4) % 4
    same = hi == xl
    mate = {"blk": blk, "sub": sub + 1 - 2 * core}
    peer = {"blk": blk, "sub": sub + 2 - 4 * xl}

    def beside(offset, to_core):
        other = (x + offset + 4) % 4
        return {"blk": blk + (other // 2 - hi) * 16, "sub": (other % 2) * 2 + to_core}

    def y_at(offset):
        return {"blk": blk - y + (y + offset + 4) % 4, "sub": sub}

    def z_at(offset):
        return {"blk": blk - 4 * z + 4 * ((z + offset + 4) % 4), "sub": sub}

    swap = {"blk": blk + (1 - 2 * hi) * 16, "sub": sub + (1 - 2 * xl) * 2}

    pltpu.make_async_copy(slab_hbm, slab, in_local).start()
    barrier = pltpu.get_barrier_semaphore()

    def greet(k, _):
        for c in range(2):
            pl.semaphore_signal(barrier, inc=1, device_id_type=MESH,
                                device_id={"blk": (blk + k) % 32, "sub": 2 * xl + c})
        return 0

    lax.fori_loop(1, 32, greet, 0)
    pl.semaphore_signal(barrier, inc=1, device_id=mate, device_id_type=MESH)
    for offset in (1, -1):
        for c in range(2):
            pl.semaphore_signal(barrier, inc=1, device_id=beside(offset, c), device_id_type=MESH)

    def slab_of(i, q):
        wide = 128 * (q + 1)
        return factor.at[2 * i + q, :, pl.ds(pl.multiple_of(256 * i, 256), wide)]

    def slab_place(j, q, at_core):
        return blocks.at[j, q, xl, at_core, :, 0:128 * (q + 1)]

    order = (0, 1, 4, 5, 2, 3, 6, 7)
    for j in order:
        for q in range(2):
            pltpu.make_async_copy(slab_of(2 * j + core, q), slab_place(j, q, core), diag_recv.at[q, j // 2]).start()

    onehot = (slots[...] == lax.broadcasted_iota(jnp.int32, (32, 32), 0)).astype(F32).astype(BF16)

    def pick(v):
        return lax.dot_general(onehot, v, NN, preferred_element_type=F32)

    for g in range(16):
        value = integrals[:, 384 * g:384 * g + 384]
        high = value.astype(BF16)
        rest = value - high.astype(F32)
        mid = rest.astype(BF16)
        low = (rest - mid.astype(F32)).astype(BF16)
        picked = pick(high) + (pick(mid) + pick(low))
        for k in range(4):
            sb[4 * g + k] = jnp.concatenate(
                [picked[8 * m:8 * m + 8, 96 * k:96 * k + 96] for m in range(4)], axis=1)

    pl.semaphore_wait(barrier, 67)

    for j in order:
        for q in range(2):
            for c in range(2):
                copy(slab_of(2 * j + c, q), slab_place(j, q, core), diag_send.at[q], diag_recv.at[q, j // 2],
                     beside(1 if j < 4 else -1, c)).start()
            copy(slab_of(2 * j + 1 - core, q), slab_place(j, q, core), diag_send.at[q], diag_recv.at[q, j // 2],
                 mate).start()

    def panels(first, last):
        for i in range(first, last):
            k, row = panel_place(i, 2 * i + 2)
            piece = factor.at[2 * i + 2:32, :, 256 * i:256 * i + 256]
            place = pan.at[k, row:row + 30 - 2 * i, core]
            group = (i > 1) + (i > 3) + (i > 7)
            pltpu.make_async_copy(piece, place, pan_recv.at[group]).start()
            copy(piece, place, pan_send, pan_recv.at[group], mate).start()

    panels(0, 4)

    def send_right_side(to):
        for c in range(2):
            copy(sb.at[2 * to + c], rhs.at[2 * blk + core], a_send, a_recv.at[blk // 2],
                 {"blk": to, "sub": 2 * xl + c}).start()

    def cross(k, _):
        send_right_side((1 - hi) * 16 + (blk + k) % 16)
        return 0

    def spread(k, _):
        send_right_side(hi * 16 + (blk + k) % 16)
        return 0

    @pl.when(hi == 0)
    def _():
        lax.fori_loop(0, 16, cross, 0)

    lax.fori_loop(1, 16, spread, 0)
    copy(sb.at[2 * blk + 1 - core], rhs.at[2 * blk + core], a_send, a_recv.at[blk // 2], mate).start()
    rhs[2 * blk + core] = sb[2 * blk + core]

    panels(4, 15)

    pltpu.make_async_copy(slab_hbm, slab, in_local).wait()
    for t in range(3):
        pairs[:, 2048 * t:2048 * t + 2048] = occ[slab[0] * NOCC + t] - virt[...]

    row = lax.broadcasted_iota(jnp.int32, (128, 128), 0)
    col = lax.broadcasted_iota(jnp.int32, (128, 128), 1)

    def invert(turn, _):
        g = (turn % 2) * 2 + turn // 2
        for q in range(2):
            piece = blocks.at[pl.ds(2 * g, 2), q, :, :, :, 0:128 * (q + 1)]
            pltpu.make_async_copy(piece, piece, diag_recv.at[q, g]).wait()

        @pl.when((turn == 2) & (hi == 1))
        def _():
            lax.fori_loop(0, 16, cross, 0)

        def block(n):
            q = n % 2
            return blocks[2 * g + n // 2, q, :, :, :, 128 * q:128 * q + 128].reshape(128, 128)

        for n in range(4):
            value = block(n)
            diag = jnp.where(row == col, value, 0.0)
            down = 1.0 / jnp.sum(diag, axis=1, keepdims=True)
            across = 1.0 / jnp.sum(diag, axis=0, keepdims=True)
            below = (row == col + 1) & (row % 2 == 1)
            half_inv[4 * g + n] = jnp.where(row == col, down, 0.0) - jnp.where(below, value * down * across, 0.0)
        size = 2
        while size < 128:
            below = (row // size == col // size + 1) & (row // (2 * size) == col // (2 * size))
            for n in range(4):
                part = jnp.where(below, block(n), 0.0)
                half_tmp[n] = dot3(split(part), split(half_inv[4 * g + n]), NN)
            for n in range(4):
                now = half_inv[4 * g + n]
                half_inv[4 * g + n] = now - dot3(split(now), split(half_tmp[n]), NN)
            size *= 2
        for n in range(2):
            lower = blocks[2 * g + n, 1, :, :, :, 0:128].reshape(128, 128)
            half_tmp[n] = dot3(split(lower), split(half_inv[4 * g + 2 * n]), NN)
        for n in range(2):
            i = 2 * (2 * g + n) + core
            dinv[i, 0:128, 0:128] = half_inv[4 * g + 2 * n]
            dinv[i, 128:256, 128:256] = half_inv[4 * g + 2 * n + 1]
            dinv[i, 0:128, 128:256] = jnp.zeros((128, 128), F32)
            dinv[i, 128:256, 0:128] = -dot3(split(half_inv[4 * g + 2 * n + 1]), split(half_tmp[n]), NN)
        for n in range(2):
            i = 2 * (2 * g + n) + core
            copy(dinv.at[i], dinv.at[i], inv_send, inv_recv.at[g], mate).start()
        return 0

    lax.fori_loop(0, 4, invert, 0)

    def offer(i, value):
        gbuf[i, :, xl] = value.reshape(2, 64, 96)
        copy(gbuf.at[i, :, xl], gbuf.at[i, :, xl], g_send, g_recv.at[i], peer).start()

    def right_side(i):
        for count, here in ((3, blk // 2 == i), (4, blk // 2 != i)):
            @pl.when(here)
            def _(count=count):
                piece = rhs.at[0:count]
                copy(piece, piece, a_send, a_recv.at[i], mate).wait_recv()

        packed = rhs[pl.ds(4 * i, 4)]
        return jnp.concatenate([packed[:, :, 96 * m:96 * m + 96] for m in range(4)], axis=1).reshape(128, 96)

    def factor_part(i, t):
        k, at = panel_place(i, 2 * t)
        return split(pan[k, pl.ds(at, 2)].reshape(128, 256))

    def own_out(i):
        half = rowbuf.at[y, i, 1 - core]
        copy(half, half, x_send, x_recv.at[i], mate).wait_recv()
        for k, offset in enumerate((1, -1)):
            copy(rowbuf.at[y, i], rowbuf.at[y, i], y_send, y_recv.at[k, i], y_at(offset)).start()

        @pl.when(same)
        def _():
            for k, offset in enumerate((1, -1)):
                copy(rowbuf.at[y, i], colbuf.at[z, i], z_send, z_recv.at[k, i], z_at(offset)).start()
            colbuf[z, i] = rowbuf[y, i]

        @pl.when(jnp.logical_not(same))
        def _():
            copy(rowbuf.at[y, i], colbuf.at[z, i], s_send, s_recv.at[i], swap).start()

    def swapped_out(i):
        @pl.when(jnp.logical_not(same))
        def _():
            copy(colbuf.at[z, i], colbuf.at[z, i], s_send, s_recv.at[i], swap).wait_recv()
            for k, offset in enumerate((1, -1)):
                copy(colbuf.at[z, i], colbuf.at[z, i], z_send, z_recv.at[k, i], z_at(offset)).start()

    def got(buf, send, recv, place, k, i):
        copy(buf.at[place, i], buf.at[place, i], send, recv.at[k, i], mate).wait_recv()

    def forward(buf, send, recv, me, at, i):
        odd = i % 2
        step = 1 - 2 * odd
        src = (me - step + 4) % 4
        got(buf, send, recv, src, odd, i)
        copy(buf.at[src, i], buf.at[src, i], send, recv.at[2, i], at(step)).start()

    def forward_y(i):
        forward(rowbuf, y_send, y_recv, y, y_at, i)

    def forward_z(i):
        forward(colbuf, z_send, z_recv, z, z_at, i)

    def whole(buf, k, c):
        return jnp.concatenate([buf[k, 2 * c].reshape(192, 128), buf[k, 2 * c + 1].reshape(192, 128)], axis=1)

    def arrived(c):
        for odd in range(2):
            i = 2 * c + odd
            step = 1 - 2 * odd
            got(rowbuf, y_send, y_recv, (y + step + 4) % 4, 1 - odd, i)
            got(colbuf, z_send, z_recv, (z + step + 4) % 4, 1 - odd, i)
            got(rowbuf, y_send, y_recv, (y + 2) % 4, 2, i)
            got(colbuf, z_send, z_recv, (z + 2) % 4, 2, i)
        for k in range(4):
            cols[k * 192:k * 192 + 192] = whole(colbuf, k, c)
        for m in range(6):
            high, low = split(cols[128 * m:128 * m + 128].T)
            colh[:, 128 * m:128 * m + 128] = high
            coll[:, 128 * m:128 * m + 128] = low

    def product_rows(c, k):
        acc[k] = acc[k] + dot3(split(whole(rowbuf, k, c)), (colh[...], coll[...]), NN)

    def product_half(c, half):
        def part(k, _):
            product_rows(c, k)
            return 0

        lax.fori_loop(2 * half, 2 * half + 2, part, 0)

    acc[...] = jnp.zeros_like(acc)
    known[...] = jnp.zeros_like(known)
    offer(0, right_side(0))

    def round_of(i, _):
        for group, (at, many, wide) in enumerate(((0, 2, 29), (2, 2, 25), (4, 4, 19), (8, 4, 14))):
            @pl.when(i == at)
            def _(group=group, many=many, wide=wide):
                piece = pan.at[0:many, 0:wide]
                pltpu.make_async_copy(piece, piece, pan_recv.at[group]).wait()

        @pl.when(i % 4 == 0)
        def _():
            copy(dinv.at[0:2], dinv.at[0:2], inv_send, inv_recv.at[i // 4], mate).wait_recv()

        inverse = split(dinv[i])

        @pl.when(i > 0)
        def _():
            def later(u, _):
                k, at = panel_place(i - 1, 4 * u)
                part = split(pan[k, pl.ds(at, 4)].reshape(256, 256))
                term = dot3(part, (xh[...], xlow[...]), NN)
                rows = pl.ds(8 * u, 8)
                known[rows] = known[rows] + term.reshape(8, 32, 96)
                return 0

            lax.fori_loop((i + 1) // 2, 8, later, 0)
            own_out(i - 1)

        @pl.when(i > 1)
        def _():
            swapped_out(i - 2)

        @pl.when((i > 5) & (i % 2 == 0))
        def _():
            arrived((i - 6) // 2)

        @pl.when(i > 5)
        def _():
            product_half((i - 6) // 2, i % 2)

        @pl.when(i > 1)
        def _():
            forward_y(i - 2)

        @pl.when(i > 2)
        def _():
            forward_z(i - 3)

        @pl.when(i < 15)
        def _():
            rest = right_side(i + 1) - known[pl.ds(4 * i + 4, 4)].reshape(128, 96)
            known[pl.ds(4 * i + 4, 4)] = rest.reshape(4, 32, 96)

        other = gbuf.at[i, :, 1 - xl]
        copy(other, other, g_send, g_recv.at[i], peer).wait_recv()
        solved = dot3(inverse, split(gbuf[i].reshape(256, 96)), NN)
        high, low = split(solved)
        xh[...] = high
        xlow[...] = low

        @pl.when(i < 15)
        def _():
            term = dot3(factor_part(i, i + 1), (high, low), NN)
            offer(i + 1, known[pl.ds(4 * i + 4, 4)].reshape(128, 96) - term)

        xbuf[...] = solved.reshape(2, 128, 96)
        tx[i] = xbuf[1 - core].T
        copy(tx.at[i], rowbuf.at[y, i, core], x_send, x_recv.at[i], mate).start()
        rowbuf[y, i, core] = xbuf[core].T
        return 0

    lax.fori_loop(0, 16, round_of, 0)

    own_out(15)
    swapped_out(14)
    forward_y(14)
    forward_z(13)
    swapped_out(15)
    arrived(5)
    product_half(5, 0)
    forward_z(14)
    forward_y(15)
    product_half(5, 1)
    arrived(6)
    product_half(6, 0)
    forward_z(15)
    product_half(6, 1)
    arrived(7)

    mine = pl.ds(pl.multiple_of(core * 384, 128), 384)
    theirs = pl.ds(pl.multiple_of((1 - core) * 384, 128), 384)
    order = ((y + 2) % 4, (y + 1) % 4, (y + 3) % 4, y)

    def trade(n):
        k = order[n]
        return copy(acc.at[k, :, theirs], exch.at[k], t_send.at[n], t_recv.at[n], mate)

    for n in range(4):
        product_rows(7, order[n])
        trade(n).start()

    def summed(n):
        trade(n).wait_recv()
        k = order[n]
        total[k] = acc[k, :, mine] + exch[k]

    summed(0)
    hops = []
    for at, offset in enumerate((1, -1)):
        hops.append(copy(total.at[order[0], 96 * at:96 * at + 96], relay.at[at],
                         e_send.at[at], e_recv.at[at], y_at(offset)))
        hops[-1].start()
    for n, offset in ((1, 1), (2, -1)):
        summed(n)
        hops.append(copy(total.at[order[n]], final.at[y], e_send.at[n + 1], e_recv.at[n + 1], y_at(offset)))
        hops[-1].start()
    for at, offset in enumerate((1, -1)):
        copy(relay.at[at], relay.at[at], e_send.at[at], e_recv.at[at], mate).wait_recv()
        src = (y - offset + 4) % 4
        hops.append(copy(relay.at[at], final.at[src, 96 * at:96 * at + 96],
                         e_send.at[4 + at], e_recv.at[4 + at], y_at(offset)))
        hops[-1].start()
    summed(3)
    final[y] = total[y]
    for n, offset in ((1, 1), (2, -1)):
        src = (y - offset + 4) % 4
        copy(final.at[src], final.at[src], e_send.at[n + 1], e_recv.at[n + 1], mate).wait_recv()
    src = (y + 2) % 4
    for at in range(2):
        piece = final.at[src, 96 * at:96 * at + 96]
        copy(piece, piece, e_send.at[4 + at], e_recv.at[4 + at], mate).wait_recv()
    window = pairs[:, pl.ds(pl.multiple_of((blk * 192) // 128 * 128, 128), 256)]
    across = jnp.where(blk % 2 == 1, window[:, 64:256], window[:, 0:192])
    line = lax.broadcasted_iota(jnp.int32, (192, 192), 0)
    lane = lax.broadcasted_iota(jnp.int32, (192, 192), 1)
    down = jnp.sum(jnp.where(line == lane, across, 0.0), axis=1, keepdims=True)
    for k in range(2):
        wide = pairs[:, pl.ds(pl.multiple_of(sub * 1536 + k * 768, 128), 768)]
        sums = jnp.concatenate([final[q, :, k * 192:k * 192 + 192] for q in range(4)], axis=1)
        out[:, k * 768:k * 768 + 768] = sums / (down + wide)
    for hop in hops:
        hop.wait_send()
    for n in range(4):
        trade(n).wait_send()

    piece = rowbuf.at[0:3]
    copy(piece, piece, y_send, y_recv.at[0, 0], mate).wait_send()
    copy(piece, piece, z_send, z_recv.at[0, 0], mate).wait_send()

    @pl.when(jnp.logical_not(same))
    def _():
        copy(rowbuf.at[0], rowbuf.at[0], s_send, s_recv.at[0], swap).wait_send()

    piece = pan.at[:, 0:30, core]
    copy(piece, piece, pan_send, pan_recv.at[0], mate).wait_send()
    piece = gbuf.at[:, :, xl]
    copy(piece, piece, g_send, g_recv.at[0], peer).wait_send()
    for q in range(2):
        piece = blocks.at[0:6, q, :, :, :, 0:128 * (q + 1)]
        copy(piece, piece, diag_send.at[q], diag_recv.at[q, 0], mate).wait_send()
    copy(sb.at[0:63], sb.at[0:63], a_send, a_recv.at[0], mate).wait_send()
    copy(dinv.at[0:8], dinv.at[0:8], inv_send, inv_recv.at[0], mate).wait_send()
    copy(tx, tx, x_send, x_recv.at[0], mate).wait_send()


def amplitude_block(integrals, slots, factor, occ, slab, virt):
    dma = pltpu.SemaphoreType.DMA
    vmem = pl.BlockSpec(memory_space=pltpu.VMEM)
    hbm = pl.BlockSpec(memory_space=pltpu.HBM)
    return pl.pallas_call(
        fused_kernel,
        out_shape=jax.ShapeDtypeStruct((192, 1536), F32),
        in_specs=[vmem, vmem, hbm, pl.BlockSpec(memory_space=pltpu.SMEM), hbm, vmem],
        out_specs=vmem,
        scratch_shapes=[
            pltpu.SMEM((1,), jnp.int32),
            pltpu.VMEM((8, 34, 2, 32, 256), F32),
            pltpu.VMEM((8, 2, 2, 2, 32, 256), F32),
            pltpu.VMEM((16, 128, 128), F32),
            pltpu.VMEM((4, 128, 128), F32),
            pltpu.VMEM((16, 256, 256), F32),
            pltpu.VMEM((64, 8, 384), F32),
            pltpu.VMEM((64, 8, 384), F32),
            pltpu.VMEM((64, 32, 96), F32),
            pltpu.VMEM((16, 2, 2, 64, 96), F32),
            pltpu.VMEM((256, 96), BF16),
            pltpu.VMEM((256, 96), BF16),
            pltpu.VMEM((2, 128, 96), F32),
            pltpu.VMEM((16, 96, 128), F32),
            pltpu.VMEM((4, 16, 2, 96, 128), F32),
            pltpu.VMEM((4, 16, 2, 96, 128), F32),
            pltpu.VMEM((4, 192, 768), F32),
            pltpu.VMEM((768, 256), F32),
            pltpu.VMEM((256, 768), BF16),
            pltpu.VMEM((256, 768), BF16),
            pltpu.VMEM((1, 6144), F32),
            pltpu.VMEM((4, 192, 384), F32),
            pltpu.VMEM((4, 192, 384), F32),
            pltpu.VMEM((4, 192, 384), F32),
            pltpu.VMEM((2, 96, 384), F32),
            dma, dma, dma((4,)), dma((2,)), dma((2, 4)), dma, dma((16,)), dma, dma((4,)),
            dma, dma((16,)), dma, dma((16,)),
            dma, dma((3, 16)), dma, dma((3, 16)), dma, dma((16,)),
            dma((4,)), dma((4,)), dma((6,)), dma((6,)),
        ],
        compiler_params=pltpu.CompilerParams(
            collective_id=0, has_side_effects=True, vmem_limit_bytes=52 * 2**20),
    )(integrals, slots, factor, occ, slab, virt)


def shards(integrals, slot_order, factor_rows, occ_energy, slab_index, virt_energy):
    return amplitude_block(integrals[0, 0], slot_order[0], factor_rows[:, 0],
                           occ_energy, slab_index, virt_energy[None])


def solution(mesh):
    in_specs = (
        P("blk", "sub", None, None),
        P("blk", "sub", None),
        P(None, "sub", None, None),
        P(),
        P(),
        P(),
    )
    out_specs = P("blk", "sub")
    return jax.shard_map(shards, mesh=mesh, in_specs=in_specs, out_specs=out_specs, check_vma=False)
```

```python
import functools

import jax
import jax.numpy as jnp
from jax import lax
from jax.experimental import pallas as pl
from jax.experimental.pallas import tpu as pltpu
from jax.sharding import PartitionSpec as P

NOCC = 3
F32 = jnp.float32
BF16 = jnp.bfloat16
MESH = pl.DeviceIdType.MESH
NN = (((1,), (0,)), ((), ()))
NT = (((1,), (1,)), ((), ()))


def split(x):
    high = x.astype(BF16)
    return high, (x - high.astype(F32)).astype(BF16)


def dot3(a, b, dims):
    def one(p, q):
        return lax.dot_general(p, q, dims, preferred_element_type=F32)

    return one(a[0], b[0]) + (one(a[0], b[1]) + one(a[1], b[0]))


def copy(src, dst, send, recv, who):
    return pltpu.make_async_remote_copy(
        src_ref=src, dst_ref=dst, send_sem=send, recv_sem=recv,
        device_id=who, device_id_type=MESH)


def panel_place(i, r):
    if isinstance(i, int):
        return (i, r - 2 * i) if i < 8 else (15 - i, r + 2)
    return jnp.where(i < 8, i, 15 - i), jnp.where(i < 8, r - 2 * i, r + 2)


def fused_kernel(integrals, slots, factor, occ, slab_hbm, virt, out, slab, pan, blocks, half_inv, half_tmp, dinv, sb, rhs, known, gbuf,
                 xh, xlow, xbuf, tx, rowbuf, colbuf, acc, cols, colh, coll, pairs, exch, total, final, relay,
                 in_local, pan_send, pan_recv, diag_send, diag_recv, a_send, a_recv,
                 inv_send, inv_recv, g_send, g_recv, x_send, x_recv,
                 y_send, y_recv, z_send, z_recv, s_send, s_recv, t_send, t_recv, e_send, e_recv):
    blk, sub = lax.axis_index("blk"), lax.axis_index("sub")
    hi = blk // 16
    xl, core = sub // 2, sub % 2
    x = 2 * hi + xl
    y, z = blk % 4, (blk // 4) % 4
    same = hi == xl
    mate = {"blk": blk, "sub": sub + 1 - 2 * core}
    peer = {"blk": blk, "sub": sub + 2 - 4 * xl}

    def beside(offset, to_core):
        other = (x + offset + 4) % 4
        return {"blk": blk + (other // 2 - hi) * 16, "sub": (other % 2) * 2 + to_core}

    def y_at(offset):
        return {"blk": blk - y + (y + offset + 4) % 4, "sub": sub}

    def z_at(offset):
        return {"blk": blk - 4 * z + 4 * ((z + offset + 4) % 4), "sub": sub}

    swap = {"blk": blk + (1 - 2 * hi) * 16, "sub": sub + (1 - 2 * xl) * 2}

    pltpu.make_async_copy(slab_hbm, slab, in_local).start()
    barrier = pltpu.get_barrier_semaphore()

    def greet(k, _):
        for c in range(2):
            pl.semaphore_signal(barrier, inc=1, device_id_type=MESH,
                                device_id={"blk": (blk + k) % 32, "sub": 2 * xl + c})
        return 0

    lax.fori_loop(1, 32, greet, 0)
    pl.semaphore_signal(barrier, inc=1, device_id=mate, device_id_type=MESH)
    for offset in (1, -1):
        for c in range(2):
            pl.semaphore_signal(barrier, inc=1, device_id=beside(offset, c), device_id_type=MESH)

    def slab_of(i, q):
        wide = 128 * (q + 1)
        return factor.at[2 * i + q, :, pl.ds(pl.multiple_of(256 * i, 256), wide)]

    def slab_place(j, q, at_core):
        return blocks.at[j, q, xl, at_core, :, 0:128 * (q + 1)]

    order = (0, 1, 4, 5, 2, 3, 6, 7)
    for j in order:
        for q in range(2):
            pltpu.make_async_copy(slab_of(2 * j + core, q), slab_place(j, q, core), diag_recv.at[q, j // 2]).start()

    onehot = (slots[...] == lax.broadcasted_iota(jnp.int32, (32, 32), 0)).astype(F32).astype(BF16)

    def pick(v):
        return lax.dot_general(onehot, v, NN, preferred_element_type=F32)

    for g in range(16):
        value = integrals[:, 384 * g:384 * g + 384]
        high = value.astype(BF16)
        rest = value - high.astype(F32)
        mid = rest.astype(BF16)
        low = (rest - mid.astype(F32)).astype(BF16)
        picked = pick(high) + (pick(mid) + pick(low))
        for k in range(4):
            sb[4 * g + k] = jnp.concatenate(
                [picked[8 * m:8 * m + 8, 96 * k:96 * k + 96] for m in range(4)], axis=1)

    pl.semaphore_wait(barrier, 67)

    for j in order:
        for q in range(2):
            for c in range(2):
                copy(slab_of(2 * j + c, q), slab_place(j, q, core), diag_send.at[q], diag_recv.at[q, j // 2],
                     beside(1 if j < 4 else -1, c)).start()
            copy(slab_of(2 * j + 1 - core, q), slab_place(j, q, core), diag_send.at[q], diag_recv.at[q, j // 2],
                 mate).start()

    def panels(first, last):
        for i in range(first, last):
            k, row = panel_place(i, 2 * i + 2)
            piece = factor.at[2 * i + 2:32, :, 256 * i:256 * i + 256]
            place = pan.at[k, row:row + 30 - 2 * i, core]
            group = (i > 1) + (i > 3) + (i > 7)
            pltpu.make_async_copy(piece, place, pan_recv.at[group]).start()
            copy(piece, place, pan_send, pan_recv.at[group], mate).start()

    panels(0, 4)

    def send_right_side(to):
        for c in range(2):
            copy(sb.at[2 * to + c], rhs.at[2 * blk + core], a_send, a_recv.at[blk // 2],
                 {"blk": to, "sub": 2 * xl + c}).start()

    def cross(k, _):
        send_right_side((1 - hi) * 16 + (blk + k) % 16)
        return 0

    def spread(k, _):
        send_right_side(hi * 16 + (blk + k) % 16)
        return 0

    @pl.when(hi == 0)
    def _():
        lax.fori_loop(0, 16, cross, 0)

    lax.fori_loop(1, 16, spread, 0)
    copy(sb.at[2 * blk + 1 - core], rhs.at[2 * blk + core], a_send, a_recv.at[blk // 2], mate).start()
    rhs[2 * blk + core] = sb[2 * blk + core]

    panels(4, 15)

    pltpu.make_async_copy(slab_hbm, slab, in_local).wait()
    for t in range(3):
        pairs[:, 2048 * t:2048 * t + 2048] = occ[slab[0] * NOCC + t] - virt[...]

    row = lax.broadcasted_iota(jnp.int32, (128, 128), 0)
    col = lax.broadcasted_iota(jnp.int32, (128, 128), 1)

    def invert(turn, _):
        g = (turn % 2) * 2 + turn // 2
        for q in range(2):
            piece = blocks.at[pl.ds(2 * g, 2), q, :, :, :, 0:128 * (q + 1)]
            pltpu.make_async_copy(piece, piece, diag_recv.at[q, g]).wait()

        @pl.when((turn == 2) & (hi == 1))
        def _():
            lax.fori_loop(0, 16, cross, 0)

        def block(n):
            q = n % 2
            return blocks[2 * g + n // 2, q, :, :, :, 128 * q:128 * q + 128].reshape(128, 128)

        for n in range(4):
            value = block(n)
            diag = jnp.where(row == col, value, 0.0)
            down = 1.0 / jnp.sum(diag, axis=1, keepdims=True)
            across = 1.0 / jnp.sum(diag, axis=0, keepdims=True)
            below = (row == col + 1) & (row % 2 == 1)
            half_inv[4 * g + n] = jnp.where(row == col, down, 0.0) - jnp.where(below, value * down * across, 0.0)
        size = 2
        while size < 128:
            below = (row // size == col // size + 1) & (row // (2 * size) == col // (2 * size))
            for n in range(4):
                part = jnp.where(below, block(n), 0.0)
                half_tmp[n] = dot3(split(part), split(half_inv[4 * g + n]), NN)
            for n in range(4):
                now = half_inv[4 * g + n]
                half_inv[4 * g + n] = now - dot3(split(now), split(half_tmp[n]), NN)
            size *= 2
        for n in range(2):
            lower = blocks[2 * g + n, 1, :, :, :, 0:128].reshape(128, 128)
            half_tmp[n] = dot3(split(lower), split(half_inv[4 * g + 2 * n]), NN)
        for n in range(2):
            i = 2 * (2 * g + n) + core
            dinv[i, 0:128, 0:128] = half_inv[4 * g + 2 * n]
            dinv[i, 128:256, 128:256] = half_inv[4 * g + 2 * n + 1]
            dinv[i, 0:128, 128:256] = jnp.zeros((128, 128), F32)
            dinv[i, 128:256, 0:128] = -dot3(split(half_inv[4 * g + 2 * n + 1]), split(half_tmp[n]), NN)
        for n in range(2):
            i = 2 * (2 * g + n) + core
            copy(dinv.at[i], dinv.at[i], inv_send, inv_recv.at[g], mate).start()
        return 0

    lax.fori_loop(0, 4, invert, 0)

    def offer(i, value):
        gbuf[i, :, xl] = value.reshape(2, 64, 96)
        copy(gbuf.at[i, :, xl], gbuf.at[i, :, xl], g_send, g_recv.at[i], peer).start()

    def right_side(i):
        for count, here in ((3, blk // 2 == i), (4, blk // 2 != i)):
            @pl.when(here)
            def _(count=count):
                piece = rhs.at[0:count]
                copy(piece, piece, a_send, a_recv.at[i], mate).wait_recv()

        packed = rhs[pl.ds(4 * i, 4)]
        return jnp.concatenate([packed[:, :, 96 * m:96 * m + 96] for m in range(4)], axis=1).reshape(128, 96)

    def factor_part(i, t):
        k, at = panel_place(i, 2 * t)
        return split(pan[k, pl.ds(at, 2)].reshape(128, 256))

    def own_out(i):
        half = rowbuf.at[y, i, 1 - core]
        copy(half, half, x_send, x_recv.at[i], mate).wait_recv()
        for k, offset in enumerate((1, -1)):
            copy(rowbuf.at[y, i], rowbuf.at[y, i], y_send, y_recv.at[k, i], y_at(offset)).start()

        @pl.when(same)
        def _():
            for k, offset in enumerate((1, -1)):
                copy(rowbuf.at[y, i], colbuf.at[z, i], z_send, z_recv.at[k, i], z_at(offset)).start()
            colbuf[z, i] = rowbuf[y, i]

        @pl.when(jnp.logical_not(same))
        def _():
            copy(rowbuf.at[y, i], colbuf.at[z, i], s_send, s_recv.at[i], swap).start()

    def swapped_out(i):
        @pl.when(jnp.logical_not(same))
        def _():
            copy(colbuf.at[z, i], colbuf.at[z, i], s_send, s_recv.at[i], swap).wait_recv()
            for k, offset in enumerate((1, -1)):
                copy(colbuf.at[z, i], colbuf.at[z, i], z_send, z_recv.at[k, i], z_at(offset)).start()

    def got(buf, send, recv, place, k, i):
        copy(buf.at[place, i], buf.at[place, i], send, recv.at[k, i], mate).wait_recv()

    def forward(buf, send, recv, me, at, i):
        odd = i % 2
        step = 1 - 2 * odd
        src = (me - step + 4) % 4
        got(buf, send, recv, src, odd, i)
        copy(buf.at[src, i], buf.at[src, i], send, recv.at[2, i], at(step)).start()

    def forward_y(i):
        forward(rowbuf, y_send, y_recv, y, y_at, i)

    def forward_z(i):
        forward(colbuf, z_send, z_recv, z, z_at, i)

    def whole(buf, k, c):
        return jnp.concatenate([buf[k, 2 * c].reshape(192, 128), buf[k, 2 * c + 1].reshape(192, 128)], axis=1)

    def arrived(c):
        for odd in range(2):
            i = 2 * c + odd
            step = 1 - 2 * odd
            got(rowbuf, y_send, y_recv, (y + step + 4) % 4, 1 - odd, i)
            got(colbuf, z_send, z_recv, (z + step + 4) % 4, 1 - odd, i)
            got(rowbuf, y_send, y_recv, (y + 2) % 4, 2, i)
            got(colbuf, z_send, z_recv, (z + 2) % 4, 2, i)
        for k in range(4):
            cols[k * 192:k * 192 + 192] = whole(colbuf, k, c)
        for m in range(6):
            high, low = split(cols[128 * m:128 * m + 128].T)
            colh[:, 128 * m:128 * m + 128] = high
            coll[:, 128 * m:128 * m + 128] = low

    def product_rows(c, k):
        acc[k] = acc[k] + dot3(split(whole(rowbuf, k, c)), (colh[...], coll[...]), NN)

    def product_half(c, half):
        def part(k, _):
            product_rows(c, k)
            return 0

        lax.fori_loop(2 * half, 2 * half + 2, part, 0)

    acc[...] = jnp.zeros_like(acc)
    known[...] = jnp.zeros_like(known)
    offer(0, right_side(0))

    def round_of(i, _):
        for group, (at, many, wide) in enumerate(((0, 2, 29), (2, 2, 25), (4, 4, 19), (8, 4, 14))):
            @pl.when(i == at)
            def _(group=group, many=many, wide=wide):
                piece = pan.at[0:many, 0:wide]
                pltpu.make_async_copy(piece, piece, pan_recv.at[group]).wait()

        @pl.when(i % 4 == 0)
        def _():
            copy(dinv.at[0:2], dinv.at[0:2], inv_send, inv_recv.at[i // 4], mate).wait_recv()

        inverse = split(dinv[i])

        @pl.when(i > 0)
        def _():
            def later(u, _):
                k, at = panel_place(i - 1, 4 * u)
                part = split(pan[k, pl.ds(at, 4)].reshape(256, 256))
                term = dot3(part, (xh[...], xlow[...]), NN)
                rows = pl.ds(8 * u, 8)
                known[rows] = known[rows] + term.reshape(8, 32, 96)
                return 0

            lax.fori_loop((i + 1) // 2, 8, later, 0)
            own_out(i - 1)

        @pl.when(i > 1)
        def _():
            swapped_out(i - 2)

        @pl.when((i > 5) & (i % 2 == 0))
        def _():
            arrived((i - 6) // 2)

        @pl.when(i > 5)
        def _():
            product_half((i - 6) // 2, i % 2)

        @pl.when(i > 1)
        def _():
            forward_y(i - 2)

        @pl.when(i > 2)
        def _():
            forward_z(i - 3)

        @pl.when(i < 15)
        def _():
            rest = right_side(i + 1) - known[pl.ds(4 * i + 4, 4)].reshape(128, 96)
            known[pl.ds(4 * i + 4, 4)] = rest.reshape(4, 32, 96)

        other = gbuf.at[i, :, 1 - xl]
        copy(other, other, g_send, g_recv.at[i], peer).wait_recv()
        solved = dot3(inverse, split(gbuf[i].reshape(256, 96)), NN)
        high, low = split(solved)
        xh[...] = high
        xlow[...] = low

        @pl.when(i < 15)
        def _():
            term = dot3(factor_part(i, i + 1), (high, low), NN)
            offer(i + 1, known[pl.ds(4 * i + 4, 4)].reshape(128, 96) - term)

        xbuf[...] = solved.reshape(2, 128, 96)
        tx[i] = xbuf[1 - core].T
        copy(tx.at[i], rowbuf.at[y, i, core], x_send, x_recv.at[i], mate).start()
        rowbuf[y, i, core] = xbuf[core].T
        return 0

    lax.fori_loop(0, 16, round_of, 0)

    own_out(15)
    swapped_out(14)
    forward_y(14)
    forward_z(13)
    swapped_out(15)
    arrived(5)
    product_half(5, 0)
    forward_z(14)
    forward_y(15)
    product_half(5, 1)
    arrived(6)
    product_half(6, 0)
    forward_z(15)
    product_half(6, 1)
    arrived(7)

    mine = pl.ds(pl.multiple_of(core * 384, 128), 384)
    theirs = pl.ds(pl.multiple_of((1 - core) * 384, 128), 384)
    order = ((y + 2) % 4, (y + 1) % 4, (y + 3) % 4, y)

    def trade(n):
        k = order[n]
        return copy(acc.at[k, :, theirs], exch.at[k], t_send.at[n], t_recv.at[n], mate)

    def finish(n):
        product_rows(7, order[n])
        trade(n).start()

    def summed(n):
        trade(n).wait_recv()
        k = order[n]
        total[k] = acc[k, :, mine] + exch[k]

    finish(0)
    finish(1)
    summed(0)
    hops = []
    for at, offset in enumerate((1, -1)):
        hops.append(copy(total.at[order[0], 96 * at:96 * at + 96], relay.at[at],
                         e_send.at[at], e_recv.at[at], y_at(offset)))
        hops[-1].start()
    for n, offset in ((1, 1), (2, -1)):
        finish(n + 1)
        summed(n)
        hops.append(copy(total.at[order[n]], final.at[y], e_send.at[n + 1], e_recv.at[n + 1], y_at(offset)))
        hops[-1].start()
    for at, offset in enumerate((1, -1)):
        copy(relay.at[at], relay.at[at], e_send.at[at], e_recv.at[at], mate).wait_recv()
        src = (y - offset + 4) % 4
        hops.append(copy(relay.at[at], final.at[src, 96 * at:96 * at + 96],
                         e_send.at[4 + at], e_recv.at[4 + at], y_at(offset)))
        hops[-1].start()
    summed(3)
    final[y] = total[y]
    for n, offset in ((1, 1), (2, -1)):
        src = (y - offset + 4) % 4
        copy(final.at[src], final.at[src], e_send.at[n + 1], e_recv.at[n + 1], mate).wait_recv()
    src = (y + 2) % 4
    for at in range(2):
        piece = final.at[src, 96 * at:96 * at + 96]
        copy(piece, piece, e_send.at[4 + at], e_recv.at[4 + at], mate).wait_recv()
    window = pairs[:, pl.ds(pl.multiple_of((blk * 192) // 128 * 128, 128), 256)]
    across = jnp.where(blk % 2 == 1, window[:, 64:256], window[:, 0:192])
    line = lax.broadcasted_iota(jnp.int32, (192, 192), 0)
    lane = lax.broadcasted_iota(jnp.int32, (192, 192), 1)
    down = jnp.sum(jnp.where(line == lane, across, 0.0), axis=1, keepdims=True)
    for k in range(2):
        wide = pairs[:, pl.ds(pl.multiple_of(sub * 1536 + k * 768, 128), 768)]
        sums = jnp.concatenate([final[q, :, k * 192:k * 192 + 192] for q in range(4)], axis=1)
        out[:, k * 768:k * 768 + 768] = sums / (down + wide)
    for hop in hops:
        hop.wait_send()
    for n in range(4):
        trade(n).wait_send()

    piece = rowbuf.at[0:3]
    copy(piece, piece, y_send, y_recv.at[0, 0], mate).wait_send()
    copy(piece, piece, z_send, z_recv.at[0, 0], mate).wait_send()

    @pl.when(jnp.logical_not(same))
    def _():
        copy(rowbuf.at[0], rowbuf.at[0], s_send, s_recv.at[0], swap).wait_send()

    piece = pan.at[:, 0:30, core]
    copy(piece, piece, pan_send, pan_recv.at[0], mate).wait_send()
    piece = gbuf.at[:, :, xl]
    copy(piece, piece, g_send, g_recv.at[0], peer).wait_send()
    for q in range(2):
        piece = blocks.at[0:6, q, :, :, :, 0:128 * (q + 1)]
        copy(piece, piece, diag_send.at[q], diag_recv.at[q, 0], mate).wait_send()
    copy(sb.at[0:63], sb.at[0:63], a_send, a_recv.at[0], mate).wait_send()
    copy(dinv.at[0:8], dinv.at[0:8], inv_send, inv_recv.at[0], mate).wait_send()
    copy(tx, tx, x_send, x_recv.at[0], mate).wait_send()


def amplitude_block(integrals, slots, factor, occ, slab, virt):
    dma = pltpu.SemaphoreType.DMA
    vmem = pl.BlockSpec(memory_space=pltpu.VMEM)
    hbm = pl.BlockSpec(memory_space=pltpu.HBM)
    return pl.pallas_call(
        fused_kernel,
        out_shape=jax.ShapeDtypeStruct((192, 1536), F32),
        in_specs=[vmem, vmem, hbm, pl.BlockSpec(memory_space=pltpu.SMEM), hbm, vmem],
        out_specs=vmem,
        scratch_shapes=[
            pltpu.SMEM((1,), jnp.int32),
            pltpu.VMEM((8, 34, 2, 32, 256), F32),
            pltpu.VMEM((8, 2, 2, 2, 32, 256), F32),
            pltpu.VMEM((16, 128, 128), F32),
            pltpu.VMEM((4, 128, 128), F32),
            pltpu.VMEM((16, 256, 256), F32),
            pltpu.VMEM((64, 8, 384), F32),
            pltpu.VMEM((64, 8, 384), F32),
            pltpu.VMEM((64, 32, 96), F32),
            pltpu.VMEM((16, 2, 2, 64, 96), F32),
            pltpu.VMEM((256, 96), BF16),
            pltpu.VMEM((256, 96), BF16),
            pltpu.VMEM((2, 128, 96), F32),
            pltpu.VMEM((16, 96, 128), F32),
            pltpu.VMEM((4, 16, 2, 96, 128), F32),
            pltpu.VMEM((4, 16, 2, 96, 128), F32),
            pltpu.VMEM((4, 192, 768), F32),
            pltpu.VMEM((768, 256), F32),
            pltpu.VMEM((256, 768), BF16),
            pltpu.VMEM((256, 768), BF16),
            pltpu.VMEM((1, 6144), F32),
            pltpu.VMEM((4, 192, 384), F32),
            pltpu.VMEM((4, 192, 384), F32),
            pltpu.VMEM((4, 192, 384), F32),
            pltpu.VMEM((2, 96, 384), F32),
            dma, dma, dma((4,)), dma((2,)), dma((2, 4)), dma, dma((16,)), dma, dma((4,)),
            dma, dma((16,)), dma, dma((16,)),
            dma, dma((3, 16)), dma, dma((3, 16)), dma, dma((16,)),
            dma((4,)), dma((4,)), dma((6,)), dma((6,)),
        ],
        compiler_params=pltpu.CompilerParams(
            collective_id=0, has_side_effects=True, vmem_limit_bytes=52 * 2**20),
    )(integrals, slots, factor, occ, slab, virt)


def shards(integrals, slot_order, factor_rows, occ_energy, slab_index, virt_energy):
    def stay(value):
        return pltpu.with_memory_space_constraint(value, pltpu.HBM)

    return amplitude_block(stay(integrals[0, 0]), stay(slot_order[0]), stay(factor_rows[:, 0]),
                           stay(occ_energy), slab_index, stay(virt_energy[None]))


def solution(mesh):
    in_specs = (
        P("blk", "sub", None, None),
        P("blk", "sub", None),
        P(None, "sub", None, None),
        P(),
        P(),
        P(),
    )
    out_specs = P("blk", "sub")
    return jax.shard_map(shards, mesh=mesh, in_specs=in_specs, out_specs=out_specs, check_vma=False)
```

```python
import functools

import jax
import jax.numpy as jnp
from jax import lax
from jax.experimental import pallas as pl
from jax.experimental.pallas import tpu as pltpu
from jax.sharding import PartitionSpec as P

NOCC = 3
F32 = jnp.float32
BF16 = jnp.bfloat16
MESH = pl.DeviceIdType.MESH
NN = (((1,), (0,)), ((), ()))
NT = (((1,), (1,)), ((), ()))


def split(x):
    high = x.astype(BF16)
    return high, (x - high.astype(F32)).astype(BF16)


def dot3(a, b, dims):
    def one(p, q):
        return lax.dot_general(p, q, dims, preferred_element_type=F32)

    return one(a[0], b[0]) + (one(a[0], b[1]) + one(a[1], b[0]))


def copy(src, dst, send, recv, who):
    return pltpu.make_async_remote_copy(
        src_ref=src, dst_ref=dst, send_sem=send, recv_sem=recv,
        device_id=who, device_id_type=MESH)


def panel_place(i, r):
    if isinstance(i, int):
        return (i, r - 2 * i) if i < 8 else (15 - i, r + 2)
    return jnp.where(i < 8, i, 15 - i), jnp.where(i < 8, r - 2 * i, r + 2)


def fused_kernel(integrals, slots, factor, occ, slab_hbm, virt, out, slab, pan, blocks, half_inv, half_tmp, dinv, sb, rhs, known, gbuf,
                 xh, xlow, xbuf, tx, rowbuf, colbuf, acc, cols, colh, coll, pairs, exch, total, final, relay,
                 in_local, pan_send, pan_recv, diag_send, diag_recv, a_send, a_recv,
                 inv_send, inv_recv, g_send, g_recv, x_send, x_recv,
                 y_send, y_recv, z_send, z_recv, s_send, s_recv, t_send, t_recv, e_send, e_recv):
    blk, sub = lax.axis_index("blk"), lax.axis_index("sub")
    hi = blk // 16
    xl, core = sub // 2, sub % 2
    x = 2 * hi + xl
    y, z = blk % 4, (blk // 4) % 4
    same = hi == xl
    mate = {"blk": blk, "sub": sub + 1 - 2 * core}
    peer = {"blk": blk, "sub": sub + 2 - 4 * xl}

    def beside(offset, to_core):
        other = (x + offset + 4) % 4
        return {"blk": blk + (other // 2 - hi) * 16, "sub": (other % 2) * 2 + to_core}

    def y_at(offset):
        return {"blk": blk - y + (y + offset + 4) % 4, "sub": sub}

    def z_at(offset):
        return {"blk": blk - 4 * z + 4 * ((z + offset + 4) % 4), "sub": sub}

    swap = {"blk": blk + (1 - 2 * hi) * 16, "sub": sub + (1 - 2 * xl) * 2}

    pltpu.make_async_copy(slab_hbm, slab, in_local).start()
    barrier = pltpu.get_barrier_semaphore()

    def greet(k, _):
        for c in range(2):
            pl.semaphore_signal(barrier, inc=1, device_id_type=MESH,
                                device_id={"blk": (blk + k) % 32, "sub": 2 * xl + c})
        return 0

    lax.fori_loop(1, 32, greet, 0)
    pl.semaphore_signal(barrier, inc=1, device_id=mate, device_id_type=MESH)
    for offset in (1, -1):
        for c in range(2):
            pl.semaphore_signal(barrier, inc=1, device_id=beside(offset, c), device_id_type=MESH)

    def slab_of(i, q):
        wide = 128 * (q + 1)
        return factor.at[2 * i + q, :, pl.ds(pl.multiple_of(256 * i, 256), wide)]

    def slab_place(j, q, at_core):
        return blocks.at[j, q, xl, at_core, :, 0:128 * (q + 1)]

    order = (0, 1, 4, 5, 2, 3, 6, 7)
    for j in order:
        for q in range(2):
            pltpu.make_async_copy(slab_of(2 * j + core, q), slab_place(j, q, core), diag_recv.at[q, j // 2]).start()

    onehot = (slots[...] == lax.broadcasted_iota(jnp.int32, (32, 32), 0)).astype(F32).astype(BF16)

    def pick(v):
        return lax.dot_general(onehot, v, NN, preferred_element_type=F32)

    for g in range(16):
        value = integrals[:, 384 * g:384 * g + 384]
        high = value.astype(BF16)
        rest = value - high.astype(F32)
        mid = rest.astype(BF16)
        low = (rest - mid.astype(F32)).astype(BF16)
        picked = pick(high) + (pick(mid) + pick(low))
        for k in range(4):
            sb[4 * g + k] = jnp.concatenate(
                [picked[8 * m:8 * m + 8, 96 * k:96 * k + 96] for m in range(4)], axis=1)

    pl.semaphore_wait(barrier, 67)

    for j in order:
        for q in range(2):
            for c in range(2):
                copy(slab_of(2 * j + c, q), slab_place(j, q, core), diag_send.at[q], diag_recv.at[q, j // 2],
                     beside(1 if j < 4 else -1, c)).start()
            copy(slab_of(2 * j + 1 - core, q), slab_place(j, q, core), diag_send.at[q], diag_recv.at[q, j // 2],
                 mate).start()

    def panels(first, last):
        for i in range(first, last):
            k, row = panel_place(i, 2 * i + 2)
            piece = factor.at[2 * i + 2:32, :, 256 * i:256 * i + 256]
            place = pan.at[k, row:row + 30 - 2 * i, core]
            group = (i > 1) + (i > 3) + (i > 7)
            pltpu.make_async_copy(piece, place, pan_recv.at[group]).start()
            copy(piece, place, pan_send, pan_recv.at[group], mate).start()

    panels(0, 4)

    def send_right_side(to):
        for c in range(2):
            copy(sb.at[2 * to + c], rhs.at[2 * blk + core], a_send, a_recv.at[blk // 2],
                 {"blk": to, "sub": 2 * xl + c}).start()

    def cross(k, _):
        send_right_side((1 - hi) * 16 + (blk + k) % 16)
        return 0

    def spread(k, _):
        send_right_side(hi * 16 + (blk + k) % 16)
        return 0

    @pl.when(hi == 0)
    def _():
        lax.fori_loop(0, 16, cross, 0)

    lax.fori_loop(1, 16, spread, 0)
    copy(sb.at[2 * blk + 1 - core], rhs.at[2 * blk + core], a_send, a_recv.at[blk // 2], mate).start()
    rhs[2 * blk + core] = sb[2 * blk + core]

    panels(4, 15)

    pltpu.make_async_copy(slab_hbm, slab, in_local).wait()
    for t in range(3):
        pairs[:, 2048 * t:2048 * t + 2048] = occ[slab[0] * NOCC + t] - virt[...]

    row = lax.broadcasted_iota(jnp.int32, (128, 128), 0)
    col = lax.broadcasted_iota(jnp.int32, (128, 128), 1)

    def invert(turn, _):
        g = (turn % 2) * 2 + turn // 2
        for q in range(2):
            piece = blocks.at[pl.ds(2 * g, 2), q, :, :, :, 0:128 * (q + 1)]
            pltpu.make_async_copy(piece, piece, diag_recv.at[q, g]).wait()

        @pl.when((turn == 2) & (hi == 1))
        def _():
            lax.fori_loop(0, 16, cross, 0)

        def block(n):
            q = n % 2
            return blocks[2 * g + n // 2, q, :, :, :, 128 * q:128 * q + 128].reshape(128, 128)

        for n in range(4):
            value = block(n)
            diag = jnp.where(row == col, value, 0.0)
            down = 1.0 / jnp.sum(diag, axis=1, keepdims=True)
            across = 1.0 / jnp.sum(diag, axis=0, keepdims=True)
            below = (row == col + 1) & (row % 2 == 1)
            half_inv[4 * g + n] = jnp.where(row == col, down, 0.0) - jnp.where(below, value * down * across, 0.0)
        size = 2
        while size < 128:
            below = (row // size == col // size + 1) & (row // (2 * size) == col // (2 * size))
            for n in range(4):
                part = jnp.where(below, block(n), 0.0)
                half_tmp[n] = dot3(split(part), split(half_inv[4 * g + n]), NN)
            for n in range(4):
                now = half_inv[4 * g + n]
                half_inv[4 * g + n] = now - dot3(split(now), split(half_tmp[n]), NN)
            size *= 2
        for n in range(2):
            lower = blocks[2 * g + n, 1, :, :, :, 0:128].reshape(128, 128)
            half_tmp[n] = dot3(split(lower), split(half_inv[4 * g + 2 * n]), NN)
        for n in range(2):
            i = 2 * (2 * g + n) + core
            dinv[i, 0:128, 0:128] = half_inv[4 * g + 2 * n]
            dinv[i, 128:256, 128:256] = half_inv[4 * g + 2 * n + 1]
            dinv[i, 0:128, 128:256] = jnp.zeros((128, 128), F32)
            dinv[i, 128:256, 0:128] = -dot3(split(half_inv[4 * g + 2 * n + 1]), split(half_tmp[n]), NN)
        for n in range(2):
            i = 2 * (2 * g + n) + core
            copy(dinv.at[i], dinv.at[i], inv_send, inv_recv.at[g], mate).start()
        return 0

    lax.fori_loop(0, 4, invert, 0)

    def offer(i, value):
        gbuf[i, :, xl] = value.reshape(2, 64, 96)
        copy(gbuf.at[i, :, xl], gbuf.at[i, :, xl], g_send, g_recv.at[i], peer).start()

    def right_side(i):
        for count, here in ((3, blk // 2 == i), (4, blk // 2 != i)):
            @pl.when(here)
            def _(count=count):
                piece = rhs.at[0:count]
                copy(piece, piece, a_send, a_recv.at[i], mate).wait_recv()

        packed = rhs[pl.ds(4 * i, 4)]
        return jnp.concatenate([packed[:, :, 96 * m:96 * m + 96] for m in range(4)], axis=1).reshape(128, 96)

    def factor_part(i, t):
        k, at = panel_place(i, 2 * t)
        return split(pan[k, pl.ds(at, 2)].reshape(128, 256))

    def own_out(i):
        half = rowbuf.at[y, i, 1 - core]
        copy(half, half, x_send, x_recv.at[i], mate).wait_recv()
        for k, offset in enumerate((1, -1)):
            copy(rowbuf.at[y, i], rowbuf.at[y, i], y_send, y_recv.at[k, i], y_at(offset)).start()

        @pl.when(same)
        def _():
            for k, offset in enumerate((1, -1)):
                copy(rowbuf.at[y, i], colbuf.at[z, i], z_send, z_recv.at[k, i], z_at(offset)).start()
            colbuf[z, i] = rowbuf[y, i]

        @pl.when(jnp.logical_not(same))
        def _():
            copy(rowbuf.at[y, i], colbuf.at[z, i], s_send, s_recv.at[i], swap).start()

    def swapped_out(i):
        @pl.when(jnp.logical_not(same))
        def _():
            copy(colbuf.at[z, i], colbuf.at[z, i], s_send, s_recv.at[i], swap).wait_recv()
            for k, offset in enumerate((1, -1)):
                copy(colbuf.at[z, i], colbuf.at[z, i], z_send, z_recv.at[k, i], z_at(offset)).start()

    def got(buf, send, recv, place, k, i):
        copy(buf.at[place, i], buf.at[place, i], send, recv.at[k, i], mate).wait_recv()

    def forward(buf, send, recv, me, at, i):
        odd = i % 2
        step = 1 - 2 * odd
        src = (me - step + 4) % 4
        got(buf, send, recv, src, odd, i)
        copy(buf.at[src, i], buf.at[src, i], send, recv.at[2, i], at(step)).start()

    def forward_y(i):
        forward(rowbuf, y_send, y_recv, y, y_at, i)

    def forward_z(i):
        forward(colbuf, z_send, z_recv, z, z_at, i)

    def whole(buf, k, c):
        return jnp.concatenate([buf[k, 2 * c].reshape(192, 128), buf[k, 2 * c + 1].reshape(192, 128)], axis=1)

    def landed(c, odds):
        for odd in odds:
            i = 2 * c + odd
            step = 1 - 2 * odd
            got(rowbuf, y_send, y_recv, (y + step + 4) % 4, 1 - odd, i)
            got(colbuf, z_send, z_recv, (z + step + 4) % 4, 1 - odd, i)
            got(rowbuf, y_send, y_recv, (y + 2) % 4, 2, i)
            got(colbuf, z_send, z_recv, (z + 2) % 4, 2, i)

    def arrived(c):
        landed(c, (0, 1))
        for k in range(4):
            cols[k * 192:k * 192 + 192] = whole(colbuf, k, c)
        for m in range(6):
            high, low = split(cols[128 * m:128 * m + 128].T)
            colh[:, 128 * m:128 * m + 128] = high
            coll[:, 128 * m:128 * m + 128] = low

    def product_rows(c, k):
        acc[k] = acc[k] + dot3(split(whole(rowbuf, k, c)), (colh[...], coll[...]), NN)

    def arrived_round(i):
        landed(i // 2, (i % 2,))
        for k in range(4):
            cols[k * 192:k * 192 + 192, 0:128] = colbuf[k, i].reshape(192, 128)
        for m in range(6):
            high, low = split(cols[128 * m:128 * m + 128, 0:128].T)
            colh[0:128, 128 * m:128 * m + 128] = high
            coll[0:128, 128 * m:128 * m + 128] = low

    def round_rows(i, k):
        acc[k] = acc[k] + dot3(split(rowbuf[k, i].reshape(192, 128)), (colh[0:128], coll[0:128]), NN)

    def product_half(c, half):
        def part(k, _):
            product_rows(c, k)
            return 0

        lax.fori_loop(2 * half, 2 * half + 2, part, 0)

    acc[...] = jnp.zeros_like(acc)
    known[...] = jnp.zeros_like(known)
    offer(0, right_side(0))

    def round_of(i, _):
        for group, (at, many, wide) in enumerate(((0, 2, 29), (2, 2, 25), (4, 4, 19), (8, 4, 14))):
            @pl.when(i == at)
            def _(group=group, many=many, wide=wide):
                piece = pan.at[0:many, 0:wide]
                pltpu.make_async_copy(piece, piece, pan_recv.at[group]).wait()

        @pl.when(i % 4 == 0)
        def _():
            copy(dinv.at[0:2], dinv.at[0:2], inv_send, inv_recv.at[i // 4], mate).wait_recv()

        inverse = split(dinv[i])

        @pl.when(i > 0)
        def _():
            def later(u, _):
                k, at = panel_place(i - 1, 4 * u)
                part = split(pan[k, pl.ds(at, 4)].reshape(256, 256))
                term = dot3(part, (xh[...], xlow[...]), NN)
                rows = pl.ds(8 * u, 8)
                known[rows] = known[rows] + term.reshape(8, 32, 96)
                return 0

            lax.fori_loop((i + 1) // 2, 8, later, 0)
            own_out(i - 1)

        @pl.when(i > 1)
        def _():
            swapped_out(i - 2)

        @pl.when((i > 5) & (i % 2 == 0))
        def _():
            arrived((i - 6) // 2)

        @pl.when(i > 5)
        def _():
            product_half((i - 6) // 2, i % 2)

        @pl.when(i > 1)
        def _():
            forward_y(i - 2)

        @pl.when(i > 2)
        def _():
            forward_z(i - 3)

        @pl.when(i < 15)
        def _():
            rest = right_side(i + 1) - known[pl.ds(4 * i + 4, 4)].reshape(128, 96)
            known[pl.ds(4 * i + 4, 4)] = rest.reshape(4, 32, 96)

        other = gbuf.at[i, :, 1 - xl]
        copy(other, other, g_send, g_recv.at[i], peer).wait_recv()
        solved = dot3(inverse, split(gbuf[i].reshape(256, 96)), NN)
        high, low = split(solved)
        xh[...] = high
        xlow[...] = low

        @pl.when(i < 15)
        def _():
            term = dot3(factor_part(i, i + 1), (high, low), NN)
            offer(i + 1, known[pl.ds(4 * i + 4, 4)].reshape(128, 96) - term)

        xbuf[...] = solved.reshape(2, 128, 96)
        tx[i] = xbuf[1 - core].T
        copy(tx.at[i], rowbuf.at[y, i, core], x_send, x_recv.at[i], mate).start()
        rowbuf[y, i, core] = xbuf[core].T
        return 0

    lax.fori_loop(0, 16, round_of, 0)

    own_out(15)
    swapped_out(14)
    forward_y(14)
    forward_z(13)
    swapped_out(15)
    arrived(5)
    product_half(5, 0)
    forward_z(14)
    forward_y(15)
    product_half(5, 1)
    arrived(6)
    product_half(6, 0)
    forward_z(15)
    product_half(6, 1)
    arrived_round(14)

    def early(k, _):
        round_rows(14, k)
        return 0

    lax.fori_loop(0, 4, early, 0)
    arrived_round(15)

    mine = pl.ds(pl.multiple_of(core * 384, 128), 384)
    theirs = pl.ds(pl.multiple_of((1 - core) * 384, 128), 384)
    order = ((y + 2) % 4, (y + 1) % 4, (y + 3) % 4, y)

    def trade(n):
        k = order[n]
        return copy(acc.at[k, :, theirs], exch.at[k], t_send.at[n], t_recv.at[n], mate)

    def finish(n):
        round_rows(15, order[n])
        trade(n).start()

    def summed(n):
        trade(n).wait_recv()
        k = order[n]
        total[k] = acc[k, :, mine] + exch[k]

    finish(0)
    finish(1)
    summed(0)
    hops = []
    for at, offset in enumerate((1, -1)):
        hops.append(copy(total.at[order[0], 96 * at:96 * at + 96], relay.at[at],
                         e_send.at[at], e_recv.at[at], y_at(offset)))
        hops[-1].start()
    for n, offset in ((1, 1), (2, -1)):
        finish(n + 1)
        summed(n)
        hops.append(copy(total.at[order[n]], final.at[y], e_send.at[n + 1], e_recv.at[n + 1], y_at(offset)))
        hops[-1].start()
    for at, offset in enumerate((1, -1)):
        copy(relay.at[at], relay.at[at], e_send.at[at], e_recv.at[at], mate).wait_recv()
        src = (y - offset + 4) % 4
        hops.append(copy(relay.at[at], final.at[src, 96 * at:96 * at + 96],
                         e_send.at[4 + at], e_recv.at[4 + at], y_at(offset)))
        hops[-1].start()
    summed(3)
    final[y] = total[y]
    for n, offset in ((1, 1), (2, -1)):
        src = (y - offset + 4) % 4
        copy(final.at[src], final.at[src], e_send.at[n + 1], e_recv.at[n + 1], mate).wait_recv()
    src = (y + 2) % 4
    for at in range(2):
        piece = final.at[src, 96 * at:96 * at + 96]
        copy(piece, piece, e_send.at[4 + at], e_recv.at[4 + at], mate).wait_recv()
    window = pairs[:, pl.ds(pl.multiple_of((blk * 192) // 128 * 128, 128), 256)]
    across = jnp.where(blk % 2 == 1, window[:, 64:256], window[:, 0:192])
    line = lax.broadcasted_iota(jnp.int32, (192, 192), 0)
    lane = lax.broadcasted_iota(jnp.int32, (192, 192), 1)
    down = jnp.sum(jnp.where(line == lane, across, 0.0), axis=1, keepdims=True)
    for k in range(2):
        wide = pairs[:, pl.ds(pl.multiple_of(sub * 1536 + k * 768, 128), 768)]
        sums = jnp.concatenate([final[q, :, k * 192:k * 192 + 192] for q in range(4)], axis=1)
        out[:, k * 768:k * 768 + 768] = sums / (down + wide)
    for hop in hops:
        hop.wait_send()
    for n in range(4):
        trade(n).wait_send()

    piece = rowbuf.at[0:3]
    copy(piece, piece, y_send, y_recv.at[0, 0], mate).wait_send()
    copy(piece, piece, z_send, z_recv.at[0, 0], mate).wait_send()

    @pl.when(jnp.logical_not(same))
    def _():
        copy(rowbuf.at[0], rowbuf.at[0], s_send, s_recv.at[0], swap).wait_send()

    piece = pan.at[:, 0:30, core]
    copy(piece, piece, pan_send, pan_recv.at[0], mate).wait_send()
    piece = gbuf.at[:, :, xl]
    copy(piece, piece, g_send, g_recv.at[0], peer).wait_send()
    for q in range(2):
        piece = blocks.at[0:6, q, :, :, :, 0:128 * (q + 1)]
        copy(piece, piece, diag_send.at[q], diag_recv.at[q, 0], mate).wait_send()
    copy(sb.at[0:63], sb.at[0:63], a_send, a_recv.at[0], mate).wait_send()
    copy(dinv.at[0:8], dinv.at[0:8], inv_send, inv_recv.at[0], mate).wait_send()
    copy(tx, tx, x_send, x_recv.at[0], mate).wait_send()


def amplitude_block(integrals, slots, factor, occ, slab, virt):
    dma = pltpu.SemaphoreType.DMA
    vmem = pl.BlockSpec(memory_space=pltpu.VMEM)
    hbm = pl.BlockSpec(memory_space=pltpu.HBM)
    return pl.pallas_call(
        fused_kernel,
        out_shape=jax.ShapeDtypeStruct((192, 1536), F32),
        in_specs=[vmem, vmem, hbm, pl.BlockSpec(memory_space=pltpu.SMEM), hbm, vmem],
        out_specs=vmem,
        scratch_shapes=[
            pltpu.SMEM((1,), jnp.int32),
            pltpu.VMEM((8, 34, 2, 32, 256), F32),
            pltpu.VMEM((8, 2, 2, 2, 32, 256), F32),
            pltpu.VMEM((16, 128, 128), F32),
            pltpu.VMEM((4, 128, 128), F32),
            pltpu.VMEM((16, 256, 256), F32),
            pltpu.VMEM((64, 8, 384), F32),
            pltpu.VMEM((64, 8, 384), F32),
            pltpu.VMEM((64, 32, 96), F32),
            pltpu.VMEM((16, 2, 2, 64, 96), F32),
            pltpu.VMEM((256, 96), BF16),
            pltpu.VMEM((256, 96), BF16),
            pltpu.VMEM((2, 128, 96), F32),
            pltpu.VMEM((16, 96, 128), F32),
            pltpu.VMEM((4, 16, 2, 96, 128), F32),
            pltpu.VMEM((4, 16, 2, 96, 128), F32),
            pltpu.VMEM((4, 192, 768), F32),
            pltpu.VMEM((768, 256), F32),
            pltpu.VMEM((256, 768), BF16),
            pltpu.VMEM((256, 768), BF16),
            pltpu.VMEM((1, 6144), F32),
            pltpu.VMEM((4, 192, 384), F32),
            pltpu.VMEM((4, 192, 384), F32),
            pltpu.VMEM((4, 192, 384), F32),
            pltpu.VMEM((2, 96, 384), F32),
            dma, dma, dma((4,)), dma((2,)), dma((2, 4)), dma, dma((16,)), dma, dma((4,)),
            dma, dma((16,)), dma, dma((16,)),
            dma, dma((3, 16)), dma, dma((3, 16)), dma, dma((16,)),
            dma((4,)), dma((4,)), dma((6,)), dma((6,)),
        ],
        compiler_params=pltpu.CompilerParams(
            collective_id=0, has_side_effects=True, vmem_limit_bytes=52 * 2**20),
    )(integrals, slots, factor, occ, slab, virt)


def shards(integrals, slot_order, factor_rows, occ_energy, slab_index, virt_energy):
    def stay(value):
        return pltpu.with_memory_space_constraint(value, pltpu.HBM)

    return amplitude_block(stay(integrals[0, 0]), stay(slot_order[0]), stay(factor_rows[:, 0]),
                           stay(occ_energy), slab_index, stay(virt_energy[None]))


def solution(mesh):
    in_specs = (
        P("blk", "sub", None, None),
        P("blk", "sub", None),
        P(None, "sub", None, None),
        P(),
        P(),
        P(),
    )
    out_specs = P("blk", "sub")
    return jax.shard_map(shards, mesh=mesh, in_specs=in_specs, out_specs=out_specs, check_vma=False)
```
